32 devices in a mesh: groups: 2 (over y), docs: 4 (over z), mp: 2 (over x), sub: 2 (over core).
Axes of the slice: x: 2, y: 2, z: 4, core: 2. Of those that a mesh axis runs over, the one named last changes fastest.
Arguments:
- embeddings: bfloat16 [4096, 1024], P(('groups', 'docs', 'mp', 'sub')), parts along dimension 0, may hold values from -6 to 6
- owner_shard: int32 [4096, 1], P(('groups', 'docs', 'mp', 'sub')), parts along dimension 0, may hold values from 0 to 3; in each aligned block of 128 rows (0 to 127, 128 to 255, ...) at most 64 rows name the same one
- query_local: int32 [4096], P(('groups', 'docs', 'mp', 'sub')), parts along dimension 0, may hold values from 0 to 1
- labels: int32 [4096], P(('groups', 'docs', 'mp', 'sub')), parts along dimension 0, may hold values from 0 to 4
- w_first: bfloat16 [1024, 1024], replicated, may hold values from -0.1875 to 0.1875
- w_second: float32 [1024], replicated, may hold values from -0.1875 to 0.1875
Outputs:
- emb_grad: bfloat16 [4096, 1024], P(('groups', 'docs', 'mp', 'sub')), parts along dimension 0
- w_first_grad: float32 [2048, 1024], P(('groups', 'mp', 'sub')), parts along dimension 0
- w_second_grad: float32 [2048], P('groups'), parts along dimension 0
The draws below stay inside these ranges and needn't reach their ends.
There are 2 independent parts, one for each index of `groups`. The reference program is written for one: setup_inputs(seed, part) draws one part's arguments, and reference() takes and returns one part's arrays. A program takes and returns all parts, laid end to end along the dimension named above; an argument that names none is the same for every part. Nothing has to cross between parts.
Inputs may be any that keep to these rules, and one draw needn't show every extreme that they name: `owner_shard`: among the 128 rows of one document shard no owner appears more than 64 times, and some owner appears exactly 64 times.
All inputs are finite; a program needn't handle non-finite values.
Results may differ from the reference program's by a relative error of at most 0.017.
Values may be sent and summed in bfloat16 or wider, within the bound.
A program may use at most 64 MiB of HBM per device.

```python
import math
import jax
import jax.numpy as jnp
import numpy as np
from jax import lax

E = 1024
H = 1024
C_DEV = 128
Q_DEV = 2
CAND = 2048
CAP = 64
N_DOCS = 4
N_MP = 2
N_SUB = 2


def with_ends(entries, own_key, low, top_value):
    place = [jax.random.randint(jax.random.fold_in(own_key, axis), (), 0, length) for axis, length in enumerate(entries.shape)]
    main_axis = entries.shape.index(max(entries.shape))
    beside = place[:main_axis] + [(place[main_axis] + 1) % entries.shape[main_axis]] + place[main_axis + 1:]
    return entries.at[tuple(place)].set(low).at[tuple(beside)].set(top_value)


def shard_levels(own_key, dims, split, least, top_value):
    def one(axis_at, shards_of):
        heights = jax.random.uniform(jax.random.fold_in(jax.random.fold_in(own_key, 6), axis_at), (shards_of,), jnp.float32, least / len(split), top_value / len(split))
        return jnp.repeat(jnp.exp(heights), dims[axis_at] // shards_of).reshape((-1,) + (1,) * (len(dims) - axis_at - 1))

    loudness = one(*split[0])
    for cut in split[1:]:
        loudness = loudness * one(*cut)
    return loudness


def shared_out(key, own, number, rows, count, top, reach, lean):
    sequence = jax.random.permutation(key, count)
    packed, ordinary = shares(count, rows * top, reach, lean, True), shares(count, rows * top, reach, lean, False)
    places = jnp.arange(count)

    def named(tallies, offset_by):
        used = int((tallies > 0).sum())
        fixed = max(1, used // 4)
        shifted = fixed + (places - fixed + offset_by * (used - fixed)) % max(1, count - fixed)
        return jnp.zeros((count,), jnp.int32).at[sequence[jnp.where(places < fixed, places, shifted)]].set(jnp.asarray(tallies, jnp.int32))

    tallies = jnp.where(number % 4 == 0, named(packed, number // 4), named(ordinary, number - number // 4 - 1))
    mixed = jax.random.permutation(jax.random.fold_in(own, 3), count)
    giver, sink = mixed[0:count // 2 * 2:2], mixed[1:count // 2 * 2:2]
    margin = jnp.minimum(tallies[giver] - 1, reach - tallies[sink]) // 2
    margin = jnp.where((giver == sequence[0]) | (sink == sequence[0]) | (tallies[sink] == 0), 0, jnp.maximum(margin, 0))
    shifted = jax.random.randint(jax.random.fold_in(own, 4), (count // 2,), 0, 1 << 20) % (margin + 1)
    tallies = tallies.at[giver].add(-shifted).at[sink].add(shifted)
    items = jnp.searchsorted(jnp.cumsum(tallies), jnp.arange(rows * top), side="right").astype(jnp.int32)
    listing = items.reshape(top, rows).T
    listing = listing[jax.random.permutation(jax.random.fold_in(own, 1), rows)]
    offset_by = jax.random.randint(jax.random.fold_in(own, 2), (rows, 1), 0, top)
    return jnp.take_along_axis(listing, (jnp.arange(top)[None, :] + offset_by) % top, axis=1)


def shares(count, total, most, slope, full):
    portions = [(1 << 20) // math.isqrt(grade ** slope) + 1 for grade in range(1, count + 1)]
    largest = most if full else min(most, max(-(-total // count), total * portions[0] // sum(portions)))
    least = 1 if total - largest >= count - 1 else 0
    holding, rest = [largest] + [least] * (count - 1), total - largest - least * (count - 1)
    while rest > 0:
        movable = [i for i in range(1, count) if holding[i] < largest] or [i for i in range(1, count) if holding[i] < most]
        mass, left = sum([portions[i] for i in movable]), rest
        for i in movable:
            extra = min(most - holding[i], max(1, left * portions[i] // mass), rest)
            holding[i] = holding[i] + extra
            rest = rest - extra
    return np.array(holding)


def scatter_about(stream_key, extent, spread, most, pieces=(), held_as=jnp.bfloat16):
    result = jax.random.normal(stream_key, extent, jnp.float32) * spread
    if len(pieces) > 0:
        result = shard_levels(stream_key, extent, pieces, -0.22, 0.18) * result
    return jnp.clip(result, min=-most, max=most).astype(held_as)


def setup_inputs(seed: int = 0, part: int = 0) -> dict:
    streams_of = jax.random.split(jax.random.key(seed), 7)
    part_keys = jax.random.split(jax.random.fold_in(streams_of[6], part), 7)
    embeddings = scatter_about(part_keys[0], (CAND, E), 1.0, 6.0, ((0, 16),))
    owner_shard_keys = jax.random.split(jax.random.fold_in(part_keys[1], 1), CAND // C_DEV)
    owner_shard_turns = jax.random.permutation(jax.random.fold_in(part_keys[1], 3), CAND // C_DEV)
    owner_shard = jax.vmap(lambda own, number: shared_out(jax.random.fold_in(part_keys[1], 2), own, number, C_DEV, N_DOCS, 1, CAP, 2))(owner_shard_keys, owner_shard_turns).reshape((CAND, 1))
    query_local = with_ends(jax.random.randint(part_keys[2], (CAND,), 0, Q_DEV), jax.random.fold_in(part_keys[2], 1), 0, Q_DEV - 1).astype(jnp.int32)
    labels = with_ends(jax.random.randint(part_keys[3], (CAND,), 0, 5), jax.random.fold_in(part_keys[3], 1), 0, 4).astype(jnp.int32)
    w_first = scatter_about(streams_of[4], (E, H), E ** -0.5, 0.1875)
    w_second = scatter_about(streams_of[5], (H,), H ** -0.5, 0.1875, (), jnp.float32)
    return {"embeddings": embeddings, "owner_shard": owner_shard, "query_local": query_local, "labels": labels, "w_first": w_first, "w_second": w_second}


ranking_softness = 1.0


def silu_slope(pre_act):
    sigmoid_v = jax.nn.sigmoid(pre_act)
    return sigmoid_v * (1.0 + pre_act * (1.0 - sigmoid_v))


def rank_rows(row_start, row_count, scorer_outputs, query_mark, grade_slot):
    row_query = lax.dynamic_slice_in_dim(query_mark, row_start, row_count)
    single_row_score = lax.dynamic_slice_in_dim(scorer_outputs, row_start, row_count)
    row_label = lax.dynamic_slice_in_dim(grade_slot, row_start, row_count)
    slot_index = jnp.arange(scorer_outputs.shape[0], dtype=jnp.int32)
    row_index = row_start + jnp.arange(row_count, dtype=jnp.int32)
    matching_query = (row_query[:, None] == query_mark[None, :]) & (row_query[:, None] > 0)
    smooth_rank = jnp.sum(jnp.where(matching_query, jax.nn.sigmoid((scorer_outputs[None, :] - single_row_score[:, None]) / ranking_softness), 0.0), axis=1) - 0.5
    higher = (grade_slot[None, :] > row_label[:, None]) | ((grade_slot[None, :] == row_label[:, None]) & (slot_index[None, :] < row_index[:, None]))
    ideal_rank = jnp.sum((matching_query & higher).astype(jnp.float32), axis=1)
    row_gain = jnp.exp2(row_label.astype(jnp.float32)) - 1.0
    return smooth_rank, row_gain / jnp.log2(2.0 + ideal_rank)


def lambda_rows(row_start, row_count, scorer_outputs, query_mark, grade_slot, discount, inv_ideal):
    gain_all = jnp.exp2(grade_slot.astype(jnp.float32)) - 1.0
    row_query = lax.dynamic_slice_in_dim(query_mark, row_start, row_count)
    single_row_score = lax.dynamic_slice_in_dim(scorer_outputs, row_start, row_count)
    row_label = lax.dynamic_slice_in_dim(grade_slot, row_start, row_count)
    row_gain = lax.dynamic_slice_in_dim(gain_all, row_start, row_count)
    row_disc = lax.dynamic_slice_in_dim(discount, row_start, row_count)
    row_inv = lax.dynamic_slice_in_dim(inv_ideal, row_start, row_count)
    matching_query = (row_query[:, None] == query_mark[None, :]) & (row_query[:, None] > 0)
    score_gap = single_row_score[:, None] - scorer_outputs[None, :]
    weights = jnp.abs(row_gain[:, None] - gain_all[None, :]) * jnp.abs(row_disc[:, None] - discount[None, :]) * row_inv[:, None]
    direction = jnp.where(row_label[:, None] > grade_slot[None, :], -jax.nn.sigmoid(-score_gap), 0.0) + jnp.where(grade_slot[None, :] > row_label[:, None], jax.nn.sigmoid(score_gap), 0.0)
    return jnp.sum(jnp.where(matching_query, weights * direction, 0.0), axis=1)


def owner_lambdas(scorer_outputs, query_mark, grade_slot):
    slot_total = scorer_outputs.shape[0]
    row_count = math.gcd(slot_total, 512)
    starts = jnp.arange(0, slot_total, row_count, dtype=jnp.int32)

    def rank_block(first_row):
        return rank_rows(first_row, row_count, scorer_outputs, query_mark, grade_slot)

    smooth_rank, ideal_term = lax.map(rank_block, starts)
    smooth_rank = smooth_rank.reshape(slot_total)
    ideal_term = ideal_term.reshape(slot_total)
    discount = 1.0 / jnp.log2(2.0 + smooth_rank)
    member = (query_mark[:, None] == jnp.arange(1, Q_DEV + 1, dtype=jnp.int32)[None, :]).astype(jnp.float32)
    per_query = jnp.dot(ideal_term, member, precision=lax.Precision.HIGHEST)
    idcg = jnp.dot(member, per_query, precision=lax.Precision.HIGHEST)
    inv_ideal = jnp.where(idcg > 0.0, 1.0 / jnp.where(idcg > 0.0, idcg, 1.0), 0.0)

    def lambda_block(first_row):
        return lambda_rows(first_row, row_count, scorer_outputs, query_mark, grade_slot, discount, inv_ideal)

    return lax.map(lambda_block, starts).reshape(slot_total)


def owner_step(triple):
    return owner_lambdas(triple[0], triple[1], triple[2])


def reference(embeddings, owner_shard, query_local, labels, w_first, w_second):
    lanes = N_MP * N_SUB
    shards = N_DOCS * lanes
    slot_total = N_DOCS * CAP
    whole = shards * slot_total
    target = owner_shard[:, 0].astype(jnp.int32)
    hits = (target.reshape(shards, C_DEV)[:, :, None] == jnp.arange(N_DOCS, dtype=jnp.int32)[None, None, :]).astype(jnp.int32)
    before = (jnp.cumsum(hits, axis=1).astype(jnp.int32) - hits) * hits
    earlier = jnp.sum(before, axis=2).astype(jnp.int32).reshape(CAND)
    block_of = jnp.arange(CAND, dtype=jnp.int32) // C_DEV
    lane_of = block_of % lanes
    source_of = block_of // lanes
    slot_of = (((lane_of * N_DOCS + target) * N_DOCS + source_of) * CAP + earlier).astype(jnp.int32)
    emb_blocks = embeddings.reshape(shards, C_DEV, E)

    def forward(block):
        pre_act = jnp.dot(block, w_first, preferred_element_type=jnp.float32)
        hidden = pre_act * jax.nn.sigmoid(pre_act)
        return jnp.dot(hidden, w_second, precision=lax.Precision.HIGHEST)

    scorer_outputs = lax.map(forward, emb_blocks).reshape(CAND)
    query_mark = jnp.zeros((whole,), jnp.int32).at[slot_of].set(query_local.astype(jnp.int32) + 1)
    grade_slot = jnp.zeros((whole,), jnp.int32).at[slot_of].set(labels.astype(jnp.int32))
    score_slot = jnp.zeros((whole,), jnp.float32).at[slot_of].set(scorer_outputs)
    lambda_slot = lax.map(owner_step, (score_slot.reshape(shards, slot_total), query_mark.reshape(shards, slot_total), grade_slot.reshape(shards, slot_total)))
    lambdas = lambda_slot.reshape(whole)[slot_of]
    lambda_blocks = lambdas.reshape(shards, C_DEV)

    def backward(carry, pair):
        block, lambda_per_block = pair
        pre_act = jnp.dot(block, w_first, preferred_element_type=jnp.float32)
        hidden = pre_act * jax.nn.sigmoid(pre_act)
        pre_grad = (lambda_per_block[:, None] * w_second[None, :] * silu_slope(pre_act)).astype(jnp.bfloat16)
        emb_part = lax.dot_general(pre_grad, w_first, (((1,), (1,)), ((), ())), preferred_element_type=jnp.float32).astype(jnp.bfloat16)
        first = carry[0] + lax.dot_general(block, pre_grad, (((0,), (0,)), ((), ())), preferred_element_type=jnp.float32)
        second = carry[1] + jnp.dot(lambda_per_block, hidden, precision=lax.Precision.HIGHEST)
        return (first, second), emb_part

    start_carry = (jnp.zeros((E, H), jnp.float32), jnp.zeros((H,), jnp.float32))
    totals, emb_parts = lax.scan(backward, start_carry, (emb_blocks, lambda_blocks))
    return emb_parts.reshape(CAND, E), totals[0], totals[1]
```

```python
import functools

import jax
import jax.numpy as jnp
from jax import lax
from jax.experimental import pallas as pl
from jax.experimental.pallas import tpu as pltpu
from jax.sharding import PartitionSpec as P

MESH = pl.DeviceIdType.MESH
LANES = 128
LOG2E = 1.4426950408889634


def log2(v):
    return jnp.log(v) * LOG2E


def across(row, rows):
    return jnp.broadcast_to(row, (rows, row.shape[1])).T


def row_tile(column):
    return jnp.broadcast_to(column, (column.shape[0], LANES)).T[0:8, :]


def kernel(
    sizes,
    emb_hbm, w1_hbm, owner_ref, local_ref, labels_ref, w2_ref,
    emb_grad_ref, w1g_ref, w2g_ref,
    w1v, embs, slope, hid, pg, at, wacc,
    minfo, sinfo, term, drow, lam, w2p,
    part, from_out, from_in, tot,
    load_sem, emb_send, emb_recv, m_send, m_recv, s_send, s_recv,
    l_send, l_recv, g_send, g_recv, in_send, out_send, fo_recv, fi_recv,
):
    D, M, S, C, E, H, rows, Kc, Kr = sizes
    L = M * S
    K = Kc * Kr
    d, m, s = lax.axis_index("docs"), lax.axis_index("mp"), lax.axis_index("sub")
    me = m * S + s

    load_w = pltpu.make_async_copy(w1_hbm, w1v, load_sem.at[0])
    load_e = pltpu.make_async_copy(emb_hbm, embs.at[pl.ds(me * C, C)], load_sem.at[1])
    load_e.start()
    load_w.start()

    def doc_peer(k):
        return lax.rem(d + k, D)

    def mp_peer(k):
        return lax.rem(m + k, M)

    def sub_peer(k):
        return lax.rem(s + k, S)

    lane_steps = [(a, b) for a in range(M) for b in range(S) if a or b]

    barrier = pltpu.get_barrier_semaphore()
    for k in range(1, D):
        pl.semaphore_signal(barrier, inc=1, device_id={"docs": doc_peer(k)}, device_id_type=MESH)
    for a, b in lane_steps:
        pl.semaphore_signal(
            barrier, inc=1, device_id={"mp": mp_peer(a), "sub": sub_peer(b)}, device_id_type=MESH
        )

    lab_own = labels_ref[...].astype(jnp.float32)
    q_own = (owner_ref[...] * 1024 + local_ref[...]).astype(jnp.float32)
    minfo[d, 0:1, :] = lab_own
    minfo[d, 1:2, :] = q_own

    pl.semaphore_wait(barrier, D - 1 + L - 1)

    def doc_send(buf, k, send, recv):
        return pltpu.make_async_remote_copy(
            src_ref=buf.at[d], dst_ref=buf.at[d], send_sem=send.at[k], recv_sem=recv.at[k],
            device_id={"docs": doc_peer(k)}, device_id_type=MESH,
        )

    load_e.wait()

    def emb_copy(lane, a, b, index):
        block = embs.at[pl.ds(lane * C, C)]
        return pltpu.make_async_remote_copy(
            src_ref=block, dst_ref=block, send_sem=emb_send.at[index], recv_sem=emb_recv.at[index],
            device_id={"mp": mp_peer(a), "sub": sub_peer(b)}, device_id_type=MESH,
        )

    for a in range(1, M):
        emb_copy(me, a, 0, a * S).start()
    for b in range(1, S):
        emb_copy(me, 0, b, b).start()
    for k in range(1, D):
        doc_send(minfo, k, m_send, m_recv).start()

    w2 = w2_ref[...]

    def forward(lane):
        at_rows = pl.ds(lane * C, C)
        act = jnp.dot(embs[at_rows, :], w1v[...], preferred_element_type=jnp.float32)
        sg = jax.nn.sigmoid(act)
        hidden = act * sg
        hid[at_rows, :] = hidden
        slope[at_rows, :] = w2 * (sg * (1.0 + act * (1.0 - sg)))
        return hidden

    load_w.wait()
    hidden = forward(me)
    sinfo[d] = row_tile(jnp.sum(hidden * w2, axis=1, keepdims=True))
    for k in range(1, D):
        doc_send(sinfo, k, s_send, s_recv).start()

    def lane_from(a, b):
        return lax.rem(m + M - a, M) * S + lax.rem(s + S - b, S)

    def recv_wait(a, b):
        emb_copy(lane_from(a, b), a, b, a * S + b).wait_recv()

    for b in range(1, S):
        recv_wait(0, b)
        forward(lane_from(0, b))

    for k in range(1, D):
        doc_send(minfo, k, m_send, m_recv).wait_recv()
    slot = lax.broadcasted_iota(jnp.int32, (1, C), 1).astype(jnp.float32)
    total = float(D * C)

    def key_of(label_row, dd):
        return label_row * total - (slot + lax.convert_element_type(dd * C, jnp.float32))

    def ideal_step(jd, carry):
        q_j = across(minfo[jd, 1:2, :], C)
        key_j = across(key_of(minfo[jd, 0:1, :], jd), C)
        out = []
        for i in range(D):
            ahead = (q_j == minfo[i, 1:2, :]) & (key_j > key_of(minfo[i, 0:1, :], i))
            out.append(carry[i] + jnp.sum(jnp.where(ahead, 1.0, 0.0), axis=0, keepdims=True))
        return tuple(out)

    zeros = tuple(jnp.zeros((1, C), jnp.float32) for _ in range(D))
    ideal = lax.fori_loop(0, D, ideal_step, zeros)
    for i in range(D):
        gain = jnp.exp2(minfo[i, 0:1, :]) - 1.0
        term[i, 0:1, :] = gain / log2(2.0 + ideal[i])
    q_i = across(q_own, C)
    gain_i = across(jnp.exp2(lab_own) - 1.0, C)
    idcg = jnp.zeros((C, C), jnp.float32)
    for j in range(D):
        idcg = idcg + jnp.where(q_i == minfo[j, 1:2, :], term[j, 0:1, :], 0.0)
    idcg = jnp.sum(idcg, axis=1, keepdims=True)
    inv = jnp.where(idcg > 0.0, 1.0 / jnp.where(idcg > 0.0, idcg, 1.0), 0.0)

    for k in range(1, D):
        doc_send(sinfo, k, s_send, s_recv).wait_recv()

    def soft_step(jd, carry):
        q_j = across(minfo[jd, 1:2, :], C)
        s_j = across(sinfo[jd, 0:1, :], C)
        out = []
        for i in range(D):
            part_of = jnp.where(
                q_j == minfo[i, 1:2, :], jax.nn.sigmoid(s_j - sinfo[i, 0:1, :]), 0.0
            )
            out.append(carry[i] + jnp.sum(part_of, axis=0, keepdims=True))
        return tuple(out)

    soft = lax.fori_loop(0, D, soft_step, zeros)
    for i in range(D):
        drow[i, 0:1, :] = 1.0 / log2(2.0 + (soft[i] - 0.5))
    disc_i = across(drow[d, 0:1, :], C)
    s_i = across(sinfo[d, 0:1, :], C)

    def lambda_step(j, acc):
        gain_j = jnp.exp2(minfo[j, 0:1, :]) - 1.0
        gap = s_i - sinfo[j, 0:1, :]
        weight = (gain_j - gain_i) * jnp.abs(disc_i - drow[j, 0:1, :])
        push = jax.nn.sigmoid(jnp.where(gain_i > gain_j, -gap, gap))
        return acc + jnp.where(q_i == minfo[j, 1:2, :], weight * push, 0.0)

    lam_acc = lax.fori_loop(0, D, lambda_step, jnp.zeros((C, C), jnp.float32))
    lam_col = jnp.sum(lam_acc, axis=1, keepdims=True) * inv
    lam[me] = row_tile(lam_col)

    def lam_copy(lane, a, b):
        return pltpu.make_async_remote_copy(
            src_ref=lam.at[lane], dst_ref=lam.at[lane],
            send_sem=l_send.at[a * S + b], recv_sem=l_recv.at[a * S + b],
            device_id={"mp": mp_peer(a), "sub": sub_peer(b)}, device_id_type=MESH,
        )

    for a, b in lane_steps:
        lam_copy(me, a, b).start()

    def scale(lane, column):
        at_rows = pl.ds(lane * C, C)
        pg[at_rows, :] = (column * slope[at_rows, :]).astype(jnp.bfloat16)

    scale(me, lam_col)
    emb_grad_ref[...] = lax.dot_general(
        pg[pl.ds(me * C, C), :], w1v[...], (((1,), (1,)), ((), ())),
        preferred_element_type=jnp.float32,
    ).astype(jnp.bfloat16)
    for a in range(1, M):
        recv_wait(a, 0)
        for b in range(1, S):
            emb_copy(lane_from(a, 0), 0, b, a * S + b).start()
        forward(lane_from(a, 0))
    for a in range(1, M):
        for b in range(1, S):
            recv_wait(a, b)
            forward(lane_from(a, b))
    width = at.shape[0]
    first = pl.multiple_of((me * rows) // LANES * LANES, LANES)
    for lane in range(L):
        at[:, pl.ds(lane * C, C)] = embs[pl.ds(lane * C, C), pl.ds(first, width)].T

    for a, b in lane_steps:
        lam_copy(lane_from(a, b), a, b).wait_recv()
        lane = lane_from(a, b)
        scale(lane, across(lam[lane, 0:1, :], C)[:, 0:1])

    half = D // 2
    left = d < half
    inward = jnp.where(left, d + 1, d - 1)
    outward = jnp.where(left, d - 1, d + 1)
    place = jnp.where(left, d, D - 1 - d)
    has_out = place > 0
    middle = place == half - 1
    cw, rh = H // Kc, rows // Kr

    def send_in(k, to_middle):
        dst, sem = (from_in, fi_recv) if to_middle else (from_out, fo_recv)
        return pltpu.make_async_remote_copy(
            src_ref=part.at[k], dst_ref=dst.at[k], send_sem=in_send.at[k], recv_sem=sem.at[k],
            device_id={"docs": inward}, device_id_type=MESH,
        )

    def send_out(k, from_total):
        src = tot if from_total else from_in
        return pltpu.make_async_remote_copy(
            src_ref=src.at[k], dst_ref=from_in.at[k], send_sem=out_send.at[k],
            recv_sem=fi_recv.at[k], device_id={"docs": outward}, device_id_type=MESH,
        )

    def start_in(k):
        pl.when(middle)(lambda: send_in(k, True).start())
        if half > 1:
            pl.when(jnp.logical_not(middle))(lambda: send_in(k, False).start())

    shift = me * rows - first
    for c in range(Kc):
        wide = jnp.dot(at[...], pg[:, c * cw : (c + 1) * cw], preferred_element_type=jnp.float32)
        wacc[c] = wide
        for r in range(Kr):
            k = c * Kr + r

            @pl.when(jnp.logical_not(has_out))
            def _():
                part[k] = wacc[c, pl.ds(pl.multiple_of(shift + r * rh, 8), rh), :].astype(
                    jnp.bfloat16
                )
                start_in(k)

    w2_part = jnp.zeros((1, H), jnp.float32)
    for lane in range(L):
        column = across(lam[lane, 0:1, :], C)[:, 0:1]
        w2_part = w2_part + jnp.sum(column * hid[pl.ds(lane * C, C), :], axis=0, keepdims=True)
    for j in range(H // LANES):
        w2p[d, j : j + 1, :] = w2_part[:, j * LANES : (j + 1) * LANES]
    for k in range(1, D):
        doc_send(w2p, k, g_send, g_recv).start()

    def gather_step(k):
        c, r = k // Kr, k % Kr

        @pl.when(has_out)
        def _():
            send_in(k, False).wait_recv()
            own = wacc[c, pl.ds(pl.multiple_of(shift + r * rh, 8), rh), :]
            part[k] = (own + from_out[k].astype(jnp.float32)).astype(jnp.bfloat16)
            start_in(k)

    def finish_step(k):
        c, r = k // Kr, k % Kr
        send_out(k, False).wait_recv()
        spot = (slice(r * rh, (r + 1) * rh), slice(c * cw, (c + 1) * cw))

        @pl.when(middle)
        def _():
            both = (part[k].astype(jnp.float32) + from_in[k].astype(jnp.float32)).astype(
                jnp.bfloat16
            )
            w1g_ref[spot] = both.astype(jnp.float32)
            if half > 1:
                tot[k] = both
                pl.when(has_out)(lambda: send_out(k, True).start())

        if half > 1:

            @pl.when(jnp.logical_not(middle))
            def _():
                pl.when(has_out)(lambda: send_out(k, False).start())
                w1g_ref[spot] = from_in[k].astype(jnp.float32)

    lag = max(1, K // 4)
    for k in range(lag):
        gather_step(k)
    for k in range(lag, K + lag):
        if k < K:
            gather_step(k)
        finish_step(k - lag)

    for k in range(1, D):
        doc_send(w2p, k, g_send, g_recv).wait_recv()
    w2_sum = w2p[d]
    for k in range(1, D):
        w2_sum = w2_sum + w2p[doc_peer(k)]
    for j in range(H // LANES):
        w2g_ref[0:1, j * LANES : (j + 1) * LANES] = w2_sum[j : j + 1, :]

    for k in range(1, D):
        doc_send(minfo, k, m_send, m_recv).wait_send()
        doc_send(sinfo, k, s_send, s_recv).wait_send()
        doc_send(w2p, k, g_send, g_recv).wait_send()
    for a, b in lane_steps:
        emb_copy(me, a, b, a * S + b).wait_send()
        lam_copy(me, a, b).wait_send()
    for k in range(K):
        send_in(k, True).wait_send()
    for k in range(K):
        pl.when(has_out)(lambda k=k: send_out(k, False).wait_send())


def write_out(a_ref, b_ref, c_ref, a_out, b_out, c_out, sem):
    pairs = ((b_ref, b_out), (a_ref, a_out), (c_ref, c_out))
    copies = [pltpu.make_async_copy(x, y, sem.at[i]) for i, (x, y) in enumerate(pairs)]
    for copy in copies:
        copy.start()
    for copy in copies:
        copy.wait()


def on_device(embeddings, owner_shard, query_local, labels, w_first, w_second):
    D, M, S = lax.axis_size("docs"), lax.axis_size("mp"), lax.axis_size("sub")
    C, E = embeddings.shape
    H = w_first.shape[1]
    L = M * S
    rows = E // L
    width = max(rows, LANES)
    Kc = 4
    Kr = max(1, rows // 32)
    K = Kc * Kr
    f32, bf16 = jnp.float32, jnp.bfloat16
    vmem = pl.BlockSpec(memory_space=pltpu.VMEM)
    hbm = pl.BlockSpec(memory_space=pl.ANY)
    dma = pltpu.SemaphoreType.DMA
    chunk = (K, rows // Kr, H // Kc)
    scratch = [
        pltpu.VMEM((E, H), bf16),
        pltpu.VMEM((L * C, E), bf16),
        pltpu.VMEM((L * C, H), f32),
        pltpu.VMEM((L * C, H), f32),
        pltpu.VMEM((L * C, H), bf16),
        pltpu.VMEM((width, L * C), bf16),
        pltpu.VMEM((Kc, width, H // Kc), f32),
        pltpu.VMEM((D, 8, C), f32),
        pltpu.VMEM((D, 8, C), f32),
        pltpu.VMEM((D, 8, C), f32),
        pltpu.VMEM((D, 8, C), f32),
        pltpu.VMEM((L, 8, C), f32),
        pltpu.VMEM((D, H // LANES, LANES), f32),
        pltpu.VMEM(chunk, bf16),
        pltpu.VMEM(chunk, bf16),
        pltpu.VMEM(chunk, bf16),
        pltpu.VMEM(chunk, bf16),
        dma((2,)),
        dma((L,)), dma((L,)),
        dma((D,)), dma((D,)),
        dma((D,)), dma((D,)),
        dma((L,)), dma((L,)),
        dma((D,)), dma((D,)),
        dma((K,)), dma((K,)), dma((K,)), dma((K,)),
    ]
    emb_grad, w1g, w2g = pl.pallas_call(
        functools.partial(kernel, (D, M, S, C, E, H, rows, Kc, Kr)),
        out_shape=(
            pltpu.VMEM((C, E), bf16),
            pltpu.VMEM((rows, H), f32),
            pltpu.VMEM((1, H), f32),
        ),
        in_specs=[hbm, hbm, vmem, vmem, vmem, vmem],
        out_specs=(vmem, vmem, vmem),
        scratch_shapes=scratch,
        compiler_params=pltpu.CompilerParams(
            collective_id=0, has_side_effects=True, vmem_limit_bytes=56 * 1024 * 1024
        ),
    )(
        embeddings, w_first, owner_shard.reshape(1, C), query_local.reshape(1, C),
        labels.reshape(1, C), w_second.reshape(1, H),
    )
    emb_grad, w1g, w2g = pl.pallas_call(
        write_out,
        out_shape=tuple(jax.ShapeDtypeStruct(v.shape, v.dtype) for v in (emb_grad, w1g, w2g)),
        in_specs=[vmem] * 3,
        out_specs=(hbm,) * 3,
        scratch_shapes=[dma((3,))],
        compiler_params=pltpu.CompilerParams(vmem_limit_bytes=4 * 1024 * 1024),
    )(emb_grad, w1g, w2g)
    return emb_grad, w1g, w2g.reshape(H)


def solution(mesh):
    return jax.shard_map(
        on_device,
        mesh=mesh,
        in_specs=(
            P(("groups", "docs", "mp", "sub"), None),
            P(("groups", "docs", "mp", "sub"), None),
            P(("groups", "docs", "mp", "sub")),
            P(("groups", "docs", "mp", "sub")),
            P(),
            P(),
        ),
        out_specs=(
            P(("groups", "docs", "mp", "sub"), None),
            P(("groups", "mp", "sub"), None),
            P("groups"),
        ),
        check_vma=False,
    )
```

```python
import functools

import jax
import jax.numpy as jnp
from jax import lax
from jax.experimental import pallas as pl
from jax.experimental.pallas import tpu as pltpu
from jax.sharding import PartitionSpec as P

MESH = pl.DeviceIdType.MESH
LANES = 128
LOG2E = 1.4426950408889634


def log2(v):
    return jnp.log(v) * LOG2E


def across(row, rows):
    return jnp.broadcast_to(row, (rows, row.shape[1])).T


def row_tile(column):
    return jnp.broadcast_to(column, (column.shape[0], LANES)).T[0:8, :]


def kernel(
    sizes,
    emb_hbm, w1_hbm, owner_ref, local_ref, labels_ref, w2_ref,
    emb_grad_ref, w1g_ref, w2g_ref,
    w1v, embs, slope, hid, pg, at, wacc,
    minfo, sinfo, term, drow, lam, w2p,
    part, from_out, from_in, tot,
    load_sem, emb_send, emb_recv, m_send, m_recv, s_send, s_recv,
    l_send, l_recv, g_send, g_recv, in_send, out_send, fo_recv, fi_recv,
):
    D, M, S, C, E, H, rows, Kc, Kr = sizes
    L = M * S
    K = Kc * Kr
    d, m, s = lax.axis_index("docs"), lax.axis_index("mp"), lax.axis_index("sub")
    me = m * S + s

    load_w = pltpu.make_async_copy(w1_hbm, w1v, load_sem.at[0])
    load_e = pltpu.make_async_copy(emb_hbm, embs.at[pl.ds(me * C, C)], load_sem.at[1])
    load_e.start()
    load_w.start()

    def doc_peer(k):
        return lax.rem(d + k, D)

    def mp_peer(k):
        return lax.rem(m + k, M)

    def sub_peer(k):
        return lax.rem(s + k, S)

    lane_steps = [(a, b) for a in range(M) for b in range(S) if a or b]

    barrier = pltpu.get_barrier_semaphore()
    for k in range(1, D):
        pl.semaphore_signal(barrier, inc=1, device_id={"docs": doc_peer(k)}, device_id_type=MESH)
    for a, b in lane_steps:
        pl.semaphore_signal(
            barrier, inc=1, device_id={"mp": mp_peer(a), "sub": sub_peer(b)}, device_id_type=MESH
        )

    lab_own = labels_ref[...].astype(jnp.float32)
    q_own = (owner_ref[...] * 1024 + local_ref[...]).astype(jnp.float32)
    minfo[d, 0:1, :] = lab_own
    minfo[d, 1:2, :] = q_own

    pl.semaphore_wait(barrier, D - 1 + L - 1)

    def doc_send(buf, k, send, recv):
        return pltpu.make_async_remote_copy(
            src_ref=buf.at[d], dst_ref=buf.at[d], send_sem=send.at[k], recv_sem=recv.at[k],
            device_id={"docs": doc_peer(k)}, device_id_type=MESH,
        )

    load_e.wait()

    def emb_copy(lane, a, b, index):
        block = embs.at[pl.ds(lane * C, C)]
        return pltpu.make_async_remote_copy(
            src_ref=block, dst_ref=block, send_sem=emb_send.at[index], recv_sem=emb_recv.at[index],
            device_id={"mp": mp_peer(a), "sub": sub_peer(b)}, device_id_type=MESH,
        )

    for a in range(1, M):
        emb_copy(me, a, 0, a * S).start()
    for b in range(1, S):
        emb_copy(me, 0, b, b).start()
    for k in range(1, D):
        doc_send(minfo, k, m_send, m_recv).start()

    w2 = w2_ref[...]

    def forward(lane):
        at_rows = pl.ds(lane * C, C)
        act = jnp.dot(embs[at_rows, :], w1v[...], preferred_element_type=jnp.float32)
        sg = jax.nn.sigmoid(act)
        hidden = act * sg
        hid[at_rows, :] = hidden
        slope[at_rows, :] = w2 * (sg * (1.0 + act * (1.0 - sg)))
        return hidden

    load_w.wait()
    hidden = forward(me)
    sinfo[d] = row_tile(jnp.sum(hidden * w2, axis=1, keepdims=True))
    for k in range(1, D):
        doc_send(sinfo, k, s_send, s_recv).start()

    def lane_from(a, b):
        return lax.rem(m + M - a, M) * S + lax.rem(s + S - b, S)

    def recv_wait(a, b):
        emb_copy(lane_from(a, b), a, b, a * S + b).wait_recv()

    for b in range(1, S):
        recv_wait(0, b)
        forward(lane_from(0, b))

    for k in range(1, D):
        doc_send(minfo, k, m_send, m_recv).wait_recv()
    slot = lax.broadcasted_iota(jnp.int32, (1, C), 1).astype(jnp.float32)
    total = float(D * C)

    def key_of(label_row, dd):
        return label_row * total - (slot + lax.convert_element_type(dd * C, jnp.float32))

    def ideal_step(jd, carry):
        q_j = across(minfo[jd, 1:2, :], C)
        key_j = across(key_of(minfo[jd, 0:1, :], jd), C)
        out = []
        for i in range(D):
            ahead = (q_j == minfo[i, 1:2, :]) & (key_j > key_of(minfo[i, 0:1, :], i))
            out.append(carry[i] + jnp.sum(jnp.where(ahead, 1.0, 0.0), axis=0, keepdims=True))
        return tuple(out)

    zeros = tuple(jnp.zeros((1, C), jnp.float32) for _ in range(D))
    ideal = lax.fori_loop(0, D, ideal_step, zeros)
    for i in range(D):
        gain = jnp.exp2(minfo[i, 0:1, :]) - 1.0
        term[i, 0:1, :] = gain / log2(2.0 + ideal[i])
    q_i = across(q_own, C)
    gain_i = across(jnp.exp2(lab_own) - 1.0, C)
    idcg = jnp.zeros((C, C), jnp.float32)
    for j in range(D):
        idcg = idcg + jnp.where(q_i == minfo[j, 1:2, :], term[j, 0:1, :], 0.0)
    idcg = jnp.sum(idcg, axis=1, keepdims=True)
    inv = jnp.where(idcg > 0.0, 1.0 / jnp.where(idcg > 0.0, idcg, 1.0), 0.0)

    for k in range(1, D):
        doc_send(sinfo, k, s_send, s_recv).wait_recv()

    def soft_step(jd, carry):
        q_j = across(minfo[jd, 1:2, :], C)
        s_j = across(sinfo[jd, 0:1, :], C)
        out = []
        for i in range(D):
            part_of = jnp.where(
                q_j == minfo[i, 1:2, :], jax.nn.sigmoid(s_j - sinfo[i, 0:1, :]), 0.0
            )
            out.append(carry[i] + jnp.sum(part_of, axis=0, keepdims=True))
        return tuple(out)

    soft = lax.fori_loop(0, D, soft_step, zeros)
    for i in range(D):
        drow[i, 0:1, :] = 1.0 / log2(2.0 + (soft[i] - 0.5))
    disc_i = across(drow[d, 0:1, :], C)
    s_i = across(sinfo[d, 0:1, :], C)

    def lambda_step(j, acc):
        gain_j = jnp.exp2(minfo[j, 0:1, :]) - 1.0
        gap = s_i - sinfo[j, 0:1, :]
        weight = (gain_j - gain_i) * jnp.abs(disc_i - drow[j, 0:1, :])
        push = jax.nn.sigmoid(jnp.where(gain_i > gain_j, -gap, gap))
        return acc + jnp.where(q_i == minfo[j, 1:2, :], weight * push, 0.0)

    lam_acc = lax.fori_loop(0, D, lambda_step, jnp.zeros((C, C), jnp.float32))
    lam_col = jnp.sum(lam_acc, axis=1, keepdims=True) * inv
    lam[me] = row_tile(lam_col)

    def lam_copy(lane, a, b):
        return pltpu.make_async_remote_copy(
            src_ref=lam.at[lane], dst_ref=lam.at[lane],
            send_sem=l_send.at[a * S + b], recv_sem=l_recv.at[a * S + b],
            device_id={"mp": mp_peer(a), "sub": sub_peer(b)}, device_id_type=MESH,
        )

    for a, b in lane_steps:
        lam_copy(me, a, b).start()

    def scale(lane, column):
        at_rows = pl.ds(lane * C, C)
        pg[at_rows, :] = (column * slope[at_rows, :]).astype(jnp.bfloat16)

    scale(me, lam_col)
    emb_grad_ref[...] = lax.dot_general(
        pg[pl.ds(me * C, C), :], w1v[...], (((1,), (1,)), ((), ())),
        preferred_element_type=jnp.float32,
    ).astype(jnp.bfloat16)
    for a in range(1, M):
        recv_wait(a, 0)
        for b in range(1, S):
            emb_copy(lane_from(a, 0), 0, b, a * S + b).start()
        forward(lane_from(a, 0))
    for a in range(1, M):
        for b in range(1, S):
            recv_wait(a, b)
            forward(lane_from(a, b))
    width = at.shape[0]
    first = pl.multiple_of((me * rows) // LANES * LANES, LANES)
    for lane in range(L):
        at[:, pl.ds(lane * C, C)] = embs[pl.ds(lane * C, C), pl.ds(first, width)].T

    for a, b in lane_steps:
        lam_copy(lane_from(a, b), a, b).wait_recv()
        lane = lane_from(a, b)
        scale(lane, across(lam[lane, 0:1, :], C)[:, 0:1])

    half = D // 2
    left = d < half
    inward = jnp.where(left, d + 1, d - 1)
    outward = jnp.where(left, d - 1, d + 1)
    place = jnp.where(left, d, D - 1 - d)
    has_out = place > 0
    middle = place == half - 1
    cw, rh = H // Kc, rows // Kr

    def send_in(k, to_middle):
        dst, sem = (from_in, fi_recv) if to_middle else (from_out, fo_recv)
        return pltpu.make_async_remote_copy(
            src_ref=part.at[k], dst_ref=dst.at[k], send_sem=in_send.at[k], recv_sem=sem.at[k],
            device_id={"docs": inward}, device_id_type=MESH,
        )

    def send_out(k, from_total):
        src = tot if from_total else from_in
        return pltpu.make_async_remote_copy(
            src_ref=src.at[k], dst_ref=from_in.at[k], send_sem=out_send.at[k],
            recv_sem=fi_recv.at[k], device_id={"docs": outward}, device_id_type=MESH,
        )

    def start_in(k):
        pl.when(middle)(lambda: send_in(k, True).start())
        if half > 1:
            pl.when(jnp.logical_not(middle))(lambda: send_in(k, False).start())

    shift = me * rows - first
    for c in range(Kc):
        wide = jnp.dot(at[...], pg[:, c * cw : (c + 1) * cw], preferred_element_type=jnp.float32)
        wacc[c] = wide
        for r in range(Kr):
            k = c * Kr + r

            @pl.when(jnp.logical_not(has_out))
            def _():
                part[k] = wacc[c, pl.ds(pl.multiple_of(shift + r * rh, 8), rh), :].astype(
                    jnp.bfloat16
                )
                start_in(k)

    w2_part = jnp.zeros((1, H), jnp.float32)
    for lane in range(L):
        column = across(lam[lane, 0:1, :], C)[:, 0:1]
        w2_part = w2_part + jnp.sum(column * hid[pl.ds(lane * C, C), :], axis=0, keepdims=True)
    for j in range(H // LANES):
        w2p[d, j : j + 1, :] = w2_part[:, j * LANES : (j + 1) * LANES]
    for k in range(1, D):
        doc_send(w2p, k, g_send, g_recv).start()

    def gather_step(k):
        c, r = k // Kr, k % Kr

        @pl.when(has_out)
        def _():
            send_in(k, False).wait_recv()
            own = wacc[c, pl.ds(pl.multiple_of(shift + r * rh, 8), rh), :]
            part[k] = (own + from_out[k].astype(jnp.float32)).astype(jnp.bfloat16)
            start_in(k)

    def finish_step(k):
        c, r = k // Kr, k % Kr
        send_out(k, False).wait_recv()
        spot = (slice(r * rh, (r + 1) * rh), slice(c * cw, (c + 1) * cw))

        @pl.when(middle)
        def _():
            both = (part[k].astype(jnp.float32) + from_in[k].astype(jnp.float32)).astype(
                jnp.bfloat16
            )
            w1g_ref[spot] = both.astype(jnp.float32)
            if half > 1:
                tot[k] = both
                pl.when(has_out)(lambda: send_out(k, True).start())

        if half > 1:

            @pl.when(jnp.logical_not(middle))
            def _():
                pl.when(has_out)(lambda: send_out(k, False).start())
                w1g_ref[spot] = from_in[k].astype(jnp.float32)

    lag = max(1, K // 4)
    for k in range(lag):
        gather_step(k)
    for k in range(lag, K + lag):
        if k < K:
            gather_step(k)
        finish_step(k - lag)

    for k in range(1, D):
        doc_send(w2p, k, g_send, g_recv).wait_recv()
    w2_sum = w2p[0]
    for j in range(1, D):
        w2_sum = w2_sum + w2p[j]
    for j in range(H // LANES):
        w2g_ref[0:1, j * LANES : (j + 1) * LANES] = w2_sum[j : j + 1, :]

    for k in range(1, D):
        doc_send(minfo, k, m_send, m_recv).wait_send()
        doc_send(sinfo, k, s_send, s_recv).wait_send()
        doc_send(w2p, k, g_send, g_recv).wait_send()
    for a, b in lane_steps:
        emb_copy(me, a, b, a * S + b).wait_send()
        lam_copy(me, a, b).wait_send()
    for k in range(K):
        send_in(k, True).wait_send()
    for k in range(K):
        pl.when(has_out)(lambda k=k: send_out(k, False).wait_send())

def ring_kernel(
    sizes,
    emb_hbm, w1_hbm, owner_hbm, local_hbm, labels_hbm, w2_hbm,
    emb_grad_ref, w1g_ref, w2g_ref,
    w1v, xs, slope, hid, small, w2v, pre, wtot,
    info, term, drow, lam_all, lam_exp, lam_row, lam_pair,
    load_sem, cw_send, cw_recv, ccw_send, ccw_recv, dd_send, dd_recv,
    i_send, i_recv, l_send, l_recv, stage_sem,
):
    D, M, S, C, E, H, rows, P = sizes
    N = D * M
    PR = C // P
    T = P * (N - 1) // 2
    d, m, s = lax.axis_index("docs"), lax.axis_index("mp"), lax.axis_index("sub")
    me = m * S + s
    other = S - 1 - s
    r = jnp.where(m == 0, d, N - 1 - d)

    def ring_at(q):
        q = lax.rem(q + 2 * N, N)
        return {"docs": jnp.where(q < D, q, N - 1 - q), "mp": jnp.where(q < D, 0, 1)}

    ahead_id, behind_id, twin_id = ring_at(r + 1), ring_at(r - 1), {"sub": other}

    def spot(slot):
        return lax.div(slot, 2), pl.multiple_of(lax.rem(slot, 2) * C, C)

    def block(slot):
        u, row = spot(slot)
        return xs.at[u, pl.ds(row, C)]

    load_e = pltpu.make_async_copy(emb_hbm, block(s), load_sem.at[0])
    load_w = pltpu.make_async_copy(w1_hbm, w1v, load_sem.at[1])
    load_small = [
        pltpu.make_async_copy(owner_hbm, small.at[0], load_sem.at[2]),
        pltpu.make_async_copy(local_hbm, small.at[1], load_sem.at[3]),
        pltpu.make_async_copy(labels_hbm, small.at[2], load_sem.at[4]),
        pltpu.make_async_copy(w2_hbm, w2v, load_sem.at[5]),
    ]
    barrier = pltpu.get_barrier_semaphore()
    for peer in (ahead_id, behind_id, twin_id):
        pl.semaphore_signal(barrier, inc=1, device_id=peer, device_id_type=MESH)
    load_e.start()
    load_w.start()
    for copy in load_small:
        copy.start()

    def remote(src, dst, send, recv, peer):
        return pltpu.make_async_remote_copy(
            src_ref=src, dst_ref=dst, send_sem=send, recv_sem=recv,
            device_id=peer, device_id_type=MESH,
        )

    def part(slot, lane_s, way):
        return block(slot).at[pl.ds((lane_s * 2 + way) * PR, PR)]

    def ahead_copy(src, t):
        return remote(src, part(S + t, s, 0), cw_send.at[t], cw_recv.at[t], ahead_id)

    def behind_copy(src, t):
        return remote(src, part(S + t, s, 1), ccw_send.at[t], ccw_recv.at[t], behind_id)

    def twin_copy(slot, lane_s):
        both = block(slot).at[pl.ds(lane_s * 2 * PR, 2 * PR)]
        return remote(both, both, dd_send.at[slot], dd_recv.at[slot], twin_id)

    own_twin = remote(block(s), block(s), dd_send.at[0], dd_recv.at[0], twin_id)

    def next_stage(k):
        for peer in (ahead_id, behind_id):
            pl.semaphore_signal(stage_sem.at[k], inc=1, device_id=peer, device_id_type=MESH)

    def stage_wait(k):
        pl.semaphore_wait(stage_sem.at[k], 2)

    pl.semaphore_wait(barrier, 3)
    load_e.wait()
    def send_own(p):
        ahead_copy(block(s).at[pl.ds(p * PR, PR)], p).start()
        behind_copy(block(s).at[pl.ds((P - 1 - p) * PR, PR)], p).start()

    for p in range(P // 2):
        send_own(p)
    own_twin.start()
    stages = stage_sem.shape[0]
    next_stage(0)

    for copy in load_small:
        copy.wait()
    load_w.wait()
    w2 = w2v[...]

    def forward(slot):
        u, row = spot(slot)
        act = jnp.dot(xs[u, pl.ds(row, C), :], w1v[...], preferred_element_type=jnp.float32)
        sg = 0.5 + 0.5 * jnp.tanh(0.5 * act)
        hidden = act * sg
        bend = sg + hidden * (1.0 - sg)
        hid[u, pl.ds(row, C), :] = hidden.astype(jnp.bfloat16)
        slope[u, pl.ds(row, C), :] = bend.astype(jnp.bfloat16)
        return hidden, bend

    hidden, bend = forward(s)
    info[d] = row_tile(jnp.sum(hidden * w2, axis=1, keepdims=True))
    info[d, 1:2, :] = small[2].astype(jnp.float32)
    info[d, 2:3, :] = (small[0] * 1024 + small[1]).astype(jnp.float32)
    stage_wait(0)
    if stages > 1:
        next_stage(1)
    pre[...] = lax.dot_general(
        (bend * w2).astype(jnp.bfloat16), w1v[...], (((1,), (1,)), ((), ())),
        preferred_element_type=jnp.float32,
    )
    def doc_peer(k):
        return lax.rem(d + k, D)

    def info_copy(k):
        return remote(
            info.at[d], info.at[d], i_send.at[k], i_recv.at[k], {"docs": doc_peer(k)}
        )

    lane_steps = [(a, b) for a in range(M) for b in range(S) if a or b]

    def lam_copy(a, b):
        peer = {"mp": lax.rem(m + a, M), "sub": lax.rem(s + b, S)}
        return remote(
            lam_all.at[me], lam_all.at[me], l_send.at[a * S + b], l_recv.at[a * S + b], peer
        )

    reach = min(stages, max(1, D - 2))
    for k in range(2, reach + 1):
        stage_wait(k - 1)
        if k < stages:
            next_stage(k)
    for k in range(1, D):
        info_copy(k).start()
    for p in range(P // 2, P):
        send_own(p)
    own_twin.wait_recv()
    forward(other)

    def relay(t):
        ahead_copy(part(S + t, s, 0), t).wait_recv()

        @pl.when(t + P < T)
        def _():
            ahead_copy(part(S + t, s, 0), t + P).start()

        behind_copy(part(S + t, s, 1), t).wait_recv()

        @pl.when(t + P < T)
        def _():
            behind_copy(part(S + t, s, 1), t + P).start()

        twin_copy(S + t, s).start()

    def step_forward(t):
        twin_copy(S + t, other).wait_recv()
        forward(S + t)

    def relay_forward(lag, t, carry):
        relay(t)
        step_forward(t - lag)
        return carry

    early, late = T // 4 + 1, T // 2 + 1
    relay(0)
    lax.fori_loop(1, early, functools.partial(relay_forward, 1), 0)

    for k in range(1, D):
        info_copy(k).wait_recv()
    slot_of = lax.broadcasted_iota(jnp.int32, (1, C), 1).astype(jnp.float32)
    total = float(D * C)

    def key_of(jd):
        return info[jd, 1:2, :] * total - (slot_of + lax.convert_element_type(jd * C, jnp.float32))

    def rank_step(jd, carry):
        q_j = across(info[jd, 2:3, :], C)
        s_j = across(info[jd, 0:1, :], C)
        key_j = across(key_of(jd), C)
        out = []
        for i in range(D):
            same = q_j == info[i, 2:3, :]
            push = 0.5 + 0.5 * jnp.tanh(0.5 * (s_j - info[i, 0:1, :]))
            ahead = same & (key_j > key_of(i))
            out.append(carry[i] + jnp.sum(jnp.where(same, push, 0.0), axis=0, keepdims=True))
            out.append(carry[D + i] + jnp.sum(jnp.where(ahead, 1.0, 0.0), axis=0, keepdims=True))
        return tuple(out[0::2] + out[1::2])

    zeros = tuple(jnp.zeros((1, C), jnp.float32) for _ in range(2 * D))
    ranks = lax.fori_loop(0, D, rank_step, zeros)
    for i in range(D):
        gain = jnp.exp2(info[i, 1:2, :]) - 1.0
        term[i, 0:1, :] = gain / log2(2.0 + ranks[D + i])
        drow[i, 0:1, :] = 1.0 / log2(2.0 + (ranks[i] - 0.5))

    relay(early)

    def lambda_step(jd, carry):
        q_j = across(info[jd, 2:3, :], C)
        s_j = across(info[jd, 0:1, :], C)
        gain_j = across(jnp.exp2(info[jd, 1:2, :]) - 1.0, C)
        disc_j = across(drow[jd, 0:1, :], C)
        term_j = across(term[jd, 0:1, :], C)
        out = []
        for i in range(D):
            same = q_j == info[i, 2:3, :]
            gain_i = jnp.exp2(info[i, 1:2, :]) - 1.0
            gap = info[i, 0:1, :] - s_j
            weight = (gain_j - gain_i) * jnp.abs(drow[i, 0:1, :] - disc_j)
            push = 0.5 + 0.5 * jnp.tanh(0.5 * jnp.where(gain_i > gain_j, -gap, gap))
            out.append(
                carry[i] + jnp.sum(jnp.where(same, weight * push, 0.0), axis=0, keepdims=True)
            )
            out.append(
                carry[D + i] + jnp.sum(jnp.where(same, term_j, 0.0), axis=0, keepdims=True)
            )
        return tuple(out[0::2] + out[1::2])

    sums = lax.fori_loop(0, D, lambda_step, zeros)
    for i in range(D):
        idcg = sums[D + i]
        inv = jnp.where(idcg > 0.0, 1.0 / jnp.where(idcg > 0.0, idcg, 1.0), 0.0)
        lam_all[me, i : i + 1, :] = sums[i] * inv
    for k in range(reach + 1, stages + 1):
        stage_wait(k - 1)
        if k < stages:
            next_stage(k)
    for a, b in lane_steps:
        lam_copy(a, b).start()

    for i in range(D):
        lam_exp[me, i] = jnp.broadcast_to(lam_all[me, i : i + 1, :], (8, C))
    emb_grad_ref[...] = (pre[...] * across(lam_exp[me, d, 0:1, :], C)[:, 0:1]).astype(jnp.bfloat16)

    lax.fori_loop(early + 1, late, functools.partial(relay_forward, 2), 0)
    step_forward(late - 2)

    for a, b in lane_steps:
        lam_copy(a, b).wait_recv()
        lane = lax.rem(m + M - a, M) * S + lax.rem(s + S - b, S)
        for i in range(D):
            lam_exp[lane, i] = jnp.broadcast_to(lam_all[lane, i : i + 1, :], (8, C))

    lane_no = lax.broadcasted_iota(jnp.int32, (8, C), 1) // PR
    row_no = lax.broadcasted_iota(jnp.int32, (16, C), 0)

    def put_lambda(slot, tile):
        cols = slice(slot % 2 * C, slot % 2 * C + C)
        lam_row[slot // 2, :, cols] = tile
        high = tile.astype(jnp.bfloat16).astype(jnp.float32)
        both = jnp.concatenate([high, tile - high], axis=0)
        lam_pair[slot // 2, :, cols] = jnp.where(row_no % 8 == 0, both, 0.0).astype(jnp.bfloat16)

    for b in range(S):
        put_lambda(b, lam_exp[m * S + b, d])
    for t in range(T):
        tile = jnp.zeros((8, C), jnp.float32)
        for way in range(2):
            q = lax.rem((r - (t // P + 1) if way == 0 else r + (t // P + 1)) + 2 * N, N)
            q_m = jnp.where(q < D, 0, 1)
            q_d = jnp.where(q < D, q, N - 1 - q)
            p = t % P if way == 0 else P - 1 - t % P
            for b in range(S):
                place = b * 2 + way
                values = lam_exp[q_m * S + b, q_d]
                if place != p:
                    values = pltpu.roll(values, ((place - p) * PR) % C, 1)
                tile = jnp.where(lane_no == place, values, tile)
        put_lambda(S + t, tile)

    first = pl.multiple_of(me * rows, LANES)
    chunk = min(H, 256)

    def gradient(u, begin):
        at = (xs[u, :, pl.ds(first, rows)].astype(jnp.float32).T * lam_row[u, 0:1, :]).astype(
            jnp.bfloat16
        )
        pair = lam_pair[u]
        for c in range(0, H, chunk):
            cols = slice(c, c + chunk)
            grad = jnp.dot(at, slope[u, :, cols], preferred_element_type=jnp.float32)
            top = jnp.dot(pair, hid[u, :, cols], preferred_element_type=jnp.float32)
            if begin:
                w1g_ref[:, cols] = grad
                wtot[:, cols] = top
            else:
                w1g_ref[:, cols] += grad
                wtot[:, cols] += top

    gradient(0, True)
    relay(late)
    step_forward(late - 1)
    gradient(1, False)
    done = (S + T) // 2 - 1
    behind = late + 1 - (done - (T - 2 - late))
    for u in range(2, late + 1 - behind):
        gradient(u, False)

    def full_step(t, carry):
        relay(t)
        step_forward(t - 1)
        gradient(t - behind, False)
        return carry

    lax.fori_loop(late + 1, T - 1, full_step, 0)
    relay(T - 1)
    step_forward(T - 2)
    step_forward(T - 1)
    gradient(done, False)
    w1g_ref[...] = w1g_ref[...] * w2
    w2g_ref[...] = jnp.sum(wtot[...], axis=0, keepdims=True)

    own_twin.wait_send()
    for k in range(1, D):
        info_copy(k).wait_send()
    for a, b in lane_steps:
        lam_copy(a, b).wait_send()

    def drain(t, carry):
        ahead_copy(part(S + t, s, 0), t).wait_send()
        behind_copy(part(S + t, s, 1), t).wait_send()
        twin_copy(S + t, s).wait_send()
        return carry

    lax.fori_loop(0, T, drain, 0)


def ring_call(sizes, operands):
    D, M, S, C, E, H, rows, P = sizes
    L, N = M * S, D * M
    T = P * (N - 1) // 2
    f32, bf16 = jnp.float32, jnp.bfloat16
    vmem = pl.BlockSpec(memory_space=pltpu.VMEM)
    hbm = pl.BlockSpec(memory_space=pl.ANY)
    dma = pltpu.SemaphoreType.DMA
    slots = S + T
    crossing = max(min(2 * (D - 1 - i), 2 * i) + 1 for i in range(D))
    stages = max(D - 1, crossing + 1) - 1
    scratch = [
        pltpu.VMEM((E, H), bf16),
        pltpu.VMEM((slots // 2, 2 * C, E), bf16),
        pltpu.VMEM((slots // 2, 2 * C, H), bf16),
        pltpu.VMEM((slots // 2, 2 * C, H), bf16),
        pltpu.VMEM((3, 1, C), jnp.int32),
        pltpu.VMEM((1, H), f32),
        pltpu.VMEM((C, E), f32),
        pltpu.VMEM((16, H), f32),
        pltpu.VMEM((D, 8, C), f32),
        pltpu.VMEM((D, 8, C), f32),
        pltpu.VMEM((D, 8, C), f32),
        pltpu.VMEM((L, 8, C), f32),
        pltpu.VMEM((L, D, 8, C), f32),
        pltpu.VMEM((slots // 2, 8, 2 * C), f32),
        pltpu.VMEM((slots // 2, 16, 2 * C), bf16),
        dma((6,)),
        dma((T,)), dma((T,)), dma((T,)), dma((T,)),
        dma((slots,)), dma((slots,)),
        dma((D,)), dma((D,)),
        dma((L,)), dma((L,)),
        pltpu.SemaphoreType.REGULAR((stages,)),
    ]
    return pl.pallas_call(
        functools.partial(ring_kernel, sizes),
        out_shape=(
            pltpu.VMEM((C, E), bf16),
            pltpu.VMEM((rows, H), f32),
            pltpu.VMEM((1, H), f32),
        ),
        in_specs=[hbm] * 6,
        out_specs=(vmem, vmem, vmem),
        scratch_shapes=scratch,
        compiler_params=pltpu.CompilerParams(
            collective_id=0, has_side_effects=True, vmem_limit_bytes=56 * 1024 * 1024
        ),
    )(*operands)


def write_out(a_ref, b_ref, c_ref, a_out, b_out, c_out, sem):
    pairs = ((b_ref, b_out), (a_ref, a_out), (c_ref, c_out))
    copies = [pltpu.make_async_copy(x, y, sem.at[i]) for i, (x, y) in enumerate(pairs)]
    for copy in copies:
        copy.start()
    for copy in copies:
        copy.wait()


def reduce_call(sizes, operands):
    D, M, S, C, E, H, rows = sizes
    L = M * S
    width = max(rows, LANES)
    Kc = 4
    Kr = max(1, rows // 32)
    K = Kc * Kr
    f32, bf16 = jnp.float32, jnp.bfloat16
    vmem = pl.BlockSpec(memory_space=pltpu.VMEM)
    hbm = pl.BlockSpec(memory_space=pl.ANY)
    dma = pltpu.SemaphoreType.DMA
    chunk = (K, rows // Kr, H // Kc)
    scratch = [
        pltpu.VMEM((E, H), bf16),
        pltpu.VMEM((L * C, E), bf16),
        pltpu.VMEM((L * C, H), f32),
        pltpu.VMEM((L * C, H), f32),
        pltpu.VMEM((L * C, H), bf16),
        pltpu.VMEM((width, L * C), bf16),
        pltpu.VMEM((Kc, width, H // Kc), f32),
        pltpu.VMEM((D, 8, C), f32),
        pltpu.VMEM((D, 8, C), f32),
        pltpu.VMEM((D, 8, C), f32),
        pltpu.VMEM((D, 8, C), f32),
        pltpu.VMEM((L, 8, C), f32),
        pltpu.VMEM((D, H // LANES, LANES), f32),
        pltpu.VMEM(chunk, bf16),
        pltpu.VMEM(chunk, bf16),
        pltpu.VMEM(chunk, bf16),
        pltpu.VMEM(chunk, bf16),
        dma((2,)),
        dma((L,)), dma((L,)),
        dma((D,)), dma((D,)),
        dma((D,)), dma((D,)),
        dma((L,)), dma((L,)),
        dma((D,)), dma((D,)),
        dma((K,)), dma((K,)), dma((K,)), dma((K,)),
    ]
    return pl.pallas_call(
        functools.partial(kernel, (D, M, S, C, E, H, rows, Kc, Kr)),
        out_shape=(
            pltpu.VMEM((C, E), bf16),
            pltpu.VMEM((rows, H), f32),
            pltpu.VMEM((1, H), f32),
        ),
        in_specs=[hbm, hbm, vmem, vmem, vmem, vmem],
        out_specs=(vmem, vmem, vmem),
        scratch_shapes=scratch,
        compiler_params=pltpu.CompilerParams(
            collective_id=0, has_side_effects=True, vmem_limit_bytes=56 * 1024 * 1024
        ),
    )(*operands)


def on_device(embeddings, owner_shard, query_local, labels, w_first, w_second):
    D, M, S = lax.axis_size("docs"), lax.axis_size("mp"), lax.axis_size("sub")
    C, E = embeddings.shape
    H = w_first.shape[1]
    L = M * S
    rows = E // L
    vmem = pl.BlockSpec(memory_space=pltpu.VMEM)
    hbm = pl.BlockSpec(memory_space=pl.ANY)
    dma = pltpu.SemaphoreType.DMA
    operands = (
        embeddings, w_first, owner_shard.reshape(1, C), query_local.reshape(1, C),
        labels.reshape(1, C), w_second.reshape(1, H),
    )
    P = 2 * S
    held = D * L * C * (E + 2 * H) * 2
    gathers = (
        M == 2 and S == 2 and D > 1 and C == LANES and rows % LANES == 0 and held <= 32 * 2**20
    )
    if gathers:
        outs = ring_call((D, M, S, C, E, H, rows, P), operands)
    else:
        outs = reduce_call((D, M, S, C, E, H, rows), operands)
    emb_grad, w1g, w2g = outs
    emb_grad, w1g, w2g = pl.pallas_call(
        write_out,
        out_shape=tuple(jax.ShapeDtypeStruct(v.shape, v.dtype) for v in (emb_grad, w1g, w2g)),
        in_specs=[vmem] * 3,
        out_specs=(hbm,) * 3,
        scratch_shapes=[dma((3,))],
        compiler_params=pltpu.CompilerParams(vmem_limit_bytes=4 * 1024 * 1024),
    )(emb_grad, w1g, w2g)
    return emb_grad, w1g, w2g.reshape(H)


def solution(mesh):
    return jax.shard_map(
        on_device,
        mesh=mesh,
        in_specs=(
            P(("groups", "docs", "mp", "sub"), None),
            P(("groups", "docs", "mp", "sub"), None),
            P(("groups", "docs", "mp", "sub")),
            P(("groups", "docs", "mp", "sub")),
            P(),
            P(),
        ),
        out_specs=(
            P(("groups", "docs", "mp", "sub"), None),
            P(("groups", "mp", "sub"), None),
            P("groups"),
        ),
        check_vma=False,
    )
```

```python
import functools

import jax
import jax.numpy as jnp
from jax import lax
from jax.experimental import pallas as pl
from jax.experimental.pallas import tpu as pltpu
from jax.sharding import PartitionSpec as P

MESH = pl.DeviceIdType.MESH
LANES = 128
LOG2E = 1.4426950408889634


def log2(v):
    return jnp.log(v) * LOG2E


def across(row, rows):
    return jnp.broadcast_to(row, (rows, row.shape[1])).T


def row_tile(column):
    return jnp.broadcast_to(column, (column.shape[0], LANES)).T[0:8, :]


def kernel(
    sizes,
    emb_hbm, w1_hbm, owner_ref, local_ref, labels_ref, w2_ref,
    emb_grad_ref, w1g_ref, w2g_ref,
    w1v, embs, slope, hid, pg, at, wacc,
    minfo, sinfo, term, drow, lam, w2p,
    part, from_out, from_in, tot,
    load_sem, emb_send, emb_recv, m_send, m_recv, s_send, s_recv,
    l_send, l_recv, g_send, g_recv, in_send, out_send, fo_recv, fi_recv,
):
    D, M, S, C, E, H, rows, Kc, Kr = sizes
    L = M * S
    K = Kc * Kr
    d, m, s = lax.axis_index("docs"), lax.axis_index("mp"), lax.axis_index("sub")
    me = m * S + s

    load_w = pltpu.make_async_copy(w1_hbm, w1v, load_sem.at[0])
    load_e = pltpu.make_async_copy(emb_hbm, embs.at[pl.ds(me * C, C)], load_sem.at[1])
    load_e.start()
    load_w.start()

    def doc_peer(k):
        return lax.rem(d + k, D)

    def mp_peer(k):
        return lax.rem(m + k, M)

    def sub_peer(k):
        return lax.rem(s + k, S)

    lane_steps = [(a, b) for a in range(M) for b in range(S) if a or b]

    barrier = pltpu.get_barrier_semaphore()
    for k in range(1, D):
        pl.semaphore_signal(barrier, inc=1, device_id={"docs": doc_peer(k)}, device_id_type=MESH)
    for a, b in lane_steps:
        pl.semaphore_signal(
            barrier, inc=1, device_id={"mp": mp_peer(a), "sub": sub_peer(b)}, device_id_type=MESH
        )

    lab_own = labels_ref[...].astype(jnp.float32)
    q_own = (owner_ref[...] * 1024 + local_ref[...]).astype(jnp.float32)
    minfo[d, 0:1, :] = lab_own
    minfo[d, 1:2, :] = q_own

    pl.semaphore_wait(barrier, D - 1 + L - 1)

    def doc_send(buf, k, send, recv):
        return pltpu.make_async_remote_copy(
            src_ref=buf.at[d], dst_ref=buf.at[d], send_sem=send.at[k], recv_sem=recv.at[k],
            device_id={"docs": doc_peer(k)}, device_id_type=MESH,
        )

    load_e.wait()

    def emb_copy(lane, a, b, index):
        block = embs.at[pl.ds(lane * C, C)]
        return pltpu.make_async_remote_copy(
            src_ref=block, dst_ref=block, send_sem=emb_send.at[index], recv_sem=emb_recv.at[index],
            device_id={"mp": mp_peer(a), "sub": sub_peer(b)}, device_id_type=MESH,
        )

    for a in range(1, M):
        emb_copy(me, a, 0, a * S).start()
    for b in range(1, S):
        emb_copy(me, 0, b, b).start()
    for k in range(1, D):
        doc_send(minfo, k, m_send, m_recv).start()

    w2 = w2_ref[...]

    def forward(lane):
        at_rows = pl.ds(lane * C, C)
        act = jnp.dot(embs[at_rows, :], w1v[...], preferred_element_type=jnp.float32)
        sg = jax.nn.sigmoid(act)
        hidden = act * sg
        hid[at_rows, :] = hidden
        slope[at_rows, :] = w2 * (sg * (1.0 + act * (1.0 - sg)))
        return hidden

    load_w.wait()
    hidden = forward(me)
    sinfo[d] = row_tile(jnp.sum(hidden * w2, axis=1, keepdims=True))
    for k in range(1, D):
        doc_send(sinfo, k, s_send, s_recv).start()

    def lane_from(a, b):
        return lax.rem(m + M - a, M) * S + lax.rem(s + S - b, S)

    def recv_wait(a, b):
        emb_copy(lane_from(a, b), a, b, a * S + b).wait_recv()

    for b in range(1, S):
        recv_wait(0, b)
        forward(lane_from(0, b))

    for k in range(1, D):
        doc_send(minfo, k, m_send, m_recv).wait_recv()
    slot = lax.broadcasted_iota(jnp.int32, (1, C), 1).astype(jnp.float32)
    total = float(D * C)

    def key_of(label_row, dd):
        return label_row * total - (slot + lax.convert_element_type(dd * C, jnp.float32))

    def ideal_step(jd, carry):
        q_j = across(minfo[jd, 1:2, :], C)
        key_j = across(key_of(minfo[jd, 0:1, :], jd), C)
        out = []
        for i in range(D):
            ahead = (q_j == minfo[i, 1:2, :]) & (key_j > key_of(minfo[i, 0:1, :], i))
            out.append(carry[i] + jnp.sum(jnp.where(ahead, 1.0, 0.0), axis=0, keepdims=True))
        return tuple(out)

    zeros = tuple(jnp.zeros((1, C), jnp.float32) for _ in range(D))
    ideal = lax.fori_loop(0, D, ideal_step, zeros)
    for i in range(D):
        gain = jnp.exp2(minfo[i, 0:1, :]) - 1.0
        term[i, 0:1, :] = gain / log2(2.0 + ideal[i])
    q_i = across(q_own, C)
    gain_i = across(jnp.exp2(lab_own) - 1.0, C)
    idcg = jnp.zeros((C, C), jnp.float32)
    for j in range(D):
        idcg = idcg + jnp.where(q_i == minfo[j, 1:2, :], term[j, 0:1, :], 0.0)
    idcg = jnp.sum(idcg, axis=1, keepdims=True)
    inv = jnp.where(idcg > 0.0, 1.0 / jnp.where(idcg > 0.0, idcg, 1.0), 0.0)

    for k in range(1, D):
        doc_send(sinfo, k, s_send, s_recv).wait_recv()

    def soft_step(jd, carry):
        q_j = across(minfo[jd, 1:2, :], C)
        s_j = across(sinfo[jd, 0:1, :], C)
        out = []
        for i in range(D):
            part_of = jnp.where(
                q_j == minfo[i, 1:2, :], jax.nn.sigmoid(s_j - sinfo[i, 0:1, :]), 0.0
            )
            out.append(carry[i] + jnp.sum(part_of, axis=0, keepdims=True))
        return tuple(out)

    soft = lax.fori_loop(0, D, soft_step, zeros)
    for i in range(D):
        drow[i, 0:1, :] = 1.0 / log2(2.0 + (soft[i] - 0.5))
    disc_i = across(drow[d, 0:1, :], C)
    s_i = across(sinfo[d, 0:1, :], C)

    def lambda_step(j, acc):
        gain_j = jnp.exp2(minfo[j, 0:1, :]) - 1.0
        gap = s_i - sinfo[j, 0:1, :]
        weight = (gain_j - gain_i) * jnp.abs(disc_i - drow[j, 0:1, :])
        push = jax.nn.sigmoid(jnp.where(gain_i > gain_j, -gap, gap))
        return acc + jnp.where(q_i == minfo[j, 1:2, :], weight * push, 0.0)

    lam_acc = lax.fori_loop(0, D, lambda_step, jnp.zeros((C, C), jnp.float32))
    lam_col = jnp.sum(lam_acc, axis=1, keepdims=True) * inv
    lam[me] = row_tile(lam_col)

    def lam_copy(lane, a, b):
        return pltpu.make_async_remote_copy(
            src_ref=lam.at[lane], dst_ref=lam.at[lane],
            send_sem=l_send.at[a * S + b], recv_sem=l_recv.at[a * S + b],
            device_id={"mp": mp_peer(a), "sub": sub_peer(b)}, device_id_type=MESH,
        )

    for a, b in lane_steps:
        lam_copy(me, a, b).start()

    def scale(lane, column):
        at_rows = pl.ds(lane * C, C)
        pg[at_rows, :] = (column * slope[at_rows, :]).astype(jnp.bfloat16)

    scale(me, lam_col)
    emb_grad_ref[...] = lax.dot_general(
        pg[pl.ds(me * C, C), :], w1v[...], (((1,), (1,)), ((), ())),
        preferred_element_type=jnp.float32,
    ).astype(jnp.bfloat16)
    for a in range(1, M):
        recv_wait(a, 0)
        for b in range(1, S):
            emb_copy(lane_from(a, 0), 0, b, a * S + b).start()
        forward(lane_from(a, 0))
    for a in range(1, M):
        for b in range(1, S):
            recv_wait(a, b)
            forward(lane_from(a, b))
    width = at.shape[0]
    first = pl.multiple_of((me * rows) // LANES * LANES, LANES)
    for lane in range(L):
        at[:, pl.ds(lane * C, C)] = embs[pl.ds(lane * C, C), pl.ds(first, width)].T

    for a, b in lane_steps:
        lam_copy(lane_from(a, b), a, b).wait_recv()
        lane = lane_from(a, b)
        scale(lane, across(lam[lane, 0:1, :], C)[:, 0:1])

    half = D // 2
    left = d < half
    inward = jnp.where(left, d + 1, d - 1)
    outward = jnp.where(left, d - 1, d + 1)
    place = jnp.where(left, d, D - 1 - d)
    has_out = place > 0
    middle = place == half - 1
    cw, rh = H // Kc, rows // Kr

    def send_in(k, to_middle):
        dst, sem = (from_in, fi_recv) if to_middle else (from_out, fo_recv)
        return pltpu.make_async_remote_copy(
            src_ref=part.at[k], dst_ref=dst.at[k], send_sem=in_send.at[k], recv_sem=sem.at[k],
            device_id={"docs": inward}, device_id_type=MESH,
        )

    def send_out(k, from_total):
        src = tot if from_total else from_in
        return pltpu.make_async_remote_copy(
            src_ref=src.at[k], dst_ref=from_in.at[k], send_sem=out_send.at[k],
            recv_sem=fi_recv.at[k], device_id={"docs": outward}, device_id_type=MESH,
        )

    def start_in(k):
        pl.when(middle)(lambda: send_in(k, True).start())
        if half > 1:
            pl.when(jnp.logical_not(middle))(lambda: send_in(k, False).start())

    shift = me * rows - first
    for c in range(Kc):
        wide = jnp.dot(at[...], pg[:, c * cw : (c + 1) * cw], preferred_element_type=jnp.float32)
        wacc[c] = wide
        for r in range(Kr):
            k = c * Kr + r

            @pl.when(jnp.logical_not(has_out))
            def _():
                part[k] = wacc[c, pl.ds(pl.multiple_of(shift + r * rh, 8), rh), :].astype(
                    jnp.bfloat16
                )
                start_in(k)

    w2_part = jnp.zeros((1, H), jnp.float32)
    for lane in range(L):
        column = across(lam[lane, 0:1, :], C)[:, 0:1]
        w2_part = w2_part + jnp.sum(column * hid[pl.ds(lane * C, C), :], axis=0, keepdims=True)
    for j in range(H // LANES):
        w2p[d, j : j + 1, :] = w2_part[:, j * LANES : (j + 1) * LANES]
    for k in range(1, D):
        doc_send(w2p, k, g_send, g_recv).start()

    def gather_step(k):
        c, r = k // Kr, k % Kr

        @pl.when(has_out)
        def _():
            send_in(k, False).wait_recv()
            own = wacc[c, pl.ds(pl.multiple_of(shift + r * rh, 8), rh), :]
            part[k] = (own + from_out[k].astype(jnp.float32)).astype(jnp.bfloat16)
            start_in(k)

    def finish_step(k):
        c, r = k // Kr, k % Kr
        send_out(k, False).wait_recv()
        spot = (slice(r * rh, (r + 1) * rh), slice(c * cw, (c + 1) * cw))

        @pl.when(middle)
        def _():
            both = (part[k].astype(jnp.float32) + from_in[k].astype(jnp.float32)).astype(
                jnp.bfloat16
            )
            w1g_ref[spot] = both.astype(jnp.float32)
            if half > 1:
                tot[k] = both
                pl.when(has_out)(lambda: send_out(k, True).start())

        if half > 1:

            @pl.when(jnp.logical_not(middle))
            def _():
                pl.when(has_out)(lambda: send_out(k, False).start())
                w1g_ref[spot] = from_in[k].astype(jnp.float32)

    lag = max(1, K // 4)
    for k in range(lag):
        gather_step(k)
    for k in range(lag, K + lag):
        if k < K:
            gather_step(k)
        finish_step(k - lag)

    for k in range(1, D):
        doc_send(w2p, k, g_send, g_recv).wait_recv()
    w2_sum = w2p[0]
    for j in range(1, D):
        w2_sum = w2_sum + w2p[j]
    for j in range(H // LANES):
        w2g_ref[0:1, j * LANES : (j + 1) * LANES] = w2_sum[j : j + 1, :]

    for k in range(1, D):
        doc_send(minfo, k, m_send, m_recv).wait_send()
        doc_send(sinfo, k, s_send, s_recv).wait_send()
        doc_send(w2p, k, g_send, g_recv).wait_send()
    for a, b in lane_steps:
        emb_copy(me, a, b, a * S + b).wait_send()
        lam_copy(me, a, b).wait_send()
    for k in range(K):
        send_in(k, True).wait_send()
    for k in range(K):
        pl.when(has_out)(lambda k=k: send_out(k, False).wait_send())

def ring_kernel(
    sizes,
    emb_hbm, w1_hbm, owner_hbm, local_hbm, labels_hbm, w2_hbm,
    emb_grad_ref, w1g_ref, wtot, at_end, pair_end, slope_end, hid_end, w2v,
    w1v, xs, slope, hid, small, pre,
    info, term, drow, lam_all, lam_exp, lam_row, lam_pair,
    load_sem, ring_recv, twin_recv, own_sem, info_sem, lam_sem, send_sem, stage_sem,
):
    D, M, S, C, E, H, rows, P = sizes
    N = D * M
    PR = C // P
    T = P * (N - 1) // 2
    d, m, s = lax.axis_index("docs"), lax.axis_index("mp"), lax.axis_index("sub")
    me = m * S + s
    other = S - 1 - s
    r = jnp.where(m == 0, d, N - 1 - d)

    def ring_at(q):
        q = lax.rem(q + 2 * N, N)
        return {"docs": jnp.where(q < D, q, N - 1 - q), "mp": jnp.where(q < D, 0, 1)}

    ahead_id, behind_id, twin_id = ring_at(r + 1), ring_at(r - 1), {"sub": other}

    def spot(slot):
        return lax.div(slot, 2), pl.multiple_of(lax.rem(slot, 2) * C, C)

    def block(slot):
        u, row = spot(slot)
        return xs.at[u, pl.ds(row, C)]

    load_e = pltpu.make_async_copy(emb_hbm, block(s), load_sem.at[0])
    load_w = pltpu.make_async_copy(w1_hbm, w1v, load_sem.at[1])
    load_small = [
        pltpu.make_async_copy(owner_hbm, small.at[0], load_sem.at[2]),
        pltpu.make_async_copy(local_hbm, small.at[1], load_sem.at[3]),
        pltpu.make_async_copy(labels_hbm, small.at[2], load_sem.at[4]),
        pltpu.make_async_copy(w2_hbm, w2v, load_sem.at[5]),
    ]
    barrier = pltpu.get_barrier_semaphore()
    for peer in (ahead_id, behind_id, twin_id):
        pl.semaphore_signal(barrier, inc=1, device_id=peer, device_id_type=MESH)
    load_e.start()
    load_w.start()
    for copy in load_small:
        copy.start()

    def remote(src, dst, send, recv, peer):
        return pltpu.make_async_remote_copy(
            src_ref=src, dst_ref=dst, send_sem=send, recv_sem=recv,
            device_id=peer, device_id_type=MESH,
        )

    def part(slot, lane_s, way):
        return block(slot).at[pl.ds((lane_s * 2 + way) * PR, PR)]

    def ahead_copy(src, t):
        return remote(src, part(S + t, s, 0), send_sem.at[0], ring_recv.at[t], ahead_id)

    def behind_copy(src, t):
        return remote(src, part(S + t, s, 1), send_sem.at[0], ring_recv.at[t], behind_id)

    def both_ways(slot, lane_s):
        return block(slot).at[pl.ds(lane_s * 2 * PR, 2 * PR)]

    def ring_wait(t):
        both = both_ways(S + t, s)
        remote(both, both, send_sem.at[0], ring_recv.at[t], ahead_id).wait_recv()

    def twin_copy(t, lane_s):
        both = both_ways(S + t, lane_s)
        return remote(both, both, send_sem.at[0], twin_recv.at[t], twin_id)

    own_twin = remote(block(s), block(s), own_sem.at[0], own_sem.at[1], twin_id)

    def next_stage(k):
        for peer in (ahead_id, behind_id):
            pl.semaphore_signal(stage_sem.at[k], inc=1, device_id=peer, device_id_type=MESH)

    def stage_wait(k):
        pl.semaphore_wait(stage_sem.at[k], 2)

    pl.semaphore_wait(barrier, 3)
    load_e.wait()
    def send_own(p):
        ahead_copy(block(s).at[pl.ds(p * PR, PR)], p).start()
        behind_copy(block(s).at[pl.ds((P - 1 - p) * PR, PR)], p).start()

    for p in range(P - 1):
        send_own(p)
    own_twin.start()
    stages = stage_sem.shape[0]
    next_stage(0)

    for copy in load_small:
        copy.wait()
    load_w.wait()
    w2 = w2v[...]

    ends = (S + T) // 2 - 1

    def forward(slot):
        u, row = spot(slot)
        act = jnp.dot(xs[u, pl.ds(row, C), :], w1v[...], preferred_element_type=jnp.float32)
        sg = 0.5 + 0.5 * jnp.tanh(0.5 * act)
        hidden = act * sg
        bend = sg + hidden * (1.0 - sg)
        if isinstance(slot, int) and slot // 2 == ends:
            hid_end[pl.ds(slot % 2 * C, C), :] = hidden.astype(jnp.bfloat16)
            slope_end[pl.ds(slot % 2 * C, C), :] = bend.astype(jnp.bfloat16)
        else:
            hid[u, pl.ds(row, C), :] = hidden.astype(jnp.bfloat16)
            slope[u, pl.ds(row, C), :] = bend.astype(jnp.bfloat16)
        return hidden, bend

    hidden, bend = forward(s)
    info[d] = row_tile(jnp.sum(hidden * w2, axis=1, keepdims=True))
    info[d, 1:2, :] = small[2].astype(jnp.float32)
    info[d, 2:3, :] = (small[0] * 1024 + small[1]).astype(jnp.float32)
    stage_wait(0)
    if stages > 1:
        next_stage(1)
    pre[...] = lax.dot_general(
        (bend * w2).astype(jnp.bfloat16), w1v[...], (((1,), (1,)), ((), ())),
        preferred_element_type=jnp.float32,
    )
    def doc_peer(k):
        return lax.rem(d + k, D)

    def info_copy(k):
        return remote(
            info.at[d], info.at[d], info_sem.at[0], info_sem.at[1], {"docs": doc_peer(k)}
        )

    lane_steps = [(a, b) for a in range(M) for b in range(S) if a or b]

    def lam_copy(a, b):
        peer = {"mp": lax.rem(m + a, M), "sub": lax.rem(s + b, S)}
        return remote(lam_all.at[me], lam_all.at[me], lam_sem.at[0], lam_sem.at[1], peer)

    infos, lams = info.at[pl.ds(0, D - 1)], lam_all.at[pl.ds(0, M * S - 1)]
    info_both = remote(infos, infos, info_sem.at[0], info_sem.at[1], twin_id)
    lam_both = remote(lams, lams, lam_sem.at[0], lam_sem.at[1], twin_id)

    reach = min(stages, max(1, D - 2))
    for k in range(2, reach + 1):
        stage_wait(k - 1)
        if k < stages:
            next_stage(k)
    for k in range(1, D):
        info_copy(k).start()
    send_own(P - 1)
    own_twin.wait_recv()
    forward(other)

    def relay(t):
        ring_wait(t)

        @pl.when(t + P < T)
        def _():
            ahead_copy(part(S + t, s, 0), t + P).start()
            behind_copy(part(S + t, s, 1), t + P).start()

        twin_copy(t, s).start()

    def step_forward(t):
        twin_copy(t, other).wait_recv()
        forward(S + t)

    def relay_forward(lag, t, carry):
        relay(t)
        step_forward(t - lag)
        return carry

    early, late = T // 4 + 1, T // 2 + 1
    relay(0)
    lax.fori_loop(1, early, functools.partial(relay_forward, 1), 0)

    info_both.wait_recv()
    slot_of = lax.broadcasted_iota(jnp.int32, (1, C), 1).astype(jnp.float32)
    total = float(D * C)

    def key_of(jd):
        return info[jd, 1:2, :] * total - (slot_of + lax.convert_element_type(jd * C, jnp.float32))

    def rank_step(jd, carry):
        q_j = across(info[jd, 2:3, :], C)
        s_j = across(info[jd, 0:1, :], C)
        key_j = across(key_of(jd), C)
        out = []
        for i in range(D):
            same = q_j == info[i, 2:3, :]
            push = 0.5 + 0.5 * jnp.tanh(0.5 * (s_j - info[i, 0:1, :]))
            ahead = same & (key_j > key_of(i))
            out.append(carry[i] + jnp.sum(jnp.where(same, push, 0.0), axis=0, keepdims=True))
            out.append(carry[D + i] + jnp.sum(jnp.where(ahead, 1.0, 0.0), axis=0, keepdims=True))
        return tuple(out[0::2] + out[1::2])

    zeros = tuple(jnp.zeros((1, C), jnp.float32) for _ in range(2 * D))
    ranks = lax.fori_loop(0, D, rank_step, zeros)
    for i in range(D):
        gain = jnp.exp2(info[i, 1:2, :]) - 1.0
        term[i, 0:1, :] = gain / log2(2.0 + ranks[D + i])
        drow[i, 0:1, :] = 1.0 / log2(2.0 + (ranks[i] - 0.5))

    relay(early)

    def lambda_step(jd, carry):
        q_j = across(info[jd, 2:3, :], C)
        s_j = across(info[jd, 0:1, :], C)
        gain_j = across(jnp.exp2(info[jd, 1:2, :]) - 1.0, C)
        disc_j = across(drow[jd, 0:1, :], C)
        term_j = across(term[jd, 0:1, :], C)
        out = []
        for i in range(D):
            same = q_j == info[i, 2:3, :]
            gain_i = jnp.exp2(info[i, 1:2, :]) - 1.0
            gap = info[i, 0:1, :] - s_j
            weight = (gain_j - gain_i) * jnp.abs(drow[i, 0:1, :] - disc_j)
            push = 0.5 + 0.5 * jnp.tanh(0.5 * jnp.where(gain_i > gain_j, -gap, gap))
            out.append(
                carry[i] + jnp.sum(jnp.where(same, weight * push, 0.0), axis=0, keepdims=True)
            )
            out.append(
                carry[D + i] + jnp.sum(jnp.where(same, term_j, 0.0), axis=0, keepdims=True)
            )
        return tuple(out[0::2] + out[1::2])

    sums = lax.fori_loop(0, D, lambda_step, zeros)
    for i in range(D):
        idcg = sums[D + i]
        inv = jnp.where(idcg > 0.0, 1.0 / jnp.where(idcg > 0.0, idcg, 1.0), 0.0)
        lam_all[me, i : i + 1, :] = sums[i] * inv
    for k in range(reach + 1, stages + 1):
        stage_wait(k - 1)
        if k < stages:
            next_stage(k)
    for a, b in lane_steps:
        lam_copy(a, b).start()

    for i in range(D):
        lam_exp[me, i] = jnp.broadcast_to(lam_all[me, i : i + 1, :], (8, C))
    emb_grad_ref[...] = (pre[...] * across(lam_exp[me, d, 0:1, :], C)[:, 0:1]).astype(jnp.bfloat16)

    lax.fori_loop(early + 1, late, functools.partial(relay_forward, 2), 0)
    step_forward(late - 2)

    lam_both.wait_recv()
    for a, b in lane_steps:
        lane = lax.rem(m + M - a, M) * S + lax.rem(s + S - b, S)
        for i in range(D):
            lam_exp[lane, i] = jnp.broadcast_to(lam_all[lane, i : i + 1, :], (8, C))

    lane_no = lax.broadcasted_iota(jnp.int32, (8, C), 1) // PR
    row_no = lax.broadcasted_iota(jnp.int32, (16, C), 0)

    def put_lambda(slot, tile):
        cols = slice(slot % 2 * C, slot % 2 * C + C)
        lam_row[slot // 2, :, cols] = tile
        high = tile.astype(jnp.bfloat16).astype(jnp.float32)
        both = jnp.concatenate([high, tile - high], axis=0)
        lam_pair[slot // 2, :, cols] = jnp.where(row_no % 8 == 0, both, 0.0).astype(jnp.bfloat16)

    for b in range(S):
        put_lambda(b, lam_exp[m * S + b, d])
    for t in range(T):
        tile = jnp.zeros((8, C), jnp.float32)
        for way in range(2):
            q = lax.rem((r - (t // P + 1) if way == 0 else r + (t // P + 1)) + 2 * N, N)
            q_m = jnp.where(q < D, 0, 1)
            q_d = jnp.where(q < D, q, N - 1 - q)
            p = t % P if way == 0 else P - 1 - t % P
            for b in range(S):
                place = b * 2 + way
                values = lam_exp[q_m * S + b, q_d]
                if place != p:
                    values = pltpu.roll(values, ((place - p) * PR) % C, 1)
                tile = jnp.where(lane_no == place, values, tile)
        put_lambda(S + t, tile)

    first = pl.multiple_of(me * rows, LANES)
    chunk = min(H, 256)

    def turned(u):
        return (xs[u, :, pl.ds(first, rows)].astype(jnp.float32).T * lam_row[u, 0:1, :]).astype(
            jnp.bfloat16
        )

    def gradient(u, begin):
        at = turned(u)
        pair = lam_pair[u]
        for c in range(0, H, chunk):
            cols = slice(c, c + chunk)
            grad = jnp.dot(at, slope[u, :, cols], preferred_element_type=jnp.float32)
            top = jnp.dot(pair, hid[u, :, cols], preferred_element_type=jnp.float32)
            if begin:
                w1g_ref[:, cols] = grad
                wtot[:, cols] = top
            else:
                w1g_ref[:, cols] += grad
                wtot[:, cols] += top

    gradient(0, True)
    relay(late)
    step_forward(late - 1)
    gradient(1, False)
    behind = late + 1 - (ends - (T - 2 - late))
    for u in range(2, late + 1 - behind):
        gradient(u, False)

    def full_step(t, carry):
        relay(t)
        step_forward(t - 1)
        gradient(t - behind, False)
        return carry

    lax.fori_loop(late + 1, T - 2, full_step, 0)
    relay(T - 2)
    step_forward(T - 3)
    relay(T - 1)
    gradient(T - 2 - behind, False)
    step_forward(T - 2)
    pair_end[...] = lam_pair[ends]
    own_twin.wait_send()
    info_both.wait_send()
    lam_both.wait_send()
    step_forward(T - 1)
    at_end[...] = turned(ends)
    sent = xs.at[pl.ds(0, T // 2)]
    remote(sent, sent, send_sem.at[0], ring_recv.at[0], twin_id).wait_send()


def ring_call(sizes, operands):
    D, M, S, C, E, H, rows, P = sizes
    L, N = M * S, D * M
    T = P * (N - 1) // 2
    f32, bf16 = jnp.float32, jnp.bfloat16
    vmem = pl.BlockSpec(memory_space=pltpu.VMEM)
    hbm = pl.BlockSpec(memory_space=pl.ANY)
    dma = pltpu.SemaphoreType.DMA
    slots = S + T
    crossing = max(min(2 * (D - 1 - i), 2 * i) + 1 for i in range(D))
    stages = max(D - 1, crossing + 1) - 1
    scratch = [
        pltpu.VMEM((E, H), bf16),
        pltpu.VMEM((slots // 2, 2 * C, E), bf16),
        pltpu.VMEM((slots // 2, 2 * C, H), bf16),
        pltpu.VMEM((slots // 2, 2 * C, H), bf16),
        pltpu.VMEM((3, 1, C), jnp.int32),
        pltpu.VMEM((C, E), f32),
        pltpu.VMEM((D, 8, C), f32),
        pltpu.VMEM((D, 8, C), f32),
        pltpu.VMEM((D, 8, C), f32),
        pltpu.VMEM((L, 8, C), f32),
        pltpu.VMEM((L, D, 8, C), f32),
        pltpu.VMEM((slots // 2, 8, 2 * C), f32),
        pltpu.VMEM((slots // 2, 16, 2 * C), bf16),
        dma((6,)), dma((T,)), dma((T,)), dma((2,)), dma((2,)), dma((2,)), dma((1,)),
        pltpu.SemaphoreType.REGULAR((stages,)),
    ]
    held = pl.pallas_call(
        functools.partial(ring_kernel, sizes),
        out_shape=(
            pltpu.VMEM((C, E), bf16),
            pltpu.VMEM((rows, H), f32),
            pltpu.VMEM((16, H), f32),
            pltpu.VMEM((rows, 2 * C), bf16),
            pltpu.VMEM((16, 2 * C), bf16),
            pltpu.VMEM((2 * C, H), bf16),
            pltpu.VMEM((2 * C, H), bf16),
            pltpu.VMEM((1, H), f32),
        ),
        in_specs=[hbm] * 6,
        out_specs=(vmem,) * 8,
        scratch_shapes=scratch,
        compiler_params=pltpu.CompilerParams(
            collective_id=0, has_side_effects=True, vmem_limit_bytes=56 * 1024 * 1024
        ),
    )(*operands)
    return pl.pallas_call(
        finish,
        out_shape=(
            jax.ShapeDtypeStruct((C, E), bf16),
            jax.ShapeDtypeStruct((rows, H), f32),
            jax.ShapeDtypeStruct((1, H), f32),
        ),
        in_specs=[vmem] * 8,
        out_specs=(hbm,) * 3,
        scratch_shapes=[pltpu.VMEM((rows, H), f32), pltpu.VMEM((1, H), f32), dma((6,))],
        compiler_params=pltpu.CompilerParams(vmem_limit_bytes=4 * 1024 * 1024),
    )(*held)


def finish(
    emb_grad, w1g, wtot, at, pair, slope, hid, w2, emb_out, w1g_out, w2g_out, w1g_end, w2g_end, sem
):
    H = w2.shape[1]
    parts = 4
    wide = H // parts
    copies = [pltpu.make_async_copy(emb_grad, emb_out, sem.at[0])]
    copies[0].start()
    for c in range(parts):
        cols = slice(c * wide, (c + 1) * wide)
        if c == parts - 1:
            top = wtot[...] + jnp.dot(pair[...], hid[...], preferred_element_type=jnp.float32)
            w2g_end[...] = jnp.sum(top, axis=0, keepdims=True)
            copies.append(pltpu.make_async_copy(w2g_end, w2g_out, sem.at[1]))
            copies[-1].start()
        grad = jnp.dot(at[...], slope[:, cols], preferred_element_type=jnp.float32)
        w1g_end[:, cols] = (w1g[:, cols] + grad) * w2[:, cols]
        copies.append(
            pltpu.make_async_copy(w1g_end.at[:, cols], w1g_out.at[:, cols], sem.at[2 + c])
        )
        copies[-1].start()
    for copy in copies:
        copy.wait()


def write_out(a_ref, b_ref, c_ref, a_out, b_out, c_out, sem):
    pairs = ((b_ref, b_out), (a_ref, a_out), (c_ref, c_out))
    copies = [pltpu.make_async_copy(x, y, sem.at[i]) for i, (x, y) in enumerate(pairs)]
    for copy in copies:
        copy.start()
    for copy in copies:
        copy.wait()


def reduce_call(sizes, operands):
    D, M, S, C, E, H, rows = sizes
    L = M * S
    width = max(rows, LANES)
    Kc = 4
    Kr = max(1, rows // 32)
    K = Kc * Kr
    f32, bf16 = jnp.float32, jnp.bfloat16
    vmem = pl.BlockSpec(memory_space=pltpu.VMEM)
    hbm = pl.BlockSpec(memory_space=pl.ANY)
    dma = pltpu.SemaphoreType.DMA
    chunk = (K, rows // Kr, H // Kc)
    scratch = [
        pltpu.VMEM((E, H), bf16),
        pltpu.VMEM((L * C, E), bf16),
        pltpu.VMEM((L * C, H), f32),
        pltpu.VMEM((L * C, H), f32),
        pltpu.VMEM((L * C, H), bf16),
        pltpu.VMEM((width, L * C), bf16),
        pltpu.VMEM((Kc, width, H // Kc), f32),
        pltpu.VMEM((D, 8, C), f32),
        pltpu.VMEM((D, 8, C), f32),
        pltpu.VMEM((D, 8, C), f32),
        pltpu.VMEM((D, 8, C), f32),
        pltpu.VMEM((L, 8, C), f32),
        pltpu.VMEM((D, H // LANES, LANES), f32),
        pltpu.VMEM(chunk, bf16),
        pltpu.VMEM(chunk, bf16),
        pltpu.VMEM(chunk, bf16),
        pltpu.VMEM(chunk, bf16),
        dma((2,)),
        dma((L,)), dma((L,)),
        dma((D,)), dma((D,)),
        dma((D,)), dma((D,)),
        dma((L,)), dma((L,)),
        dma((D,)), dma((D,)),
        dma((K,)), dma((K,)), dma((K,)), dma((K,)),
    ]
    return pl.pallas_call(
        functools.partial(kernel, (D, M, S, C, E, H, rows, Kc, Kr)),
        out_shape=(
            pltpu.VMEM((C, E), bf16),
            pltpu.VMEM((rows, H), f32),
            pltpu.VMEM((1, H), f32),
        ),
        in_specs=[hbm, hbm, vmem, vmem, vmem, vmem],
        out_specs=(vmem, vmem, vmem),
        scratch_shapes=scratch,
        compiler_params=pltpu.CompilerParams(
            collective_id=0, has_side_effects=True, vmem_limit_bytes=56 * 1024 * 1024
        ),
    )(*operands)


def on_device(embeddings, owner_shard, query_local, labels, w_first, w_second):
    D, M, S = lax.axis_size("docs"), lax.axis_size("mp"), lax.axis_size("sub")
    C, E = embeddings.shape
    H = w_first.shape[1]
    L = M * S
    rows = E // L
    vmem = pl.BlockSpec(memory_space=pltpu.VMEM)
    hbm = pl.BlockSpec(memory_space=pl.ANY)
    dma = pltpu.SemaphoreType.DMA
    operands = (
        embeddings, w_first, owner_shard.reshape(1, C), query_local.reshape(1, C),
        labels.reshape(1, C), w_second.reshape(1, H),
    )
    P = 2 * S
    held = D * L * C * (E + 2 * H) * 2
    gathers = (
        M == 2 and S == 2 and D > 1 and C == LANES and rows % LANES == 0 and held <= 32 * 2**20
    )
    if gathers:
        emb_grad, w1g, w2g = ring_call((D, M, S, C, E, H, rows, P), operands)
        return emb_grad, w1g, w2g.reshape(H)
    emb_grad, w1g, w2g = reduce_call((D, M, S, C, E, H, rows), operands)
    emb_grad, w1g, w2g = pl.pallas_call(
        write_out,
        out_shape=tuple(jax.ShapeDtypeStruct(v.shape, v.dtype) for v in (emb_grad, w1g, w2g)),
        in_specs=[vmem] * 3,
        out_specs=(hbm,) * 3,
        scratch_shapes=[dma((3,))],
        compiler_params=pltpu.CompilerParams(vmem_limit_bytes=4 * 1024 * 1024),
    )(emb_grad, w1g, w2g)
    return emb_grad, w1g, w2g.reshape(H)


def solution(mesh):
    return jax.shard_map(
        on_device,
        mesh=mesh,
        in_specs=(
            P(("groups", "docs", "mp", "sub"), None),
            P(("groups", "docs", "mp", "sub"), None),
            P(("groups", "docs", "mp", "sub")),
            P(("groups", "docs", "mp", "sub")),
            P(),
            P(),
        ),
        out_specs=(
            P(("groups", "docs", "mp", "sub"), None),
            P(("groups", "mp", "sub"), None),
            P("groups"),
        ),
        check_vma=False,
    )
```

```python
import functools

import jax
import jax.numpy as jnp
from jax import lax
from jax.experimental import pallas as pl
from jax.experimental.pallas import tpu as pltpu
from jax.sharding import PartitionSpec as P

MESH = pl.DeviceIdType.MESH
LANES = 128
LOG2E = 1.4426950408889634


def log2(v):
    return jnp.log(v) * LOG2E


def across(row, rows):
    return jnp.broadcast_to(row, (rows, row.shape[1])).T


def row_tile(column):
    return jnp.broadcast_to(column, (column.shape[0], LANES)).T[0:8, :]


def kernel(
    sizes,
    emb_hbm, w1_hbm, owner_ref, local_ref, labels_ref, w2_ref,
    emb_grad_ref, w1g_ref, w2g_ref,
    w1v, embs, slope, hid, pg, at, wacc,
    minfo, sinfo, term, drow, lam, w2p,
    part, from_out, from_in, tot,
    load_sem, emb_send, emb_recv, m_send, m_recv, s_send, s_recv,
    l_send, l_recv, g_send, g_recv, in_send, out_send, fo_recv, fi_recv,
):
    D, M, S, C, E, H, rows, Kc, Kr = sizes
    L = M * S
    K = Kc * Kr
    d, m, s = lax.axis_index("docs"), lax.axis_index("mp"), lax.axis_index("sub")
    me = m * S + s

    load_w = pltpu.make_async_copy(w1_hbm, w1v, load_sem.at[0])
    load_e = pltpu.make_async_copy(emb_hbm, embs.at[pl.ds(me * C, C)], load_sem.at[1])
    load_e.start()
    load_w.start()

    def doc_peer(k):
        return lax.rem(d + k, D)

    def mp_peer(k):
        return lax.rem(m + k, M)

    def sub_peer(k):
        return lax.rem(s + k, S)

    lane_steps = [(a, b) for a in range(M) for b in range(S) if a or b]

    barrier = pltpu.get_barrier_semaphore()
    for k in range(1, D):
        pl.semaphore_signal(barrier, inc=1, device_id={"docs": doc_peer(k)}, device_id_type=MESH)
    for a, b in lane_steps:
        pl.semaphore_signal(
            barrier, inc=1, device_id={"mp": mp_peer(a), "sub": sub_peer(b)}, device_id_type=MESH
        )

    lab_own = labels_ref[...].astype(jnp.float32)
    q_own = (owner_ref[...] * 1024 + local_ref[...]).astype(jnp.float32)
    minfo[d, 0:1, :] = lab_own
    minfo[d, 1:2, :] = q_own

    pl.semaphore_wait(barrier, D - 1 + L - 1)

    def doc_send(buf, k, send, recv):
        return pltpu.make_async_remote_copy(
            src_ref=buf.at[d], dst_ref=buf.at[d], send_sem=send.at[k], recv_sem=recv.at[k],
            device_id={"docs": doc_peer(k)}, device_id_type=MESH,
        )

    load_e.wait()

    def emb_copy(lane, a, b, index):
        block = embs.at[pl.ds(lane * C, C)]
        return pltpu.make_async_remote_copy(
            src_ref=block, dst_ref=block, send_sem=emb_send.at[index], recv_sem=emb_recv.at[index],
            device_id={"mp": mp_peer(a), "sub": sub_peer(b)}, device_id_type=MESH,
        )

    for a in range(1, M):
        emb_copy(me, a, 0, a * S).start()
    for b in range(1, S):
        emb_copy(me, 0, b, b).start()
    for k in range(1, D):
        doc_send(minfo, k, m_send, m_recv).start()

    w2 = w2_ref[...]

    def forward(lane):
        at_rows = pl.ds(lane * C, C)
        act = jnp.dot(embs[at_rows, :], w1v[...], preferred_element_type=jnp.float32)
        sg = jax.nn.sigmoid(act)
        hidden = act * sg
        hid[at_rows, :] = hidden
        slope[at_rows, :] = w2 * (sg * (1.0 + act * (1.0 - sg)))
        return hidden

    load_w.wait()
    hidden = forward(me)
    sinfo[d] = row_tile(jnp.sum(hidden * w2, axis=1, keepdims=True))
    for k in range(1, D):
        doc_send(sinfo, k, s_send, s_recv).start()

    def lane_from(a, b):
        return lax.rem(m + M - a, M) * S + lax.rem(s + S - b, S)

    def recv_wait(a, b):
        emb_copy(lane_from(a, b), a, b, a * S + b).wait_recv()

    for b in range(1, S):
        recv_wait(0, b)
        forward(lane_from(0, b))

    for k in range(1, D):
        doc_send(minfo, k, m_send, m_recv).wait_recv()
    slot = lax.broadcasted_iota(jnp.int32, (1, C), 1).astype(jnp.float32)
    total = float(D * C)

    def key_of(label_row, dd):
        return label_row * total - (slot + lax.convert_element_type(dd * C, jnp.float32))

    def ideal_step(jd, carry):
        q_j = across(minfo[jd, 1:2, :], C)
        key_j = across(key_of(minfo[jd, 0:1, :], jd), C)
        out = []
        for i in range(D):
            ahead = (q_j == minfo[i, 1:2, :]) & (key_j > key_of(minfo[i, 0:1, :], i))
            out.append(carry[i] + jnp.sum(jnp.where(ahead, 1.0, 0.0), axis=0, keepdims=True))
        return tuple(out)

    zeros = tuple(jnp.zeros((1, C), jnp.float32) for _ in range(D))
    ideal = lax.fori_loop(0, D, ideal_step, zeros)
    for i in range(D):
        gain = jnp.exp2(minfo[i, 0:1, :]) - 1.0
        term[i, 0:1, :] = gain / log2(2.0 + ideal[i])
    q_i = across(q_own, C)
    gain_i = across(jnp.exp2(lab_own) - 1.0, C)
    idcg = jnp.zeros((C, C), jnp.float32)
    for j in range(D):
        idcg = idcg + jnp.where(q_i == minfo[j, 1:2, :], term[j, 0:1, :], 0.0)
    idcg = jnp.sum(idcg, axis=1, keepdims=True)
    inv = jnp.where(idcg > 0.0, 1.0 / jnp.where(idcg > 0.0, idcg, 1.0), 0.0)

    for k in range(1, D):
        doc_send(sinfo, k, s_send, s_recv).wait_recv()

    def soft_step(jd, carry):
        q_j = across(minfo[jd, 1:2, :], C)
        s_j = across(sinfo[jd, 0:1, :], C)
        out = []
        for i in range(D):
            part_of = jnp.where(
                q_j == minfo[i, 1:2, :], jax.nn.sigmoid(s_j - sinfo[i, 0:1, :]), 0.0
            )
            out.append(carry[i] + jnp.sum(part_of, axis=0, keepdims=True))
        return tuple(out)

    soft = lax.fori_loop(0, D, soft_step, zeros)
    for i in range(D):
        drow[i, 0:1, :] = 1.0 / log2(2.0 + (soft[i] - 0.5))
    disc_i = across(drow[d, 0:1, :], C)
    s_i = across(sinfo[d, 0:1, :], C)

    def lambda_step(j, acc):
        gain_j = jnp.exp2(minfo[j, 0:1, :]) - 1.0
        gap = s_i - sinfo[j, 0:1, :]
        weight = (gain_j - gain_i) * jnp.abs(disc_i - drow[j, 0:1, :])
        push = jax.nn.sigmoid(jnp.where(gain_i > gain_j, -gap, gap))
        return acc + jnp.where(q_i == minfo[j, 1:2, :], weight * push, 0.0)

    lam_acc = lax.fori_loop(0, D, lambda_step, jnp.zeros((C, C), jnp.float32))
    lam_col = jnp.sum(lam_acc, axis=1, keepdims=True) * inv
    lam[me] = row_tile(lam_col)

    def lam_copy(lane, a, b):
        return pltpu.make_async_remote_copy(
            src_ref=lam.at[lane], dst_ref=lam.at[lane],
            send_sem=l_send.at[a * S + b], recv_sem=l_recv.at[a * S + b],
            device_id={"mp": mp_peer(a), "sub": sub_peer(b)}, device_id_type=MESH,
        )

    for a, b in lane_steps:
        lam_copy(me, a, b).start()

    def scale(lane, column):
        at_rows = pl.ds(lane * C, C)
        pg[at_rows, :] = (column * slope[at_rows, :]).astype(jnp.bfloat16)

    scale(me, lam_col)
    emb_grad_ref[...] = lax.dot_general(
        pg[pl.ds(me * C, C), :], w1v[...], (((1,), (1,)), ((), ())),
        preferred_element_type=jnp.float32,
    ).astype(jnp.bfloat16)
    for a in range(1, M):
        recv_wait(a, 0)
        for b in range(1, S):
            emb_copy(lane_from(a, 0), 0, b, a * S + b).start()
        forward(lane_from(a, 0))
    for a in range(1, M):
        for b in range(1, S):
            recv_wait(a, b)
            forward(lane_from(a, b))
    width = at.shape[0]
    first = pl.multiple_of((me * rows) // LANES * LANES, LANES)
    for lane in range(L):
        at[:, pl.ds(lane * C, C)] = embs[pl.ds(lane * C, C), pl.ds(first, width)].T

    for a, b in lane_steps:
        lam_copy(lane_from(a, b), a, b).wait_recv()
        lane = lane_from(a, b)
        scale(lane, across(lam[lane, 0:1, :], C)[:, 0:1])

    half = D // 2
    left = d < half
    inward = jnp.where(left, d + 1, d - 1)
    outward = jnp.where(left, d - 1, d + 1)
    place = jnp.where(left, d, D - 1 - d)
    has_out = place > 0
    middle = place == half - 1
    cw, rh = H // Kc, rows // Kr

    def send_in(k, to_middle):
        dst, sem = (from_in, fi_recv) if to_middle else (from_out, fo_recv)
        return pltpu.make_async_remote_copy(
            src_ref=part.at[k], dst_ref=dst.at[k], send_sem=in_send.at[k], recv_sem=sem.at[k],
            device_id={"docs": inward}, device_id_type=MESH,
        )

    def send_out(k, from_total):
        src = tot if from_total else from_in
        return pltpu.make_async_remote_copy(
            src_ref=src.at[k], dst_ref=from_in.at[k], send_sem=out_send.at[k],
            recv_sem=fi_recv.at[k], device_id={"docs": outward}, device_id_type=MESH,
        )

    def start_in(k):
        pl.when(middle)(lambda: send_in(k, True).start())
        if half > 1:
            pl.when(jnp.logical_not(middle))(lambda: send_in(k, False).start())

    shift = me * rows - first
    for c in range(Kc):
        wide = jnp.dot(at[...], pg[:, c * cw : (c + 1) * cw], preferred_element_type=jnp.float32)
        wacc[c] = wide
        for r in range(Kr):
            k = c * Kr + r

            @pl.when(jnp.logical_not(has_out))
            def _():
                part[k] = wacc[c, pl.ds(pl.multiple_of(shift + r * rh, 8), rh), :].astype(
                    jnp.bfloat16
                )
                start_in(k)

    w2_part = jnp.zeros((1, H), jnp.float32)
    for lane in range(L):
        column = across(lam[lane, 0:1, :], C)[:, 0:1]
        w2_part = w2_part + jnp.sum(column * hid[pl.ds(lane * C, C), :], axis=0, keepdims=True)
    for j in range(H // LANES):
        w2p[d, j : j + 1, :] = w2_part[:, j * LANES : (j + 1) * LANES]
    for k in range(1, D):
        doc_send(w2p, k, g_send, g_recv).start()

    def gather_step(k):
        c, r = k // Kr, k % Kr

        @pl.when(has_out)
        def _():
            send_in(k, False).wait_recv()
            own = wacc[c, pl.ds(pl.multiple_of(shift + r * rh, 8), rh), :]
            part[k] = (own + from_out[k].astype(jnp.float32)).astype(jnp.bfloat16)
            start_in(k)

    def finish_step(k):
        c, r = k // Kr, k % Kr
        send_out(k, False).wait_recv()
        spot = (slice(r * rh, (r + 1) * rh), slice(c * cw, (c + 1) * cw))

        @pl.when(middle)
        def _():
            both = (part[k].astype(jnp.float32) + from_in[k].astype(jnp.float32)).astype(
                jnp.bfloat16
            )
            w1g_ref[spot] = both.astype(jnp.float32)
            if half > 1:
                tot[k] = both
                pl.when(has_out)(lambda: send_out(k, True).start())

        if half > 1:

            @pl.when(jnp.logical_not(middle))
            def _():
                pl.when(has_out)(lambda: send_out(k, False).start())
                w1g_ref[spot] = from_in[k].astype(jnp.float32)

    lag = max(1, K // 4)
    for k in range(lag):
        gather_step(k)
    for k in range(lag, K + lag):
        if k < K:
            gather_step(k)
        finish_step(k - lag)

    for k in range(1, D):
        doc_send(w2p, k, g_send, g_recv).wait_recv()
    w2_sum = w2p[0]
    for j in range(1, D):
        w2_sum = w2_sum + w2p[j]
    for j in range(H // LANES):
        w2g_ref[0:1, j * LANES : (j + 1) * LANES] = w2_sum[j : j + 1, :]

    for k in range(1, D):
        doc_send(minfo, k, m_send, m_recv).wait_send()
        doc_send(sinfo, k, s_send, s_recv).wait_send()
        doc_send(w2p, k, g_send, g_recv).wait_send()
    for a, b in lane_steps:
        emb_copy(me, a, b, a * S + b).wait_send()
        lam_copy(me, a, b).wait_send()
    for k in range(K):
        send_in(k, True).wait_send()
    for k in range(K):
        pl.when(has_out)(lambda k=k: send_out(k, False).wait_send())

LEAD = 2
PARTS = 4


def ring_kernel(
    sizes,
    emb_hbm, w1_hbm, owner_hbm, local_hbm, labels_hbm, w2_hbm,
    emb_grad_ref, w1g_ref, w2g_ref, at_end, slope_end, w2v,
    w1v, xs, slope, hid, small, pre, wtot,
    info, term, drow, lam_all, lam_exp, lam_row, lam_pair,
    load_sem, ring_recv, twin_recv, own_sem, info_sem, lam_sem, send_sem, stage_sem, up_sem,
):
    D, M, S, C, E, H, rows, P = sizes
    N = D * M
    PR = C // P
    T = P * (N - 1) // 2
    d, m, s = lax.axis_index("docs"), lax.axis_index("mp"), lax.axis_index("sub")
    me = m * S + s
    other = S - 1 - s
    r = jnp.where(m == 0, d, N - 1 - d)

    def ring_at(q):
        q = lax.rem(q + 2 * N, N)
        return {"docs": jnp.where(q < D, q, N - 1 - q), "mp": jnp.where(q < D, 0, 1)}

    ahead_id, behind_id, twin_id = ring_at(r + 1), ring_at(r - 1), {"sub": other}

    def spot(slot):
        return lax.div(slot, 2), pl.multiple_of(lax.rem(slot, 2) * C, C)

    def block(slot):
        u, row = spot(slot)
        return xs.at[u, pl.ds(row, C)]

    load_e = pltpu.make_async_copy(emb_hbm, block(s), load_sem.at[0])
    load_w = pltpu.make_async_copy(w1_hbm, w1v, load_sem.at[1])
    load_small = [
        pltpu.make_async_copy(owner_hbm, small.at[0], load_sem.at[2]),
        pltpu.make_async_copy(local_hbm, small.at[1], load_sem.at[3]),
        pltpu.make_async_copy(labels_hbm, small.at[2], load_sem.at[4]),
        pltpu.make_async_copy(w2_hbm, w2v, load_sem.at[5]),
    ]
    barrier = pltpu.get_barrier_semaphore()

    def flows(act):
        def of(first, second):
            pl.when(m == 0)(lambda: act(*first))
            pl.when(m > 0)(lambda: act(*second))

        return of

    @flows
    def hello_up(peer):
        pl.semaphore_signal(barrier, inc=1, device_id=peer, device_id_type=MESH)

    pl.semaphore_signal(barrier, inc=1, device_id=twin_id, device_id_type=MESH)
    hello_up((ahead_id,), (behind_id,))

    @pl.when((d == 0) | (d == D - 1))
    def _():
        hello_up((behind_id,), (ahead_id,))

    load_e.start()
    load_w.start()
    for copy in load_small:
        copy.start()

    def remote(src, dst, send, recv, peer):
        return pltpu.make_async_remote_copy(
            src_ref=src, dst_ref=dst, send_sem=send, recv_sem=recv,
            device_id=peer, device_id_type=MESH,
        )

    def part(slot, lane_s, way):
        return block(slot).at[pl.ds((lane_s * 2 + way) * PR, PR)]

    def ahead_copy(src, t):
        return remote(src, part(S + t, s, 0), send_sem.at[0], ring_recv.at[t], ahead_id)

    def behind_copy(src, t):
        return remote(src, part(S + t, s, 1), send_sem.at[0], ring_recv.at[t], behind_id)

    def both_ways(slot, lane_s):
        return block(slot).at[pl.ds(lane_s * 2 * PR, 2 * PR)]

    def ring_wait(t):
        both = both_ways(S + t, s)
        remote(both, both, send_sem.at[0], ring_recv.at[t], ahead_id).wait_recv()

    def twin_copy(t, lane_s):
        both = both_ways(S + t, lane_s)
        return remote(both, both, send_sem.at[0], twin_recv.at[t], twin_id)

    own_twin = remote(block(s), block(s), own_sem.at[0], own_sem.at[1], twin_id)

    def next_stage(k):
        for peer in (ahead_id, behind_id):
            pl.semaphore_signal(stage_sem.at[k], inc=1, device_id=peer, device_id_type=MESH)

    def stage_wait(k):
        pl.semaphore_wait(stage_sem.at[k], 2)

    def send_ahead(p):
        ahead_copy(block(s).at[pl.ds(p * PR, PR)], p).start()

    def send_behind(p):
        behind_copy(block(s).at[pl.ds((P - 1 - p) * PR, PR)], p).start()

    def send_both(p):
        send_ahead(p)
        send_behind(p)

    @flows
    def send_first(send):
        for p in range(P - 1):
            send(p)

    @flows
    def answer(peer):
        pl.semaphore_signal(up_sem.at[0], inc=1, device_id=peer, device_id_type=MESH)

    pl.semaphore_wait(barrier, jnp.where(d >= D - 2, 3, 2))

    @pl.when((d > 0) & (d < D - 1))
    def _():
        answer((behind_id,), (ahead_id,))

    load_e.wait()
    send_first((send_behind,), (send_ahead,))
    own_twin.start()

    @pl.when(d < D - 2)
    def _():
        pl.semaphore_wait(up_sem.at[0], 1)

    send_first((send_ahead,), (send_behind,))
    stages = stage_sem.shape[0]
    next_stage(0)

    for copy in load_small:
        copy.wait()
    load_w.wait()
    w2 = w2v[...]

    ends = (S + T) // 2 - 1

    early, late = T // 4 + 1, T // 2 + 2
    direct = (S + late + 1) // 2

    def forward(slot):
        u, row = spot(slot)
        act = jnp.dot(xs[u, pl.ds(row, C), :], w1v[...], preferred_element_type=jnp.float32)
        sg = 0.5 + 0.5 * jnp.tanh(0.5 * act)
        hidden = act * sg
        bend = sg + hidden * (1.0 - sg)
        known = isinstance(slot, int)
        if known and slot // 2 == ends:
            slope_end[pl.ds(slot % 2 * C, C), :] = bend.astype(jnp.bfloat16)
        else:
            slope[u, pl.ds(row, C), :] = bend.astype(jnp.bfloat16)
        if known and slot // 2 >= direct:
            column = across(lam_row[slot // 2, 0:1, slot % 2 * C : slot % 2 * C + C], C)[:, 0:1]
            w2g_ref[...] += jnp.sum(hidden * column, axis=0, keepdims=True)
        else:
            hid[u, pl.ds(row, C), :] = hidden.astype(jnp.bfloat16)
        return hidden, bend

    hidden, bend = forward(s)
    info[d, 0] = row_tile(jnp.sum(hidden * w2, axis=1, keepdims=True))[0:1, :]
    info[d, 1] = small[2].astype(jnp.float32)
    info[d, 2] = (small[0] * 1024 + small[1]).astype(jnp.float32)
    stage_wait(0)
    if stages > 1:
        next_stage(1)
    pre[...] = lax.dot_general(
        (bend * w2).astype(jnp.bfloat16), w1v[...], (((1,), (1,)), ((), ())),
        preferred_element_type=jnp.float32,
    )
    def doc_peer(k):
        return lax.rem(d + k, D)

    def info_copy(k):
        return remote(
            info.at[d], info.at[d], info_sem.at[0], info_sem.at[1], {"docs": doc_peer(k)}
        )

    lane_steps = [(a, b) for a in range(M) for b in range(S) if a or b]

    def lam_copy(a, b):
        peer = {"mp": lax.rem(m + a, M), "sub": lax.rem(s + b, S)}
        return remote(lam_all.at[me], lam_all.at[me], lam_sem.at[0], lam_sem.at[1], peer)

    infos, lams = info.at[pl.ds(0, D - 1)], lam_all.at[pl.ds(0, M * S - 1)]
    info_both = remote(infos, infos, info_sem.at[0], info_sem.at[1], twin_id)
    lam_both = remote(lams, lams, lam_sem.at[0], lam_sem.at[1], twin_id)

    reach = min(stages, max(1, D - 2))
    for k in range(2, reach + 1):
        stage_wait(k - 1)
        if k < stages:
            next_stage(k)
    for k in range(1, D):
        info_copy(k).start()
    send_both(P - 1)
    own_twin.wait_recv()
    forward(other)

    def relay(t):
        ring_wait(t)

        @pl.when(t + P < T)
        def _():
            ahead_copy(part(S + t, s, 0), t + P).start()
            behind_copy(part(S + t, s, 1), t + P).start()

        twin_copy(t, s).start()

    def lead_relay(t):
        q = t + LEAD * s
        if isinstance(t, int) and t + LEAD * (S - 1) < T:
            relay(q)
        else:
            pl.when(q < T)(lambda: relay(q))

    def step_forward(t):
        twin_copy(t, other).wait_recv()
        forward(S + t)

    def relay_forward(t, carry):
        lead_relay(t)
        step_forward(t)
        return carry

    @pl.when(s > 0)
    def _():
        for t in range(LEAD):
            relay(t)

    lax.fori_loop(0, early, relay_forward, 0)

    info_both.wait_recv()
    slot_of = lax.broadcasted_iota(jnp.int32, (1, C), 1).astype(jnp.float32)
    total = float(D * C)

    def key_of(jd):
        return info[jd, 1] * total - (slot_of + lax.convert_element_type(jd * C, jnp.float32))

    def rank_step(jd, carry):
        q_j = across(info[jd, 2], C)
        s_j = across(info[jd, 0], C)
        key_j = across(key_of(jd), C)
        out = []
        for i in range(D):
            same = q_j == info[i, 2]
            push = 0.5 + 0.5 * jnp.tanh(0.5 * (s_j - info[i, 0]))
            ahead = same & (key_j > key_of(i))
            out.append(carry[i] + jnp.sum(jnp.where(same, push, 0.0), axis=0, keepdims=True))
            out.append(carry[D + i] + jnp.sum(jnp.where(ahead, 1.0, 0.0), axis=0, keepdims=True))
        return tuple(out[0::2] + out[1::2])

    zeros = tuple(jnp.zeros((1, C), jnp.float32) for _ in range(2 * D))
    ranks = lax.fori_loop(0, D, rank_step, zeros)
    for i in range(D):
        gain = jnp.exp2(info[i, 1]) - 1.0
        term[i, 0:1, :] = gain / log2(2.0 + ranks[D + i])
        drow[i, 0:1, :] = 1.0 / log2(2.0 + (ranks[i] - 0.5))

    pl.when(s == 0)(lambda: relay(early))

    def lambda_step(jd, carry):
        q_j = across(info[jd, 2], C)
        s_j = across(info[jd, 0], C)
        gain_j = across(jnp.exp2(info[jd, 1]) - 1.0, C)
        disc_j = across(drow[jd, 0:1, :], C)
        term_j = across(term[jd, 0:1, :], C)
        out = []
        for i in range(D):
            same = q_j == info[i, 2]
            gain_i = jnp.exp2(info[i, 1]) - 1.0
            gap = info[i, 0] - s_j
            weight = (gain_j - gain_i) * jnp.abs(drow[i, 0:1, :] - disc_j)
            push = 0.5 + 0.5 * jnp.tanh(0.5 * jnp.where(gain_i > gain_j, -gap, gap))
            out.append(
                carry[i] + jnp.sum(jnp.where(same, weight * push, 0.0), axis=0, keepdims=True)
            )
            out.append(
                carry[D + i] + jnp.sum(jnp.where(same, term_j, 0.0), axis=0, keepdims=True)
            )
        return tuple(out[0::2] + out[1::2])

    sums = lax.fori_loop(0, D, lambda_step, zeros)
    for i in range(D):
        idcg = sums[D + i]
        inv = jnp.where(idcg > 0.0, 1.0 / jnp.where(idcg > 0.0, idcg, 1.0), 0.0)
        lam_all[me, i] = sums[i] * inv
    for k in range(reach + 1, stages + 1):
        stage_wait(k - 1)
        if k < stages:
            next_stage(k)
    for a, b in lane_steps:
        lam_copy(a, b).start()

    for i in range(D):
        lam_exp[me, i] = jnp.broadcast_to(lam_all[me, i], (8, C))
    emb_grad_ref[...] = (pre[...] * across(lam_exp[me, d, 0:1, :], C)[:, 0:1]).astype(jnp.bfloat16)

    pl.when(s > 0)(lambda: relay(early + LEAD))
    lead_relay(early + 1)
    step_forward(early)
    step_forward(early + 1)
    lax.fori_loop(early + 2, late, relay_forward, 0)

    lam_both.wait_recv()
    for a, b in lane_steps:
        lane = lax.rem(m + M - a, M) * S + lax.rem(s + S - b, S)
        for i in range(D):
            lam_exp[lane, i] = jnp.broadcast_to(lam_all[lane, i], (8, C))

    lane_no = lax.broadcasted_iota(jnp.int32, (8, C), 1) // PR
    row_no = lax.broadcasted_iota(jnp.int32, (16, C), 0)

    def put_lambda(slot, tile):
        cols = slice(slot % 2 * C, slot % 2 * C + C)
        lam_row[slot // 2, :, cols] = tile
        high = tile.astype(jnp.bfloat16).astype(jnp.float32)
        both = jnp.concatenate([high, tile - high], axis=0)
        lam_pair[slot // 2, :, cols] = jnp.where(row_no % 8 == 0, both, 0.0).astype(jnp.bfloat16)

    for b in range(S):
        put_lambda(b, lam_exp[m * S + b, d])
    for t in range(T):
        tile = jnp.zeros((8, C), jnp.float32)
        for way in range(2):
            q = lax.rem((r - (t // P + 1) if way == 0 else r + (t // P + 1)) + 2 * N, N)
            q_m = jnp.where(q < D, 0, 1)
            q_d = jnp.where(q < D, q, N - 1 - q)
            p = t % P if way == 0 else P - 1 - t % P
            for b in range(S):
                place = b * 2 + way
                values = lam_exp[q_m * S + b, q_d]
                if place != p:
                    values = pltpu.roll(values, ((place - p) * PR) % C, 1)
                tile = jnp.where(lane_no == place, values, tile)
        put_lambda(S + t, tile)

    first = pl.multiple_of(me * rows, LANES)
    chunk = min(H, 256)

    def turned(u, begin=0, count=2 * C):
        values = xs[u, begin : begin + count, pl.ds(first, rows)].astype(jnp.float32)
        return (values.T * lam_row[u, 0:1, begin : begin + count]).astype(jnp.bfloat16)

    def gradient(u, begin):
        at = turned(u)
        pair = lam_pair[u] if u < direct else None
        for c in range(0, H, chunk):
            cols = slice(c, c + chunk)
            grad = jnp.dot(at, slope[u, :, cols], preferred_element_type=jnp.float32)
            w1g_ref[:, cols] = grad if begin else w1g_ref[:, cols] + grad
            if u < direct:
                top = jnp.dot(pair, hid[u, :, cols], preferred_element_type=jnp.float32)
                wtot[:, cols] = top if begin else wtot[:, cols] + top

    w2g_ref[...] = jnp.zeros(w2g_ref.shape, jnp.float32)
    gradient(0, True)
    left = list(range(1, ends))
    for t in range(late, T - 1):
        lead_relay(t)
        step_forward(t)
        if t < T - 2:
            ready = [u for u in left if 2 * u <= t + 1]
            for u in ready if t == T - 3 else ready[:2]:
                gradient(u, False)
                left.remove(u)
    for u in left:
        gradient(u, False)
    w2g_ref[...] += jnp.sum(wtot[...], axis=0, keepdims=True)
    lead_relay(T - 1)
    own_twin.wait_send()
    info_both.wait_send()
    lam_both.wait_send()
    at_end[:, 0:C] = turned(ends, 0, C)
    twin_copy(T - 1, other).wait_recv()
    at_end[:, C : 2 * C] = turned(ends, C, C)
    forward(S + T - 1)
    sent = xs.at[pl.ds(0, T // 2)]
    remote(sent, sent, send_sem.at[0], ring_recv.at[0], twin_id).wait_send()


def ring_call(sizes, operands):
    D, M, S, C, E, H, rows, P = sizes
    L, N = M * S, D * M
    T = P * (N - 1) // 2
    f32, bf16 = jnp.float32, jnp.bfloat16
    vmem = pl.BlockSpec(memory_space=pltpu.VMEM)
    hbm = pl.BlockSpec(memory_space=pl.ANY)
    dma = pltpu.SemaphoreType.DMA
    slots = S + T
    crossing = max(min(2 * (D - 1 - i), 2 * i) + 1 for i in range(D))
    stages = max(D - 1, crossing + 1) - 1
    scratch = [
        pltpu.VMEM((E, H), bf16),
        pltpu.VMEM((slots // 2, 2 * C, E), bf16),
        pltpu.VMEM((slots // 2, 2 * C, H), bf16),
        pltpu.VMEM((slots // 2, 2 * C, H), bf16),
        pltpu.VMEM((3, 1, C), jnp.int32),
        pltpu.VMEM((C, E), f32),
        pltpu.VMEM((16, H), f32),
        pltpu.VMEM((D, 3, 1, C), f32),
        pltpu.VMEM((D, 8, C), f32),
        pltpu.VMEM((D, 8, C), f32),
        pltpu.VMEM((L, D, 1, C), f32),
        pltpu.VMEM((L, D, 8, C), f32),
        pltpu.VMEM((slots // 2, 8, 2 * C), f32),
        pltpu.VMEM((slots // 2, 16, 2 * C), bf16),
        dma((6,)), dma((T,)), dma((T,)), dma((2,)), dma((2,)), dma((2,)), dma((1,)),
        pltpu.SemaphoreType.REGULAR((stages,)),
        pltpu.SemaphoreType.REGULAR((1,)),
    ]
    held = pl.pallas_call(
        functools.partial(ring_kernel, sizes),
        out_shape=(
            pltpu.VMEM((C, E), bf16),
            pltpu.VMEM((rows, H), f32),
            pltpu.VMEM((1, H), f32),
            pltpu.VMEM((rows, 2 * C), bf16),
            pltpu.VMEM((2 * C, H), bf16),
            pltpu.VMEM((1, H), f32),
        ),
        in_specs=[hbm] * 6,
        out_specs=(vmem,) * 6,
        scratch_shapes=scratch,
        compiler_params=pltpu.CompilerParams(
            collective_id=0, has_side_effects=True, vmem_limit_bytes=56 * 1024 * 1024
        ),
    )(*operands)
    return pl.pallas_call(
        finish,
        out_shape=(
            jax.ShapeDtypeStruct((C, E), bf16),
            jax.ShapeDtypeStruct((rows, H), f32),
            jax.ShapeDtypeStruct((1, H), f32),
        ),
        in_specs=[vmem] * 6,
        out_specs=(hbm,) * 3,
        scratch_shapes=[pltpu.VMEM((rows, H), f32), dma((2 + PARTS,))],
        compiler_params=pltpu.CompilerParams(vmem_limit_bytes=4 * 1024 * 1024),
    )(*held)


def finish(emb_grad, w1g, w2g, at, slope, w2, emb_out, w1g_out, w2g_out, w1g_end, sem):
    H = w2.shape[1]
    parts = PARTS
    wide = H // parts
    copies = [
        pltpu.make_async_copy(emb_grad, emb_out, sem.at[0]),
        pltpu.make_async_copy(w2g, w2g_out, sem.at[1]),
    ]
    for copy in copies:
        copy.start()
    for c in range(parts):
        cols = slice(c * wide, (c + 1) * wide)
        grad = jnp.dot(at[...], slope[:, cols], preferred_element_type=jnp.float32)
        w1g_end[:, cols] = (w1g[:, cols] + grad) * w2[:, cols]
        copies.append(
            pltpu.make_async_copy(w1g_end.at[:, cols], w1g_out.at[:, cols], sem.at[2 + c])
        )
        copies[-1].start()
    for copy in copies:
        copy.wait()


def write_out(a_ref, b_ref, c_ref, a_out, b_out, c_out, sem):
    pairs = ((b_ref, b_out), (a_ref, a_out), (c_ref, c_out))
    copies = [pltpu.make_async_copy(x, y, sem.at[i]) for i, (x, y) in enumerate(pairs)]
    for copy in copies:
        copy.start()
    for copy in copies:
        copy.wait()


def reduce_call(sizes, operands):
    D, M, S, C, E, H, rows = sizes
    L = M * S
    width = max(rows, LANES)
    Kc = 4
    Kr = max(1, rows // 32)
    K = Kc * Kr
    f32, bf16 = jnp.float32, jnp.bfloat16
    vmem = pl.BlockSpec(memory_space=pltpu.VMEM)
    hbm = pl.BlockSpec(memory_space=pl.ANY)
    dma = pltpu.SemaphoreType.DMA
    chunk = (K, rows // Kr, H // Kc)
    scratch = [
        pltpu.VMEM((E, H), bf16),
        pltpu.VMEM((L * C, E), bf16),
        pltpu.VMEM((L * C, H), f32),
        pltpu.VMEM((L * C, H), f32),
        pltpu.VMEM((L * C, H), bf16),
        pltpu.VMEM((width, L * C), bf16),
        pltpu.VMEM((Kc, width, H // Kc), f32),
        pltpu.VMEM((D, 8, C), f32),
        pltpu.VMEM((D, 8, C), f32),
        pltpu.VMEM((D, 8, C), f32),
        pltpu.VMEM((D, 8, C), f32),
        pltpu.VMEM((L, 8, C), f32),
        pltpu.VMEM((D, H // LANES, LANES), f32),
        pltpu.VMEM(chunk, bf16),
        pltpu.VMEM(chunk, bf16),
        pltpu.VMEM(chunk, bf16),
        pltpu.VMEM(chunk, bf16),
        dma((2,)),
        dma((L,)), dma((L,)),
        dma((D,)), dma((D,)),
        dma((D,)), dma((D,)),
        dma((L,)), dma((L,)),
        dma((D,)), dma((D,)),
        dma((K,)), dma((K,)), dma((K,)), dma((K,)),
    ]
    return pl.pallas_call(
        functools.partial(kernel, (D, M, S, C, E, H, rows, Kc, Kr)),
        out_shape=(
            pltpu.VMEM((C, E), bf16),
            pltpu.VMEM((rows, H), f32),
            pltpu.VMEM((1, H), f32),
        ),
        in_specs=[hbm, hbm, vmem, vmem, vmem, vmem],
        out_specs=(vmem, vmem, vmem),
        scratch_shapes=scratch,
        compiler_params=pltpu.CompilerParams(
            collective_id=0, has_side_effects=True, vmem_limit_bytes=56 * 1024 * 1024
        ),
    )(*operands)


def on_device(embeddings, owner_shard, query_local, labels, w_first, w_second):
    D, M, S = lax.axis_size("docs"), lax.axis_size("mp"), lax.axis_size("sub")
    C, E = embeddings.shape
    H = w_first.shape[1]
    L = M * S
    rows = E // L
    vmem = pl.BlockSpec(memory_space=pltpu.VMEM)
    hbm = pl.BlockSpec(memory_space=pl.ANY)
    dma = pltpu.SemaphoreType.DMA
    operands = (
        embeddings, w_first, owner_shard.reshape(1, C), query_local.reshape(1, C),
        labels.reshape(1, C), w_second.reshape(1, H),
    )
    P = 2 * S
    held = D * L * C * (E + 2 * H) * 2
    gathers = (
        M == 2 and S == 2 and D > 1 and C == LANES and rows % LANES == 0 and held <= 32 * 2**20
    )
    if gathers:
        emb_grad, w1g, w2g = ring_call((D, M, S, C, E, H, rows, P), operands)
        return emb_grad, w1g, w2g.reshape(H)
    emb_grad, w1g, w2g = reduce_call((D, M, S, C, E, H, rows), operands)
    emb_grad, w1g, w2g = pl.pallas_call(
        write_out,
        out_shape=tuple(jax.ShapeDtypeStruct(v.shape, v.dtype) for v in (emb_grad, w1g, w2g)),
        in_specs=[vmem] * 3,
        out_specs=(hbm,) * 3,
        scratch_shapes=[dma((3,))],
        compiler_params=pltpu.CompilerParams(vmem_limit_bytes=4 * 1024 * 1024),
    )(emb_grad, w1g, w2g)
    return emb_grad, w1g, w2g.reshape(H)


def solution(mesh):
    return jax.shard_map(
        on_device,
        mesh=mesh,
        in_specs=(
            P(("groups", "docs", "mp", "sub"), None),
            P(("groups", "docs", "mp", "sub"), None),
            P(("groups", "docs", "mp", "sub")),
            P(("groups", "docs", "mp", "sub")),
            P(),
            P(),
        ),
        out_specs=(
            P(("groups", "docs", "mp", "sub"), None),
            P(("groups", "mp", "sub"), None),
            P("groups"),
        ),
        check_vma=False,
    )
```

```python
import functools

import jax
import jax.numpy as jnp
from jax import lax
from jax.experimental import pallas as pl
from jax.experimental.pallas import tpu as pltpu
from jax.sharding import PartitionSpec as P

MESH = pl.DeviceIdType.MESH
LANES = 128
LOG2E = 1.4426950408889634


def log2(v):
    return jnp.log(v) * LOG2E


def across(row, rows):
    return jnp.broadcast_to(row, (rows, row.shape[1])).T


def row_tile(column):
    return jnp.broadcast_to(column, (column.shape[0], LANES)).T[0:8, :]


def kernel(
    sizes,
    emb_hbm, w1_hbm, owner_ref, local_ref, labels_ref, w2_ref,
    emb_grad_ref, w1g_ref, w2g_ref,
    w1v, embs, slope, hid, pg, at, wacc,
    minfo, sinfo, term, drow, lam, w2p,
    part, from_out, from_in, tot,
    load_sem, emb_send, emb_recv, m_send, m_recv, s_send, s_recv,
    l_send, l_recv, g_send, g_recv, in_send, out_send, fo_recv, fi_recv,
):
    D, M, S, C, E, H, rows, Kc, Kr = sizes
    L = M * S
    K = Kc * Kr
    d, m, s = lax.axis_index("docs"), lax.axis_index("mp"), lax.axis_index("sub")
    me = m * S + s

    load_w = pltpu.make_async_copy(w1_hbm, w1v, load_sem.at[0])
    load_e = pltpu.make_async_copy(emb_hbm, embs.at[pl.ds(me * C, C)], load_sem.at[1])
    load_e.start()
    load_w.start()

    def doc_peer(k):
        return lax.rem(d + k, D)

    def mp_peer(k):
        return lax.rem(m + k, M)

    def sub_peer(k):
        return lax.rem(s + k, S)

    lane_steps = [(a, b) for a in range(M) for b in range(S) if a or b]

    barrier = pltpu.get_barrier_semaphore()
    for k in range(1, D):
        pl.semaphore_signal(barrier, inc=1, device_id={"docs": doc_peer(k)}, device_id_type=MESH)
    for a, b in lane_steps:
        pl.semaphore_signal(
            barrier, inc=1, device_id={"mp": mp_peer(a), "sub": sub_peer(b)}, device_id_type=MESH
        )

    lab_own = labels_ref[...].astype(jnp.float32)
    q_own = (owner_ref[...] * 1024 + local_ref[...]).astype(jnp.float32)
    minfo[d, 0:1, :] = lab_own
    minfo[d, 1:2, :] = q_own

    pl.semaphore_wait(barrier, D - 1 + L - 1)

    def doc_send(buf, k, send, recv):
        return pltpu.make_async_remote_copy(
            src_ref=buf.at[d], dst_ref=buf.at[d], send_sem=send.at[k], recv_sem=recv.at[k],
            device_id={"docs": doc_peer(k)}, device_id_type=MESH,
        )

    load_e.wait()

    def emb_copy(lane, a, b, index):
        block = embs.at[pl.ds(lane * C, C)]
        return pltpu.make_async_remote_copy(
            src_ref=block, dst_ref=block, send_sem=emb_send.at[index], recv_sem=emb_recv.at[index],
            device_id={"mp": mp_peer(a), "sub": sub_peer(b)}, device_id_type=MESH,
        )

    for a in range(1, M):
        emb_copy(me, a, 0, a * S).start()
    for b in range(1, S):
        emb_copy(me, 0, b, b).start()
    for k in range(1, D):
        doc_send(minfo, k, m_send, m_recv).start()

    w2 = w2_ref[...]

    def forward(lane):
        at_rows = pl.ds(lane * C, C)
        act = jnp.dot(embs[at_rows, :], w1v[...], preferred_element_type=jnp.float32)
        sg = jax.nn.sigmoid(act)
        hidden = act * sg
        hid[at_rows, :] = hidden
        slope[at_rows, :] = w2 * (sg * (1.0 + act * (1.0 - sg)))
        return hidden

    load_w.wait()
    hidden = forward(me)
    sinfo[d] = row_tile(jnp.sum(hidden * w2, axis=1, keepdims=True))
    for k in range(1, D):
        doc_send(sinfo, k, s_send, s_recv).start()

    def lane_from(a, b):
        return lax.rem(m + M - a, M) * S + lax.rem(s + S - b, S)

    def recv_wait(a, b):
        emb_copy(lane_from(a, b), a, b, a * S + b).wait_recv()

    for b in range(1, S):
        recv_wait(0, b)
        forward(lane_from(0, b))

    for k in range(1, D):
        doc_send(minfo, k, m_send, m_recv).wait_recv()
    slot = lax.broadcasted_iota(jnp.int32, (1, C), 1).astype(jnp.float32)
    total = float(D * C)

    def key_of(label_row, dd):
        return label_row * total - (slot + lax.convert_element_type(dd * C, jnp.float32))

    def ideal_step(jd, carry):
        q_j = across(minfo[jd, 1:2, :], C)
        key_j = across(key_of(minfo[jd, 0:1, :], jd), C)
        out = []
        for i in range(D):
            ahead = (q_j == minfo[i, 1:2, :]) & (key_j > key_of(minfo[i, 0:1, :], i))
            out.append(carry[i] + jnp.sum(jnp.where(ahead, 1.0, 0.0), axis=0, keepdims=True))
        return tuple(out)

    zeros = tuple(jnp.zeros((1, C), jnp.float32) for _ in range(D))
    ideal = lax.fori_loop(0, D, ideal_step, zeros)
    for i in range(D):
        gain = jnp.exp2(minfo[i, 0:1, :]) - 1.0
        term[i, 0:1, :] = gain / log2(2.0 + ideal[i])
    q_i = across(q_own, C)
    gain_i = across(jnp.exp2(lab_own) - 1.0, C)
    idcg = jnp.zeros((C, C), jnp.float32)
    for j in range(D):
        idcg = idcg + jnp.where(q_i == minfo[j, 1:2, :], term[j, 0:1, :], 0.0)
    idcg = jnp.sum(idcg, axis=1, keepdims=True)
    inv = jnp.where(idcg > 0.0, 1.0 / jnp.where(idcg > 0.0, idcg, 1.0), 0.0)

    for k in range(1, D):
        doc_send(sinfo, k, s_send, s_recv).wait_recv()

    def soft_step(jd, carry):
        q_j = across(minfo[jd, 1:2, :], C)
        s_j = across(sinfo[jd, 0:1, :], C)
        out = []
        for i in range(D):
            part_of = jnp.where(
                q_j == minfo[i, 1:2, :], jax.nn.sigmoid(s_j - sinfo[i, 0:1, :]), 0.0
            )
            out.append(carry[i] + jnp.sum(part_of, axis=0, keepdims=True))
        return tuple(out)

    soft = lax.fori_loop(0, D, soft_step, zeros)
    for i in range(D):
        drow[i, 0:1, :] = 1.0 / log2(2.0 + (soft[i] - 0.5))
    disc_i = across(drow[d, 0:1, :], C)
    s_i = across(sinfo[d, 0:1, :], C)

    def lambda_step(j, acc):
        gain_j = jnp.exp2(minfo[j, 0:1, :]) - 1.0
        gap = s_i - sinfo[j, 0:1, :]
        weight = (gain_j - gain_i) * jnp.abs(disc_i - drow[j, 0:1, :])
        push = jax.nn.sigmoid(jnp.where(gain_i > gain_j, -gap, gap))
        return acc + jnp.where(q_i == minfo[j, 1:2, :], weight * push, 0.0)

    lam_acc = lax.fori_loop(0, D, lambda_step, jnp.zeros((C, C), jnp.float32))
    lam_col = jnp.sum(lam_acc, axis=1, keepdims=True) * inv
    lam[me] = row_tile(lam_col)

    def lam_copy(lane, a, b):
        return pltpu.make_async_remote_copy(
            src_ref=lam.at[lane], dst_ref=lam.at[lane],
            send_sem=l_send.at[a * S + b], recv_sem=l_recv.at[a * S + b],
            device_id={"mp": mp_peer(a), "sub": sub_peer(b)}, device_id_type=MESH,
        )

    for a, b in lane_steps:
        lam_copy(me, a, b).start()

    def scale(lane, column):
        at_rows = pl.ds(lane * C, C)
        pg[at_rows, :] = (column * slope[at_rows, :]).astype(jnp.bfloat16)

    scale(me, lam_col)
    emb_grad_ref[...] = lax.dot_general(
        pg[pl.ds(me * C, C), :], w1v[...], (((1,), (1,)), ((), ())),
        preferred_element_type=jnp.float32,
    ).astype(jnp.bfloat16)
    for a in range(1, M):
        recv_wait(a, 0)
        for b in range(1, S):
            emb_copy(lane_from(a, 0), 0, b, a * S + b).start()
        forward(lane_from(a, 0))
    for a in range(1, M):
        for b in range(1, S):
            recv_wait(a, b)
            forward(lane_from(a, b))
    width = at.shape[0]
    first = pl.multiple_of((me * rows) // LANES * LANES, LANES)
    for lane in range(L):
        at[:, pl.ds(lane * C, C)] = embs[pl.ds(lane * C, C), pl.ds(first, width)].T

    for a, b in lane_steps:
        lam_copy(lane_from(a, b), a, b).wait_recv()
        lane = lane_from(a, b)
        scale(lane, across(lam[lane, 0:1, :], C)[:, 0:1])

    half = D // 2
    left = d < half
    inward = jnp.where(left, d + 1, d - 1)
    outward = jnp.where(left, d - 1, d + 1)
    place = jnp.where(left, d, D - 1 - d)
    has_out = place > 0
    middle = place == half - 1
    cw, rh = H // Kc, rows // Kr

    def send_in(k, to_middle):
        dst, sem = (from_in, fi_recv) if to_middle else (from_out, fo_recv)
        return pltpu.make_async_remote_copy(
            src_ref=part.at[k], dst_ref=dst.at[k], send_sem=in_send.at[k], recv_sem=sem.at[k],
            device_id={"docs": inward}, device_id_type=MESH,
        )

    def send_out(k, from_total):
        src = tot if from_total else from_in
        return pltpu.make_async_remote_copy(
            src_ref=src.at[k], dst_ref=from_in.at[k], send_sem=out_send.at[k],
            recv_sem=fi_recv.at[k], device_id={"docs": outward}, device_id_type=MESH,
        )

    def start_in(k):
        pl.when(middle)(lambda: send_in(k, True).start())
        if half > 1:
            pl.when(jnp.logical_not(middle))(lambda: send_in(k, False).start())

    shift = me * rows - first
    for c in range(Kc):
        wide = jnp.dot(at[...], pg[:, c * cw : (c + 1) * cw], preferred_element_type=jnp.float32)
        wacc[c] = wide
        for r in range(Kr):
            k = c * Kr + r

            @pl.when(jnp.logical_not(has_out))
            def _():
                part[k] = wacc[c, pl.ds(pl.multiple_of(shift + r * rh, 8), rh), :].astype(
                    jnp.bfloat16
                )
                start_in(k)

    w2_part = jnp.zeros((1, H), jnp.float32)
    for lane in range(L):
        column = across(lam[lane, 0:1, :], C)[:, 0:1]
        w2_part = w2_part + jnp.sum(column * hid[pl.ds(lane * C, C), :], axis=0, keepdims=True)
    for j in range(H // LANES):
        w2p[d, j : j + 1, :] = w2_part[:, j * LANES : (j + 1) * LANES]
    for k in range(1, D):
        doc_send(w2p, k, g_send, g_recv).start()

    def gather_step(k):
        c, r = k // Kr, k % Kr

        @pl.when(has_out)
        def _():
            send_in(k, False).wait_recv()
            own = wacc[c, pl.ds(pl.multiple_of(shift + r * rh, 8), rh), :]
            part[k] = (own + from_out[k].astype(jnp.float32)).astype(jnp.bfloat16)
            start_in(k)

    def finish_step(k):
        c, r = k // Kr, k % Kr
        send_out(k, False).wait_recv()
        spot = (slice(r * rh, (r + 1) * rh), slice(c * cw, (c + 1) * cw))

        @pl.when(middle)
        def _():
            both = (part[k].astype(jnp.float32) + from_in[k].astype(jnp.float32)).astype(
                jnp.bfloat16
            )
            w1g_ref[spot] = both.astype(jnp.float32)
            if half > 1:
                tot[k] = both
                pl.when(has_out)(lambda: send_out(k, True).start())

        if half > 1:

            @pl.when(jnp.logical_not(middle))
            def _():
                pl.when(has_out)(lambda: send_out(k, False).start())
                w1g_ref[spot] = from_in[k].astype(jnp.float32)

    lag = max(1, K // 4)
    for k in range(lag):
        gather_step(k)
    for k in range(lag, K + lag):
        if k < K:
            gather_step(k)
        finish_step(k - lag)

    for k in range(1, D):
        doc_send(w2p, k, g_send, g_recv).wait_recv()
    w2_sum = w2p[0]
    for j in range(1, D):
        w2_sum = w2_sum + w2p[j]
    for j in range(H // LANES):
        w2g_ref[0:1, j * LANES : (j + 1) * LANES] = w2_sum[j : j + 1, :]

    for k in range(1, D):
        doc_send(minfo, k, m_send, m_recv).wait_send()
        doc_send(sinfo, k, s_send, s_recv).wait_send()
        doc_send(w2p, k, g_send, g_recv).wait_send()
    for a, b in lane_steps:
        emb_copy(me, a, b, a * S + b).wait_send()
        lam_copy(me, a, b).wait_send()
    for k in range(K):
        send_in(k, True).wait_send()
    for k in range(K):
        pl.when(has_out)(lambda k=k: send_out(k, False).wait_send())

LEAD = 2
PARTS = 4


def ring_kernel(
    sizes,
    emb_hbm, w1_hbm, owner_hbm, local_hbm, labels_hbm, w2_hbm,
    emb_grad_ref, w1g_ref, w2g_ref, at_end, slope_end, w2v,
    w1v, xs, slope, hid, small, pre, wtot,
    info, term, drow, lam_all, lam_exp, lam_row, lam_pair,
    load_sem, ring_recv, twin_recv, own_sem, info_sem, lam_sem, send_sem, stage_sem, up_sem,
):
    D, M, S, C, E, H, rows, P = sizes
    N = D * M
    PR = C // P
    T = P * (N - 1) // 2
    d, m, s = lax.axis_index("docs"), lax.axis_index("mp"), lax.axis_index("sub")
    me = m * S + s
    other = S - 1 - s
    r = jnp.where(m == 0, d, N - 1 - d)

    def ring_at(q):
        q = lax.rem(q + 2 * N, N)
        return {"docs": jnp.where(q < D, q, N - 1 - q), "mp": jnp.where(q < D, 0, 1)}

    ahead_id, behind_id, twin_id = ring_at(r + 1), ring_at(r - 1), {"sub": other}

    def spot(slot):
        return lax.div(slot, 2), pl.multiple_of(lax.rem(slot, 2) * C, C)

    def block(slot):
        return xs.at[pl.ds(pl.multiple_of(slot * C, C), C)]

    load_e = pltpu.make_async_copy(emb_hbm, block(s), load_sem.at[0])
    load_w = pltpu.make_async_copy(w1_hbm, w1v, load_sem.at[1])
    load_small = [
        pltpu.make_async_copy(owner_hbm, small.at[0], load_sem.at[2]),
        pltpu.make_async_copy(local_hbm, small.at[1], load_sem.at[3]),
        pltpu.make_async_copy(labels_hbm, small.at[2], load_sem.at[4]),
        pltpu.make_async_copy(w2_hbm, w2v, load_sem.at[5]),
    ]
    load_e.start()
    barrier = pltpu.get_barrier_semaphore()

    def flows(act):
        def of(first, second):
            pl.when(m == 0)(lambda: act(*first))
            pl.when(m > 0)(lambda: act(*second))

        return of

    @flows
    def hello_up(peer):
        pl.semaphore_signal(barrier, inc=1, device_id=peer, device_id_type=MESH)

    pl.semaphore_signal(barrier, inc=1, device_id=twin_id, device_id_type=MESH)
    hello_up((ahead_id,), (behind_id,))

    @pl.when((d == 0) | (d == D - 1))
    def _():
        hello_up((behind_id,), (ahead_id,))

    load_w.start()
    for copy in load_small:
        copy.start()

    def remote(src, dst, send, recv, peer):
        return pltpu.make_async_remote_copy(
            src_ref=src, dst_ref=dst, send_sem=send, recv_sem=recv,
            device_id=peer, device_id_type=MESH,
        )

    def part(slot, lane_s, way):
        return block(slot).at[pl.ds((lane_s * 2 + way) * PR, PR)]

    def ahead_copy(src, t):
        return remote(src, part(S + t, s, 0), send_sem.at[0], ring_recv.at[t], ahead_id)

    def behind_copy(src, t):
        return remote(src, part(S + t, s, 1), send_sem.at[0], ring_recv.at[t], behind_id)

    def both_ways(slot, lane_s):
        return block(slot).at[pl.ds(lane_s * 2 * PR, 2 * PR)]

    def ring_wait(t):
        both = both_ways(S + t, s)
        remote(both, both, send_sem.at[0], ring_recv.at[t], ahead_id).wait_recv()

    def twin_copy(t, lane_s):
        both = both_ways(S + t, lane_s)
        return remote(both, both, send_sem.at[0], twin_recv.at[t], twin_id)

    own_twin = remote(block(s), block(s), own_sem.at[0], own_sem.at[1], twin_id)

    def next_stage(k):
        for peer in (ahead_id, behind_id):
            pl.semaphore_signal(stage_sem.at[k], inc=1, device_id=peer, device_id_type=MESH)

    def stage_wait(k):
        pl.semaphore_wait(stage_sem.at[k], 2)

    def send_ahead(p):
        ahead_copy(block(s).at[pl.ds(p * PR, PR)], p).start()

    def send_behind(p):
        behind_copy(block(s).at[pl.ds((P - 1 - p) * PR, PR)], p).start()

    def send_both(p):
        send_ahead(p)
        send_behind(p)

    @flows
    def send_first(send):
        for p in range(P - 1):
            send(p)

    @flows
    def answer(peer):
        pl.semaphore_signal(up_sem.at[0], inc=1, device_id=peer, device_id_type=MESH)

    pl.semaphore_wait(barrier, jnp.where(d >= D - 2, 3, 2))

    @pl.when((d > 0) & (d < D - 1))
    def _():
        answer((behind_id,), (ahead_id,))

    load_e.wait()
    send_first((send_behind,), (send_ahead,))
    own_twin.start()

    @pl.when(d < D - 2)
    def _():
        pl.semaphore_wait(up_sem.at[0], 1)

    send_first((send_ahead,), (send_behind,))
    stages = stage_sem.shape[0]
    next_stage(0)

    for copy in load_small:
        copy.wait()
    load_w.wait()
    w2 = w2v[...]

    ends = (S + T) // 2 - 1

    early, late = T // 4 + 1, T // 2 + 2
    direct = (S + late + 1) // 2

    def forward(slot):
        u, row = spot(slot)
        act = jnp.dot(block(slot)[...], w1v[...], preferred_element_type=jnp.float32)
        sg = 0.5 + 0.5 * jnp.tanh(0.5 * act)
        hidden = act * sg
        bend = sg + hidden * (1.0 - sg)
        slope[u, pl.ds(row, C), :] = bend.astype(jnp.bfloat16)
        if isinstance(slot, int) and slot // 2 >= direct:
            column = across(lam_row[slot // 2, 0:1, slot % 2 * C : slot % 2 * C + C], C)[:, 0:1]
            w2g_ref[...] += jnp.sum(hidden * column, axis=0, keepdims=True)
        else:
            hid[u, pl.ds(row, C), :] = hidden.astype(jnp.bfloat16)
        return hidden, bend

    hidden, bend = forward(s)
    info[d, 0] = row_tile(jnp.sum(hidden * w2, axis=1, keepdims=True))[0:1, :]
    info[d, 1] = small[2].astype(jnp.float32)
    info[d, 2] = (small[0] * 1024 + small[1]).astype(jnp.float32)
    stage_wait(0)
    if stages > 1:
        next_stage(1)
    pre[...] = lax.dot_general(
        (bend * w2).astype(jnp.bfloat16), w1v[...], (((1,), (1,)), ((), ())),
        preferred_element_type=jnp.float32,
    )
    def doc_peer(k):
        return lax.rem(d + k, D)

    def info_copy(k):
        return remote(
            info.at[d], info.at[d], info_sem.at[0], info_sem.at[1], {"docs": doc_peer(k)}
        )

    lane_steps = [(a, b) for a in range(M) for b in range(S) if a or b]

    def lam_copy(a, b):
        peer = {"mp": lax.rem(m + a, M), "sub": lax.rem(s + b, S)}
        return remote(lam_all.at[me], lam_all.at[me], lam_sem.at[0], lam_sem.at[1], peer)

    infos, lams = info.at[pl.ds(0, D - 1)], lam_all.at[pl.ds(0, M * S - 1)]
    info_both = remote(infos, infos, info_sem.at[0], info_sem.at[1], twin_id)
    lam_both = remote(lams, lams, lam_sem.at[0], lam_sem.at[1], twin_id)

    reach = min(stages, max(1, D - 2))
    for k in range(2, reach + 1):
        stage_wait(k - 1)
        if k < stages:
            next_stage(k)
    for k in range(1, D):
        info_copy(k).start()
    send_both(P - 1)
    own_twin.wait_recv()
    forward(other)

    def relay(t):
        ring_wait(t)

        @pl.when(t + P < T)
        def _():
            ahead_copy(part(S + t, s, 0), t + P).start()
            behind_copy(part(S + t, s, 1), t + P).start()

        @pl.when((s == 0) & (t == T - 1 - P))
        def _():
            for way, peer in ((0, ahead_id), (1, behind_id)):
                remote(
                    part(S + t, 0, way), part(S + T - 1, 0, way), send_sem.at[0],
                    twin_recv.at[T - 1], {**peer, "sub": other},
                ).start()

        pl.when((s > 0) | (t < T - 1))(lambda: twin_copy(t, s).start())

    def lead_relay(t):
        q = t + LEAD * s
        if isinstance(t, int) and t + LEAD * (S - 1) < T:
            relay(q)
        else:
            pl.when(q < T)(lambda: relay(q))

    half = 2 * PR

    def lane_forward(lane_s):
        spots = [(S + t) * C + lane_s * half for t in (T - 2, T - 1)]
        x = jnp.concatenate([xs[pl.ds(spot, half), :] for spot in spots], axis=0)
        act = jnp.dot(x, w1v[...], preferred_element_type=jnp.float32)
        sg = 0.5 + 0.5 * jnp.tanh(0.5 * act)
        hidden = act * sg
        bend = (sg + hidden * (1.0 - sg)).astype(jnp.bfloat16)
        for k in range(2):
            here = slice(k * half, (k + 1) * half)
            begin = k * C + lane_s * half
            slope_end[begin : begin + half, :] = bend[here, :]
            column = across(lam_row[ends, 0:1, k * C : k * C + C], C)
            column = column[lane_s * half : (lane_s + 1) * half, 0:1]
            w2g_ref[...] += jnp.sum(hidden[here, :] * column, axis=0, keepdims=True)

    def step_forward(t):
        twin_copy(t, other).wait_recv()
        forward(S + t)

    def relay_forward(t, carry):
        lead_relay(t)
        step_forward(t)
        return carry

    @pl.when(s > 0)
    def _():
        for t in range(LEAD):
            relay(t)

    lax.fori_loop(0, early, relay_forward, 0)

    info_both.wait_recv()
    slot_of = lax.broadcasted_iota(jnp.int32, (1, C), 1).astype(jnp.float32)
    total = float(D * C)

    def key_of(jd):
        return info[jd, 1] * total - (slot_of + lax.convert_element_type(jd * C, jnp.float32))

    def rank_step(jd, carry):
        q_j = across(info[jd, 2], C)
        s_j = across(info[jd, 0], C)
        key_j = across(key_of(jd), C)
        out = []
        for i in range(D):
            same = q_j == info[i, 2]
            push = 0.5 + 0.5 * jnp.tanh(0.5 * (s_j - info[i, 0]))
            ahead = same & (key_j > key_of(i))
            out.append(carry[i] + jnp.sum(jnp.where(same, push, 0.0), axis=0, keepdims=True))
            out.append(carry[D + i] + jnp.sum(jnp.where(ahead, 1.0, 0.0), axis=0, keepdims=True))
        return tuple(out[0::2] + out[1::2])

    zeros = tuple(jnp.zeros((1, C), jnp.float32) for _ in range(2 * D))
    ranks = lax.fori_loop(0, D, rank_step, zeros)
    for i in range(D):
        gain = jnp.exp2(info[i, 1]) - 1.0
        term[i, 0:1, :] = gain / log2(2.0 + ranks[D + i])
        drow[i, 0:1, :] = 1.0 / log2(2.0 + (ranks[i] - 0.5))

    pl.when(s == 0)(lambda: relay(early))

    def lambda_step(jd, carry):
        q_j = across(info[jd, 2], C)
        s_j = across(info[jd, 0], C)
        gain_j = across(jnp.exp2(info[jd, 1]) - 1.0, C)
        disc_j = across(drow[jd, 0:1, :], C)
        term_j = across(term[jd, 0:1, :], C)
        out = []
        for i in range(D):
            same = q_j == info[i, 2]
            gain_i = jnp.exp2(info[i, 1]) - 1.0
            gap = info[i, 0] - s_j
            weight = (gain_j - gain_i) * jnp.abs(drow[i, 0:1, :] - disc_j)
            push = 0.5 + 0.5 * jnp.tanh(0.5 * jnp.where(gain_i > gain_j, -gap, gap))
            out.append(
                carry[i] + jnp.sum(jnp.where(same, weight * push, 0.0), axis=0, keepdims=True)
            )
            out.append(
                carry[D + i] + jnp.sum(jnp.where(same, term_j, 0.0), axis=0, keepdims=True)
            )
        return tuple(out[0::2] + out[1::2])

    sums = lax.fori_loop(0, D, lambda_step, zeros)
    for i in range(D):
        idcg = sums[D + i]
        inv = jnp.where(idcg > 0.0, 1.0 / jnp.where(idcg > 0.0, idcg, 1.0), 0.0)
        lam_all[me, i] = sums[i] * inv
    for k in range(reach + 1, stages + 1):
        stage_wait(k - 1)
        if k < stages:
            next_stage(k)
    for a, b in lane_steps:
        lam_copy(a, b).start()

    for i in range(D):
        lam_exp[me, i] = jnp.broadcast_to(lam_all[me, i], (8, C))
    emb_grad_ref[...] = (pre[...] * across(lam_exp[me, d, 0:1, :], C)[:, 0:1]).astype(jnp.bfloat16)

    pl.when(s > 0)(lambda: relay(early + LEAD))
    lead_relay(early + 1)
    step_forward(early)
    step_forward(early + 1)
    lax.fori_loop(early + 2, late, relay_forward, 0)

    lam_both.wait_recv()
    for a, b in lane_steps:
        lane = lax.rem(m + M - a, M) * S + lax.rem(s + S - b, S)
        for i in range(D):
            lam_exp[lane, i] = jnp.broadcast_to(lam_all[lane, i], (8, C))

    lane_no = lax.broadcasted_iota(jnp.int32, (8, C), 1) // PR
    row_no = lax.broadcasted_iota(jnp.int32, (16, C), 0)

    def put_lambda(slot, tile):
        cols = slice(slot % 2 * C, slot % 2 * C + C)
        lam_row[slot // 2, :, cols] = tile
        high = tile.astype(jnp.bfloat16).astype(jnp.float32)
        both = jnp.concatenate([high, tile - high], axis=0)
        lam_pair[slot // 2, :, cols] = jnp.where(row_no % 8 == 0, both, 0.0).astype(jnp.bfloat16)

    for b in range(S):
        put_lambda(b, lam_exp[m * S + b, d])
    for t in range(T):
        tile = jnp.zeros((8, C), jnp.float32)
        for way in range(2):
            q = lax.rem((r - (t // P + 1) if way == 0 else r + (t // P + 1)) + 2 * N, N)
            q_m = jnp.where(q < D, 0, 1)
            q_d = jnp.where(q < D, q, N - 1 - q)
            p = t % P if way == 0 else P - 1 - t % P
            for b in range(S):
                place = b * 2 + way
                values = lam_exp[q_m * S + b, q_d]
                if place != p:
                    values = pltpu.roll(values, ((place - p) * PR) % C, 1)
                tile = jnp.where(lane_no == place, values, tile)
        put_lambda(S + t, tile)

    first = pl.multiple_of(me * rows, LANES)
    chunk = min(H, 256)

    def turned(u, begin=0, count=2 * C):
        values = xs[pl.ds(u * 2 * C + begin, count), pl.ds(first, rows)].astype(jnp.float32)
        return (values.T * lam_row[u, 0:1, begin : begin + count]).astype(jnp.bfloat16)

    def gradient(u, begin):
        at = turned(u)
        pair = lam_pair[u] if u < direct else None
        for c in range(0, H, chunk):
            cols = slice(c, c + chunk)
            grad = jnp.dot(at, slope[u, :, cols], preferred_element_type=jnp.float32)
            w1g_ref[:, cols] = grad if begin else w1g_ref[:, cols] + grad
            if u < direct:
                top = jnp.dot(pair, hid[u, :, cols], preferred_element_type=jnp.float32)
                wtot[:, cols] = top if begin else wtot[:, cols] + top

    w2g_ref[...] = jnp.zeros(w2g_ref.shape, jnp.float32)
    gradient(0, True)
    gradient(1, False)
    left = list(range(2, ends))
    for t in range(late, T - 2):
        if t < T - 4:
            lead_relay(t)
        else:
            pl.when(s == 0)(lambda t=t: relay(t))
        if t == T - 3:
            pl.when(s > 0)(lambda: lane_forward(1))
        step_forward(t)
        if t == T - 4:
            pl.when(s > 0)(lambda: relay(T - 2))
        ready = [u for u in left if 2 * u <= t + 1]
        for u in ready if t == T - 3 else ready[:2]:
            gradient(u, False)
            left.remove(u)
        if t == T - 4:
            pl.when(s > 0)(lambda: relay(T - 1))
    w2g_ref[...] += jnp.sum(wtot[...], axis=0, keepdims=True)

    @pl.when(s == 0)
    def _():
        relay(T - 2)
        relay(T - 1)
        lane_forward(0)

    own_twin.wait_send()
    info_both.wait_send()
    lam_both.wait_send()
    for t in (T - 2, T - 1):
        twin_copy(t, other).wait_recv()
    at_end[...] = turned(ends)
    pl.when(s == 0)(lambda: lane_forward(1))
    pl.when(s > 0)(lambda: lane_forward(0))
    sent = xs.at[pl.ds(0, T * 4 * PR)]
    remote(sent, sent, send_sem.at[0], ring_recv.at[0], twin_id).wait_send()


def ring_call(sizes, operands):
    D, M, S, C, E, H, rows, P = sizes
    L, N = M * S, D * M
    T = P * (N - 1) // 2
    f32, bf16 = jnp.float32, jnp.bfloat16
    vmem = pl.BlockSpec(memory_space=pltpu.VMEM)
    hbm = pl.BlockSpec(memory_space=pl.ANY)
    dma = pltpu.SemaphoreType.DMA
    slots = S + T
    crossing = max(min(2 * (D - 1 - i), 2 * i) + 1 for i in range(D))
    stages = max(D - 1, crossing + 1) - 1
    scratch = [
        pltpu.VMEM((E, H), bf16),
        pltpu.VMEM((slots * C, E), bf16),
        pltpu.VMEM((slots // 2, 2 * C, H), bf16),
        pltpu.VMEM((slots // 2, 2 * C, H), bf16),
        pltpu.VMEM((3, 1, C), jnp.int32),
        pltpu.VMEM((C, E), f32),
        pltpu.VMEM((16, H), f32),
        pltpu.VMEM((D, 3, 1, C), f32),
        pltpu.VMEM((D, 8, C), f32),
        pltpu.VMEM((D, 8, C), f32),
        pltpu.VMEM((L, D, 1, C), f32),
        pltpu.VMEM((L, D, 8, C), f32),
        pltpu.VMEM((slots // 2, 8, 2 * C), f32),
        pltpu.VMEM((slots // 2, 16, 2 * C), bf16),
        dma((6,)), dma((T,)), dma((T,)), dma((2,)), dma((2,)), dma((2,)), dma((1,)),
        pltpu.SemaphoreType.REGULAR((stages,)),
        pltpu.SemaphoreType.REGULAR((1,)),
    ]
    held = pl.pallas_call(
        functools.partial(ring_kernel, sizes),
        out_shape=(
            pltpu.VMEM((C, E), bf16),
            pltpu.VMEM((rows, H), f32),
            pltpu.VMEM((1, H), f32),
            pltpu.VMEM((rows, 2 * C), bf16),
            pltpu.VMEM((2 * C, H), bf16),
            pltpu.VMEM((1, H), f32),
        ),
        in_specs=[hbm] * 6,
        out_specs=(vmem,) * 6,
        scratch_shapes=scratch,
        compiler_params=pltpu.CompilerParams(
            collective_id=0, has_side_effects=True, vmem_limit_bytes=56 * 1024 * 1024
        ),
    )(*operands)
    return pl.pallas_call(
        finish,
        out_shape=(
            jax.ShapeDtypeStruct((C, E), bf16),
            jax.ShapeDtypeStruct((rows, H), f32),
            jax.ShapeDtypeStruct((1, H), f32),
        ),
        in_specs=[vmem] * 6,
        out_specs=(hbm,) * 3,
        scratch_shapes=[pltpu.VMEM((rows, H), f32), dma((3,))],
        compiler_params=pltpu.CompilerParams(vmem_limit_bytes=4 * 1024 * 1024),
    )(*held)


def finish(emb_grad, w1g, w2g, at, slope, w2, emb_out, w1g_out, w2g_out, w1g_end, sem):
    H = w2.shape[1]
    parts = PARTS
    wide = H // parts
    copies = [
        pltpu.make_async_copy(emb_grad, emb_out, sem.at[0]),
        pltpu.make_async_copy(w2g, w2g_out, sem.at[1]),
    ]
    for copy in copies:
        copy.start()
    for c in range(parts):
        cols = slice(c * wide, (c + 1) * wide)
        grad = jnp.dot(at[...], slope[:, cols], preferred_element_type=jnp.float32)
        w1g_end[:, cols] = (w1g[:, cols] + grad) * w2[:, cols]
        pltpu.make_async_copy(w1g_end.at[:, cols], w1g_out.at[:, cols], sem.at[2]).start()
    for copy in copies:
        copy.wait()
    pltpu.make_async_copy(w1g_end, w1g_out, sem.at[2]).wait()


def write_out(a_ref, b_ref, c_ref, a_out, b_out, c_out, sem):
    pairs = ((b_ref, b_out), (a_ref, a_out), (c_ref, c_out))
    copies = [pltpu.make_async_copy(x, y, sem.at[i]) for i, (x, y) in enumerate(pairs)]
    for copy in copies:
        copy.start()
    for copy in copies:
        copy.wait()


def reduce_call(sizes, operands):
    D, M, S, C, E, H, rows = sizes
    L = M * S
    width = max(rows, LANES)
    Kc = 4
    Kr = max(1, rows // 32)
    K = Kc * Kr
    f32, bf16 = jnp.float32, jnp.bfloat16
    vmem = pl.BlockSpec(memory_space=pltpu.VMEM)
    hbm = pl.BlockSpec(memory_space=pl.ANY)
    dma = pltpu.SemaphoreType.DMA
    chunk = (K, rows // Kr, H // Kc)
    scratch = [
        pltpu.VMEM((E, H), bf16),
        pltpu.VMEM((L * C, E), bf16),
        pltpu.VMEM((L * C, H), f32),
        pltpu.VMEM((L * C, H), f32),
        pltpu.VMEM((L * C, H), bf16),
        pltpu.VMEM((width, L * C), bf16),
        pltpu.VMEM((Kc, width, H // Kc), f32),
        pltpu.VMEM((D, 8, C), f32),
        pltpu.VMEM((D, 8, C), f32),
        pltpu.VMEM((D, 8, C), f32),
        pltpu.VMEM((D, 8, C), f32),
        pltpu.VMEM((L, 8, C), f32),
        pltpu.VMEM((D, H // LANES, LANES), f32),
        pltpu.VMEM(chunk, bf16),
        pltpu.VMEM(chunk, bf16),
        pltpu.VMEM(chunk, bf16),
        pltpu.VMEM(chunk, bf16),
        dma((2,)),
        dma((L,)), dma((L,)),
        dma((D,)), dma((D,)),
        dma((D,)), dma((D,)),
        dma((L,)), dma((L,)),
        dma((D,)), dma((D,)),
        dma((K,)), dma((K,)), dma((K,)), dma((K,)),
    ]
    return pl.pallas_call(
        functools.partial(kernel, (D, M, S, C, E, H, rows, Kc, Kr)),
        out_shape=(
            pltpu.VMEM((C, E), bf16),
            pltpu.VMEM((rows, H), f32),
            pltpu.VMEM((1, H), f32),
        ),
        in_specs=[hbm, hbm, vmem, vmem, vmem, vmem],
        out_specs=(vmem, vmem, vmem),
        scratch_shapes=scratch,
        compiler_params=pltpu.CompilerParams(
            collective_id=0, has_side_effects=True, vmem_limit_bytes=56 * 1024 * 1024
        ),
    )(*operands)


def on_device(embeddings, owner_shard, query_local, labels, w_first, w_second):
    D, M, S = lax.axis_size("docs"), lax.axis_size("mp"), lax.axis_size("sub")
    C, E = embeddings.shape
    H = w_first.shape[1]
    L = M * S
    rows = E // L
    vmem = pl.BlockSpec(memory_space=pltpu.VMEM)
    hbm = pl.BlockSpec(memory_space=pl.ANY)
    dma = pltpu.SemaphoreType.DMA
    operands = (
        embeddings, w_first, owner_shard.reshape(1, C), query_local.reshape(1, C),
        labels.reshape(1, C), w_second.reshape(1, H),
    )
    P = 2 * S
    held = D * L * C * (E + 2 * H) * 2
    gathers = (
        M == 2 and S == 2 and D > 3 and C == LANES and rows % LANES == 0 and held <= 32 * 2**20
    )
    if gathers:
        emb_grad, w1g, w2g = ring_call((D, M, S, C, E, H, rows, P), operands)
        return emb_grad, w1g, w2g.reshape(H)
    emb_grad, w1g, w2g = reduce_call((D, M, S, C, E, H, rows), operands)
    emb_grad, w1g, w2g = pl.pallas_call(
        write_out,
        out_shape=tuple(jax.ShapeDtypeStruct(v.shape, v.dtype) for v in (emb_grad, w1g, w2g)),
        in_specs=[vmem] * 3,
        out_specs=(hbm,) * 3,
        scratch_shapes=[dma((3,))],
        compiler_params=pltpu.CompilerParams(vmem_limit_bytes=4 * 1024 * 1024),
    )(emb_grad, w1g, w2g)
    return emb_grad, w1g, w2g.reshape(H)


def solution(mesh):
    return jax.shard_map(
        on_device,
        mesh=mesh,
        in_specs=(
            P(("groups", "docs", "mp", "sub"), None),
            P(("groups", "docs", "mp", "sub"), None),
            P(("groups", "docs", "mp", "sub")),
            P(("groups", "docs", "mp", "sub")),
            P(),
            P(),
        ),
        out_specs=(
            P(("groups", "docs", "mp", "sub"), None),
            P(("groups", "mp", "sub"), None),
            P("groups"),
        ),
        check_vma=False,
    )
```

```python
import functools

import jax
import jax.numpy as jnp
from jax import lax
from jax.experimental import pallas as pl
from jax.experimental.pallas import tpu as pltpu
from jax.sharding import PartitionSpec as P

MESH = pl.DeviceIdType.MESH
LANES = 128
LOG2E = 1.4426950408889634


def log2(v):
    return jnp.log(v) * LOG2E


def across(row, rows):
    return jnp.broadcast_to(row, (rows, row.shape[1])).T


def row_tile(column):
    return jnp.broadcast_to(column, (column.shape[0], LANES)).T[0:8, :]


def kernel(
    sizes,
    emb_hbm, w1_hbm, owner_ref, local_ref, labels_ref, w2_ref,
    emb_grad_ref, w1g_ref, w2g_ref,
    w1v, embs, slope, hid, pg, at, wacc,
    minfo, sinfo, term, drow, lam, w2p,
    part, from_out, from_in, tot,
    load_sem, emb_send, emb_recv, m_send, m_recv, s_send, s_recv,
    l_send, l_recv, g_send, g_recv, in_send, out_send, fo_recv, fi_recv,
):
    D, M, S, C, E, H, rows, Kc, Kr = sizes
    L = M * S
    K = Kc * Kr
    d, m, s = lax.axis_index("docs"), lax.axis_index("mp"), lax.axis_index("sub")
    me = m * S + s

    load_w = pltpu.make_async_copy(w1_hbm, w1v, load_sem.at[0])
    load_e = pltpu.make_async_copy(emb_hbm, embs.at[pl.ds(me * C, C)], load_sem.at[1])
    load_e.start()
    load_w.start()

    def doc_peer(k):
        return lax.rem(d + k, D)

    def mp_peer(k):
        return lax.rem(m + k, M)

    def sub_peer(k):
        return lax.rem(s + k, S)

    lane_steps = [(a, b) for a in range(M) for b in range(S) if a or b]

    barrier = pltpu.get_barrier_semaphore()
    for k in range(1, D):
        pl.semaphore_signal(barrier, inc=1, device_id={"docs": doc_peer(k)}, device_id_type=MESH)
    for a, b in lane_steps:
        pl.semaphore_signal(
            barrier, inc=1, device_id={"mp": mp_peer(a), "sub": sub_peer(b)}, device_id_type=MESH
        )

    lab_own = labels_ref[...].astype(jnp.float32)
    q_own = (owner_ref[...] * 1024 + local_ref[...]).astype(jnp.float32)
    minfo[d, 0:1, :] = lab_own
    minfo[d, 1:2, :] = q_own

    pl.semaphore_wait(barrier, D - 1 + L - 1)

    def doc_send(buf, k, send, recv):
        return pltpu.make_async_remote_copy(
            src_ref=buf.at[d], dst_ref=buf.at[d], send_sem=send.at[k], recv_sem=recv.at[k],
            device_id={"docs": doc_peer(k)}, device_id_type=MESH,
        )

    load_e.wait()

    def emb_copy(lane, a, b, index):
        block = embs.at[pl.ds(lane * C, C)]
        return pltpu.make_async_remote_copy(
            src_ref=block, dst_ref=block, send_sem=emb_send.at[index], recv_sem=emb_recv.at[index],
            device_id={"mp": mp_peer(a), "sub": sub_peer(b)}, device_id_type=MESH,
        )

    for a in range(1, M):
        emb_copy(me, a, 0, a * S).start()
    for b in range(1, S):
        emb_copy(me, 0, b, b).start()
    for k in range(1, D):
        doc_send(minfo, k, m_send, m_recv).start()

    w2 = w2_ref[...]

    def forward(lane):
        at_rows = pl.ds(lane * C, C)
        act = jnp.dot(embs[at_rows, :], w1v[...], preferred_element_type=jnp.float32)
        sg = jax.nn.sigmoid(act)
        hidden = act * sg
        hid[at_rows, :] = hidden
        slope[at_rows, :] = w2 * (sg * (1.0 + act * (1.0 - sg)))
        return hidden

    load_w.wait()
    hidden = forward(me)
    sinfo[d] = row_tile(jnp.sum(hidden * w2, axis=1, keepdims=True))
    for k in range(1, D):
        doc_send(sinfo, k, s_send, s_recv).start()

    def lane_from(a, b):
        return lax.rem(m + M - a, M) * S + lax.rem(s + S - b, S)

    def recv_wait(a, b):
        emb_copy(lane_from(a, b), a, b, a * S + b).wait_recv()

    for b in range(1, S):
        recv_wait(0, b)
        forward(lane_from(0, b))

    for k in range(1, D):
        doc_send(minfo, k, m_send, m_recv).wait_recv()
    slot = lax.broadcasted_iota(jnp.int32, (1, C), 1).astype(jnp.float32)
    total = float(D * C)

    def key_of(label_row, dd):
        return label_row * total - (slot + lax.convert_element_type(dd * C, jnp.float32))

    def ideal_step(jd, carry):
        q_j = across(minfo[jd, 1:2, :], C)
        key_j = across(key_of(minfo[jd, 0:1, :], jd), C)
        out = []
        for i in range(D):
            ahead = (q_j == minfo[i, 1:2, :]) & (key_j > key_of(minfo[i, 0:1, :], i))
            out.append(carry[i] + jnp.sum(jnp.where(ahead, 1.0, 0.0), axis=0, keepdims=True))
        return tuple(out)

    zeros = tuple(jnp.zeros((1, C), jnp.float32) for _ in range(D))
    ideal = lax.fori_loop(0, D, ideal_step, zeros)
    for i in range(D):
        gain = jnp.exp2(minfo[i, 0:1, :]) - 1.0
        term[i, 0:1, :] = gain / log2(2.0 + ideal[i])
    q_i = across(q_own, C)
    gain_i = across(jnp.exp2(lab_own) - 1.0, C)
    idcg = jnp.zeros((C, C), jnp.float32)
    for j in range(D):
        idcg = idcg + jnp.where(q_i == minfo[j, 1:2, :], term[j, 0:1, :], 0.0)
    idcg = jnp.sum(idcg, axis=1, keepdims=True)
    inv = jnp.where(idcg > 0.0, 1.0 / jnp.where(idcg > 0.0, idcg, 1.0), 0.0)

    for k in range(1, D):
        doc_send(sinfo, k, s_send, s_recv).wait_recv()

    def soft_step(jd, carry):
        q_j = across(minfo[jd, 1:2, :], C)
        s_j = across(sinfo[jd, 0:1, :], C)
        out = []
        for i in range(D):
            part_of = jnp.where(
                q_j == minfo[i, 1:2, :], jax.nn.sigmoid(s_j - sinfo[i, 0:1, :]), 0.0
            )
            out.append(carry[i] + jnp.sum(part_of, axis=0, keepdims=True))
        return tuple(out)

    soft = lax.fori_loop(0, D, soft_step, zeros)
    for i in range(D):
        drow[i, 0:1, :] = 1.0 / log2(2.0 + (soft[i] - 0.5))
    disc_i = across(drow[d, 0:1, :], C)
    s_i = across(sinfo[d, 0:1, :], C)

    def lambda_step(j, acc):
        gain_j = jnp.exp2(minfo[j, 0:1, :]) - 1.0
        gap = s_i - sinfo[j, 0:1, :]
        weight = (gain_j - gain_i) * jnp.abs(disc_i - drow[j, 0:1, :])
        push = jax.nn.sigmoid(jnp.where(gain_i > gain_j, -gap, gap))
        return acc + jnp.where(q_i == minfo[j, 1:2, :], weight * push, 0.0)

    lam_acc = lax.fori_loop(0, D, lambda_step, jnp.zeros((C, C), jnp.float32))
    lam_col = jnp.sum(lam_acc, axis=1, keepdims=True) * inv
    lam[me] = row_tile(lam_col)

    def lam_copy(lane, a, b):
        return pltpu.make_async_remote_copy(
            src_ref=lam.at[lane], dst_ref=lam.at[lane],
            send_sem=l_send.at[a * S + b], recv_sem=l_recv.at[a * S + b],
            device_id={"mp": mp_peer(a), "sub": sub_peer(b)}, device_id_type=MESH,
        )

    for a, b in lane_steps:
        lam_copy(me, a, b).start()

    def scale(lane, column):
        at_rows = pl.ds(lane * C, C)
        pg[at_rows, :] = (column * slope[at_rows, :]).astype(jnp.bfloat16)

    scale(me, lam_col)
    emb_grad_ref[...] = lax.dot_general(
        pg[pl.ds(me * C, C), :], w1v[...], (((1,), (1,)), ((), ())),
        preferred_element_type=jnp.float32,
    ).astype(jnp.bfloat16)
    for a in range(1, M):
        recv_wait(a, 0)
        for b in range(1, S):
            emb_copy(lane_from(a, 0), 0, b, a * S + b).start()
        forward(lane_from(a, 0))
    for a in range(1, M):
        for b in range(1, S):
            recv_wait(a, b)
            forward(lane_from(a, b))
    width = at.shape[0]
    first = pl.multiple_of((me * rows) // LANES * LANES, LANES)
    for lane in range(L):
        at[:, pl.ds(lane * C, C)] = embs[pl.ds(lane * C, C), pl.ds(first, width)].T

    for a, b in lane_steps:
        lam_copy(lane_from(a, b), a, b).wait_recv()
        lane = lane_from(a, b)
        scale(lane, across(lam[lane, 0:1, :], C)[:, 0:1])

    half = D // 2
    left = d < half
    inward = jnp.where(left, d + 1, d - 1)
    outward = jnp.where(left, d - 1, d + 1)
    place = jnp.where(left, d, D - 1 - d)
    has_out = place > 0
    middle = place == half - 1
    cw, rh = H // Kc, rows // Kr

    def send_in(k, to_middle):
        dst, sem = (from_in, fi_recv) if to_middle else (from_out, fo_recv)
        return pltpu.make_async_remote_copy(
            src_ref=part.at[k], dst_ref=dst.at[k], send_sem=in_send.at[k], recv_sem=sem.at[k],
            device_id={"docs": inward}, device_id_type=MESH,
        )

    def send_out(k, from_total):
        src = tot if from_total else from_in
        return pltpu.make_async_remote_copy(
            src_ref=src.at[k], dst_ref=from_in.at[k], send_sem=out_send.at[k],
            recv_sem=fi_recv.at[k], device_id={"docs": outward}, device_id_type=MESH,
        )

    def start_in(k):
        pl.when(middle)(lambda: send_in(k, True).start())
        if half > 1:
            pl.when(jnp.logical_not(middle))(lambda: send_in(k, False).start())

    shift = me * rows - first
    for c in range(Kc):
        wide = jnp.dot(at[...], pg[:, c * cw : (c + 1) * cw], preferred_element_type=jnp.float32)
        wacc[c] = wide
        for r in range(Kr):
            k = c * Kr + r

            @pl.when(jnp.logical_not(has_out))
            def _():
                part[k] = wacc[c, pl.ds(pl.multiple_of(shift + r * rh, 8), rh), :].astype(
                    jnp.bfloat16
                )
                start_in(k)

    w2_part = jnp.zeros((1, H), jnp.float32)
    for lane in range(L):
        column = across(lam[lane, 0:1, :], C)[:, 0:1]
        w2_part = w2_part + jnp.sum(column * hid[pl.ds(lane * C, C), :], axis=0, keepdims=True)
    for j in range(H // LANES):
        w2p[d, j : j + 1, :] = w2_part[:, j * LANES : (j + 1) * LANES]
    for k in range(1, D):
        doc_send(w2p, k, g_send, g_recv).start()

    def gather_step(k):
        c, r = k // Kr, k % Kr

        @pl.when(has_out)
        def _():
            send_in(k, False).wait_recv()
            own = wacc[c, pl.ds(pl.multiple_of(shift + r * rh, 8), rh), :]
            part[k] = (own + from_out[k].astype(jnp.float32)).astype(jnp.bfloat16)
            start_in(k)

    def finish_step(k):
        c, r = k // Kr, k % Kr
        send_out(k, False).wait_recv()
        spot = (slice(r * rh, (r + 1) * rh), slice(c * cw, (c + 1) * cw))

        @pl.when(middle)
        def _():
            both = (part[k].astype(jnp.float32) + from_in[k].astype(jnp.float32)).astype(
                jnp.bfloat16
            )
            w1g_ref[spot] = both.astype(jnp.float32)
            if half > 1:
                tot[k] = both
                pl.when(has_out)(lambda: send_out(k, True).start())

        if half > 1:

            @pl.when(jnp.logical_not(middle))
            def _():
                pl.when(has_out)(lambda: send_out(k, False).start())
                w1g_ref[spot] = from_in[k].astype(jnp.float32)

    lag = max(1, K // 4)
    for k in range(lag):
        gather_step(k)
    for k in range(lag, K + lag):
        if k < K:
            gather_step(k)
        finish_step(k - lag)

    for k in range(1, D):
        doc_send(w2p, k, g_send, g_recv).wait_recv()
    w2_sum = w2p[0]
    for j in range(1, D):
        w2_sum = w2_sum + w2p[j]
    for j in range(H // LANES):
        w2g_ref[0:1, j * LANES : (j + 1) * LANES] = w2_sum[j : j + 1, :]

    for k in range(1, D):
        doc_send(minfo, k, m_send, m_recv).wait_send()
        doc_send(sinfo, k, s_send, s_recv).wait_send()
        doc_send(w2p, k, g_send, g_recv).wait_send()
    for a, b in lane_steps:
        emb_copy(me, a, b, a * S + b).wait_send()
        lam_copy(me, a, b).wait_send()
    for k in range(K):
        send_in(k, True).wait_send()
    for k in range(K):
        pl.when(has_out)(lambda k=k: send_out(k, False).wait_send())

LEAD = 2
PARTS = 4


def ring_kernel(
    sizes,
    emb_hbm, w1_hbm, owner_hbm, local_hbm, labels_hbm, w2_hbm,
    emb_grad_ref, w1g_ref, w2g_ref, at_end, slope_end, w2v,
    w1v, xs, slope, hid, small, pre, wtot,
    info, term, drow, lam_all, lam_exp, lam_row, lam_pair,
    load_sem, ring_recv, twin_recv, own_sem, info_sem, lam_sem, send_sem, stage_sem, up_sem,
):
    D, M, S, C, E, H, rows, P = sizes
    N = D * M
    PR = C // P
    T = P * (N - 1) // 2
    d, m, s = lax.axis_index("docs"), lax.axis_index("mp"), lax.axis_index("sub")
    me = m * S + s
    other = S - 1 - s
    r = jnp.where(m == 0, d, N - 1 - d)

    def ring_at(q):
        q = lax.rem(q + 2 * N, N)
        return {"docs": jnp.where(q < D, q, N - 1 - q), "mp": jnp.where(q < D, 0, 1)}

    ahead_id, behind_id, twin_id = ring_at(r + 1), ring_at(r - 1), {"sub": other}

    def spot(slot):
        return lax.div(slot, 2), pl.multiple_of(lax.rem(slot, 2) * C, C)

    def block(slot):
        return xs.at[pl.ds(pl.multiple_of(slot * C, C), C)]

    load_e = pltpu.make_async_copy(emb_hbm, block(s), load_sem.at[0])
    load_w = pltpu.make_async_copy(w1_hbm, w1v, load_sem.at[1])
    load_small = [
        pltpu.make_async_copy(owner_hbm, small.at[0], load_sem.at[2]),
        pltpu.make_async_copy(local_hbm, small.at[1], load_sem.at[3]),
        pltpu.make_async_copy(labels_hbm, small.at[2], load_sem.at[4]),
        pltpu.make_async_copy(w2_hbm, w2v, load_sem.at[5]),
    ]
    load_e.start()
    barrier = pltpu.get_barrier_semaphore()

    def flows(act):
        def of(first, second):
            pl.when(m == 0)(lambda: act(*first))
            pl.when(m > 0)(lambda: act(*second))

        return of

    @flows
    def hello_up(peer):
        pl.semaphore_signal(barrier, inc=1, device_id=peer, device_id_type=MESH)

    pl.semaphore_signal(barrier, inc=1, device_id=twin_id, device_id_type=MESH)
    hello_up((ahead_id,), (behind_id,))

    @pl.when((d == 0) | (d == D - 1))
    def _():
        hello_up((behind_id,), (ahead_id,))

    load_w.start()
    for copy in load_small:
        copy.start()

    def remote(src, dst, send, recv, peer):
        return pltpu.make_async_remote_copy(
            src_ref=src, dst_ref=dst, send_sem=send, recv_sem=recv,
            device_id=peer, device_id_type=MESH,
        )

    def part(slot, lane_s, way):
        return block(slot).at[pl.ds((lane_s * 2 + way) * PR, PR)]

    def ahead_copy(src, t):
        return remote(src, part(S + t, s, 0), send_sem.at[0], ring_recv.at[t], ahead_id)

    def behind_copy(src, t):
        return remote(src, part(S + t, s, 1), send_sem.at[0], ring_recv.at[t], behind_id)

    def both_ways(slot, lane_s):
        return block(slot).at[pl.ds(lane_s * 2 * PR, 2 * PR)]

    def ring_wait(t):
        both = both_ways(S + t, s)
        remote(both, both, send_sem.at[0], ring_recv.at[t], ahead_id).wait_recv()

    def twin_copy(t, lane_s):
        both = both_ways(S + t, lane_s)
        return remote(both, both, send_sem.at[0], twin_recv.at[t], twin_id)

    own_twin = remote(block(s), block(s), own_sem.at[0], own_sem.at[1], twin_id)

    def next_stage(k):
        for peer in (ahead_id, behind_id):
            pl.semaphore_signal(stage_sem.at[k], inc=1, device_id=peer, device_id_type=MESH)

    def stage_wait(k):
        pl.semaphore_wait(stage_sem.at[k], 2)

    def send_ahead(p):
        ahead_copy(block(s).at[pl.ds(p * PR, PR)], p).start()

    def send_behind(p):
        behind_copy(block(s).at[pl.ds((P - 1 - p) * PR, PR)], p).start()

    def send_both(p):
        send_ahead(p)
        send_behind(p)

    @flows
    def send_first(send):
        for p in range(P - 1):
            send(p)

    @flows
    def answer(peer):
        pl.semaphore_signal(up_sem.at[0], inc=1, device_id=peer, device_id_type=MESH)

    pl.semaphore_wait(barrier, jnp.where(d >= D - 2, 3, 2))

    @pl.when((d > 0) & (d < D - 1))
    def _():
        answer((behind_id,), (ahead_id,))

    load_e.wait()
    send_first((send_behind,), (send_ahead,))
    own_twin.start()

    @pl.when(d < D - 2)
    def _():
        pl.semaphore_wait(up_sem.at[0], 1)

    send_first((send_ahead,), (send_behind,))
    stages = stage_sem.shape[0]
    next_stage(0)

    for copy in load_small:
        copy.wait()
    load_w.wait()
    w2 = w2v[...]

    ends = (S + T) // 2 - 1

    early, late = T // 4 + 1, T // 2 + 2
    direct = (S + late + 1) // 2

    def forward(slot):
        u, row = spot(slot)
        act = jnp.dot(block(slot)[...], w1v[...], preferred_element_type=jnp.float32)
        sg = 0.5 + 0.5 * jnp.tanh(0.5 * act)
        hidden = act * sg
        bend = sg + hidden * (1.0 - sg)
        slope[u, pl.ds(row, C), :] = bend.astype(jnp.bfloat16)
        if isinstance(slot, int) and slot // 2 >= direct:
            column = across(lam_row[slot // 2, 0:1, slot % 2 * C : slot % 2 * C + C], C)[:, 0:1]
            w2g_ref[...] += jnp.sum(hidden * column, axis=0, keepdims=True)
        else:
            hid[u, pl.ds(row, C), :] = hidden.astype(jnp.bfloat16)
        return hidden, bend

    hidden, bend = forward(s)
    info[d, 0] = row_tile(jnp.sum(hidden * w2, axis=1, keepdims=True))[0:1, :]
    info[d, 1] = small[2].astype(jnp.float32)
    info[d, 2] = (small[0] * 1024 + small[1]).astype(jnp.float32)
    stage_wait(0)
    if stages > 1:
        next_stage(1)
    pre[...] = lax.dot_general(
        (bend * w2).astype(jnp.bfloat16), w1v[...], (((1,), (1,)), ((), ())),
        preferred_element_type=jnp.float32,
    )
    def doc_peer(k):
        return lax.rem(d + k, D)

    def info_copy(k):
        return remote(
            info.at[d], info.at[d], info_sem.at[0], info_sem.at[1], {"docs": doc_peer(k)}
        )

    lane_steps = [(a, b) for a in range(M) for b in range(S) if a or b]

    def lam_copy(a, b):
        peer = {"mp": lax.rem(m + a, M), "sub": lax.rem(s + b, S)}
        return remote(lam_all.at[me], lam_all.at[me], lam_sem.at[0], lam_sem.at[1], peer)

    infos, lams = info.at[pl.ds(0, D - 1)], lam_all.at[pl.ds(0, M * S - 1)]
    info_both = remote(infos, infos, info_sem.at[0], info_sem.at[1], twin_id)
    lam_both = remote(lams, lams, lam_sem.at[0], lam_sem.at[1], twin_id)

    reach = min(stages, max(1, D - 2))
    for k in range(2, reach + 1):
        stage_wait(k - 1)
        if k < stages:
            next_stage(k)
    for k in range(1, D):
        info_copy(k).start()
    send_both(P - 1)
    own_twin.wait_recv()
    forward(other)

    def relay(t):
        ring_wait(t)

        @pl.when(t + P < T)
        def _():
            ahead_copy(part(S + t, s, 0), t + P).start()
            behind_copy(part(S + t, s, 1), t + P).start()

        @pl.when((s == 0) & (t == T - 1 - P))
        def _():
            for way, peer in ((0, ahead_id), (1, behind_id)):
                remote(
                    part(S + t, 0, way), part(S + T - 1, 0, way), send_sem.at[0],
                    twin_recv.at[T - 1], {**peer, "sub": other},
                ).start()

        pl.when((s > 0) | (t < T - 1))(lambda: twin_copy(t, s).start())

    def lead_relay(t):
        q = t + LEAD * s
        if isinstance(t, int) and t + LEAD * (S - 1) < T:
            relay(q)
        else:
            pl.when(q < T)(lambda: relay(q))

    half = 2 * PR

    def lane_forward(lane_s):
        spots = [(S + t) * C + lane_s * half for t in (T - 2, T - 1)]
        x = jnp.concatenate([xs[pl.ds(spot, half), :] for spot in spots], axis=0)
        act = jnp.dot(x, w1v[...], preferred_element_type=jnp.float32)
        sg = 0.5 + 0.5 * jnp.tanh(0.5 * act)
        hidden = act * sg
        bend = (sg + hidden * (1.0 - sg)).astype(jnp.bfloat16)
        for k in range(2):
            here = slice(k * half, (k + 1) * half)
            begin = k * C + lane_s * half
            slope_end[begin : begin + half, :] = bend[here, :]
            column = across(lam_row[ends, 0:1, k * C : k * C + C], C)
            column = column[lane_s * half : (lane_s + 1) * half, 0:1]
            w2g_ref[...] += jnp.sum(hidden[here, :] * column, axis=0, keepdims=True)

    def step_forward(t):
        twin_copy(t, other).wait_recv()
        forward(S + t)

    def relay_forward(t, carry):
        lead_relay(t)
        step_forward(t)
        return carry

    @pl.when(s > 0)
    def _():
        for t in range(LEAD):
            relay(t)

    lax.fori_loop(0, early, relay_forward, 0)

    info_both.wait_recv()
    slot_of = lax.broadcasted_iota(jnp.int32, (1, C), 1).astype(jnp.float32)
    total = float(D * C)

    def key_of(jd):
        return info[jd, 1] * total - (slot_of + lax.convert_element_type(jd * C, jnp.float32))

    def rank_step(jd, carry):
        q_j = across(info[jd, 2], C)
        s_j = across(info[jd, 0], C)
        key_j = across(key_of(jd), C)
        out = []
        for i in range(D):
            same = q_j == info[i, 2]
            push = 0.5 + 0.5 * jnp.tanh(0.5 * (s_j - info[i, 0]))
            ahead = same & (key_j > key_of(i))
            out.append(carry[i] + jnp.sum(jnp.where(same, push, 0.0), axis=0, keepdims=True))
            out.append(carry[D + i] + jnp.sum(jnp.where(ahead, 1.0, 0.0), axis=0, keepdims=True))
        return tuple(out[0::2] + out[1::2])

    zeros = tuple(jnp.zeros((1, C), jnp.float32) for _ in range(2 * D))
    ranks = lax.fori_loop(0, D, rank_step, zeros)
    for i in range(D):
        gain = jnp.exp2(info[i, 1]) - 1.0
        term[i, 0:1, :] = gain / log2(2.0 + ranks[D + i])
        drow[i, 0:1, :] = 1.0 / log2(2.0 + (ranks[i] - 0.5))

    pl.when(s == 0)(lambda: relay(early))

    def lambda_step(jd, carry):
        q_j = across(info[jd, 2], C)
        s_j = across(info[jd, 0], C)
        gain_j = across(jnp.exp2(info[jd, 1]) - 1.0, C)
        disc_j = across(drow[jd, 0:1, :], C)
        term_j = across(term[jd, 0:1, :], C)
        out = []
        for i in range(D):
            same = q_j == info[i, 2]
            gain_i = jnp.exp2(info[i, 1]) - 1.0
            gap = info[i, 0] - s_j
            weight = (gain_j - gain_i) * jnp.abs(drow[i, 0:1, :] - disc_j)
            push = 0.5 + 0.5 * jnp.tanh(0.5 * jnp.where(gain_i > gain_j, -gap, gap))
            out.append(
                carry[i] + jnp.sum(jnp.where(same, weight * push, 0.0), axis=0, keepdims=True)
            )
            out.append(
                carry[D + i] + jnp.sum(jnp.where(same, term_j, 0.0), axis=0, keepdims=True)
            )
        return tuple(out[0::2] + out[1::2])

    sums = lax.fori_loop(0, D, lambda_step, zeros)
    for i in range(D):
        idcg = sums[D + i]
        inv = jnp.where(idcg > 0.0, 1.0 / jnp.where(idcg > 0.0, idcg, 1.0), 0.0)
        lam_all[me, i] = sums[i] * inv
    for k in range(reach + 1, stages + 1):
        stage_wait(k - 1)
        if k < stages:
            next_stage(k)
    for a, b in lane_steps:
        lam_copy(a, b).start()

    for i in range(D):
        lam_exp[me, i] = jnp.broadcast_to(lam_all[me, i], (8, C))
    emb_grad_ref[...] = (pre[...] * across(lam_exp[me, d, 0:1, :], C)[:, 0:1]).astype(jnp.bfloat16)

    pl.when(s > 0)(lambda: relay(early + LEAD))
    lead_relay(early + 1)
    step_forward(early)
    step_forward(early + 1)
    lax.fori_loop(early + 2, late, relay_forward, 0)

    lam_both.wait_recv()
    for a, b in lane_steps:
        lane = lax.rem(m + M - a, M) * S + lax.rem(s + S - b, S)
        for i in range(D):
            lam_exp[lane, i] = jnp.broadcast_to(lam_all[lane, i], (8, C))

    lane_no = lax.broadcasted_iota(jnp.int32, (8, C), 1) // PR
    row_no = lax.broadcasted_iota(jnp.int32, (16, C), 0)

    def put_lambda(slot, tile):
        cols = slice(slot % 2 * C, slot % 2 * C + C)
        lam_row[slot // 2, :, cols] = tile
        high = tile.astype(jnp.bfloat16).astype(jnp.float32)
        both = jnp.concatenate([high, tile - high], axis=0)
        lam_pair[slot // 2, :, cols] = jnp.where(row_no % 8 == 0, both, 0.0).astype(jnp.bfloat16)

    for b in range(S):
        put_lambda(b, lam_exp[m * S + b, d])
    for t in range(T):
        tile = jnp.zeros((8, C), jnp.float32)
        for way in range(2):
            q = lax.rem((r - (t // P + 1) if way == 0 else r + (t // P + 1)) + 2 * N, N)
            q_m = jnp.where(q < D, 0, 1)
            q_d = jnp.where(q < D, q, N - 1 - q)
            p = t % P if way == 0 else P - 1 - t % P
            for b in range(S):
                place = b * 2 + way
                values = lam_exp[q_m * S + b, q_d]
                if place != p:
                    values = pltpu.roll(values, ((place - p) * PR) % C, 1)
                tile = jnp.where(lane_no == place, values, tile)
        put_lambda(S + t, tile)

    first = pl.multiple_of(me * rows, LANES)
    chunk = min(H, 256)

    def turned(u, begin=0, count=2 * C):
        values = xs[pl.ds(u * 2 * C + begin, count), pl.ds(first, rows)].astype(jnp.float32)
        return (values.T * lam_row[u, 0:1, begin : begin + count]).astype(jnp.bfloat16)

    def gradient(u, begin):
        at = turned(u)
        pair = lam_pair[u] if u < direct else None
        for c in range(0, H, chunk):
            cols = slice(c, c + chunk)
            grad = jnp.dot(at, slope[u, :, cols], preferred_element_type=jnp.float32)
            w1g_ref[:, cols] = grad if begin else w1g_ref[:, cols] + grad
            if u < direct:
                top = jnp.dot(pair, hid[u, :, cols], preferred_element_type=jnp.float32)
                wtot[:, cols] = top if begin else wtot[:, cols] + top

    w2g_ref[...] = jnp.zeros(w2g_ref.shape, jnp.float32)
    gradient(0, True)
    gradient(1, False)
    left = list(range(2, ends))
    for t in range(late, T - 2):
        if t < T - 4:
            lead_relay(t)
        else:
            pl.when(s == 0)(lambda t=t: relay(t))
        if t == T - 3:
            pl.when(s > 0)(lambda: lane_forward(1))
        step_forward(t)
        if t == T - 4:
            pl.when(s > 0)(lambda: relay(T - 2))
        ready = [u for u in left if 2 * u <= t + 1]
        for u in ready if t == T - 3 else ready[:2]:
            gradient(u, False)
            left.remove(u)
        if t == T - 4:
            pl.when(s > 0)(lambda: relay(T - 1))
    w2g_ref[...] += jnp.sum(wtot[...], axis=0, keepdims=True)

    @pl.when(s == 0)
    def _():
        relay(T - 2)
        relay(T - 1)
        lane_forward(0)

    own_twin.wait_send()
    info_both.wait_send()
    lam_both.wait_send()
    for t in (T - 2, T - 1):
        twin_copy(t, other).wait_recv()

    @pl.when(s == 0)
    def _():
        at_end[...] = turned(ends)
        lane_forward(1)

    @pl.when(s > 0)
    def _():
        at_end[...] = turned(ends)
        lane_forward(0)

    sent = xs.at[pl.ds(0, T * 4 * PR)]
    remote(sent, sent, send_sem.at[0], ring_recv.at[0], twin_id).wait_send()


def ring_call(sizes, operands):
    D, M, S, C, E, H, rows, P = sizes
    L, N = M * S, D * M
    T = P * (N - 1) // 2
    f32, bf16 = jnp.float32, jnp.bfloat16
    vmem = pl.BlockSpec(memory_space=pltpu.VMEM)
    hbm = pl.BlockSpec(memory_space=pl.ANY)
    dma = pltpu.SemaphoreType.DMA
    slots = S + T
    crossing = max(min(2 * (D - 1 - i), 2 * i) + 1 for i in range(D))
    stages = max(D - 1, crossing + 1) - 1
    scratch = [
        pltpu.VMEM((E, H), bf16),
        pltpu.VMEM((slots * C, E), bf16),
        pltpu.VMEM((slots // 2, 2 * C, H), bf16),
        pltpu.VMEM((slots // 2, 2 * C, H), bf16),
        pltpu.VMEM((3, 1, C), jnp.int32),
        pltpu.VMEM((C, E), f32),
        pltpu.VMEM((16, H), f32),
        pltpu.VMEM((D, 3, 1, C), f32),
        pltpu.VMEM((D, 8, C), f32),
        pltpu.VMEM((D, 8, C), f32),
        pltpu.VMEM((L, D, 1, C), f32),
        pltpu.VMEM((L, D, 8, C), f32),
        pltpu.VMEM((slots // 2, 8, 2 * C), f32),
        pltpu.VMEM((slots // 2, 16, 2 * C), bf16),
        dma((6,)), dma((T,)), dma((T,)), dma((2,)), dma((2,)), dma((2,)), dma((1,)),
        pltpu.SemaphoreType.REGULAR((stages,)),
        pltpu.SemaphoreType.REGULAR((1,)),
    ]
    held = pl.pallas_call(
        functools.partial(ring_kernel, sizes),
        out_shape=(
            pltpu.VMEM((C, E), bf16),
            pltpu.VMEM((rows, H), f32),
            pltpu.VMEM((1, H), f32),
            pltpu.VMEM((rows, 2 * C), bf16),
            pltpu.VMEM((2 * C, H), bf16),
            pltpu.VMEM((1, H), f32),
        ),
        in_specs=[hbm] * 6,
        out_specs=(vmem,) * 6,
        scratch_shapes=scratch,
        compiler_params=pltpu.CompilerParams(
            collective_id=0, has_side_effects=True, vmem_limit_bytes=56 * 1024 * 1024
        ),
    )(*operands)
    return pl.pallas_call(
        finish,
        out_shape=(
            jax.ShapeDtypeStruct((C, E), bf16),
            jax.ShapeDtypeStruct((rows, H), f32),
            jax.ShapeDtypeStruct((1, H), f32),
        ),
        in_specs=[vmem] * 6,
        out_specs=(hbm,) * 3,
        scratch_shapes=[pltpu.VMEM((rows, H), f32), dma((3,))],
        compiler_params=pltpu.CompilerParams(vmem_limit_bytes=4 * 1024 * 1024),
    )(*held)


def finish(emb_grad, w1g, w2g, at, slope, w2, emb_out, w1g_out, w2g_out, w1g_end, sem):
    H = w2.shape[1]
    parts = PARTS
    wide = H // parts
    copies = [
        pltpu.make_async_copy(emb_grad, emb_out, sem.at[0]),
        pltpu.make_async_copy(w2g, w2g_out, sem.at[1]),
    ]
    for copy in copies:
        copy.start()
    for c in range(parts):
        cols = slice(c * wide, (c + 1) * wide)
        grad = jnp.dot(at[...], slope[:, cols], preferred_element_type=jnp.float32)
        w1g_end[:, cols] = (w1g[:, cols] + grad) * w2[:, cols]
        pltpu.make_async_copy(w1g_end.at[:, cols], w1g_out.at[:, cols], sem.at[2]).start()
    for copy in copies:
        copy.wait()
    pltpu.make_async_copy(w1g_end, w1g_out, sem.at[2]).wait()


def write_out(a_ref, b_ref, c_ref, a_out, b_out, c_out, sem):
    pairs = ((b_ref, b_out), (a_ref, a_out), (c_ref, c_out))
    copies = [pltpu.make_async_copy(x, y, sem.at[i]) for i, (x, y) in enumerate(pairs)]
    for copy in copies:
        copy.start()
    for copy in copies:
        copy.wait()


def reduce_call(sizes, operands):
    D, M, S, C, E, H, rows = sizes
    L = M * S
    width = max(rows, LANES)
    Kc = 4
    Kr = max(1, rows // 32)
    K = Kc * Kr
    f32, bf16 = jnp.float32, jnp.bfloat16
    vmem = pl.BlockSpec(memory_space=pltpu.VMEM)
    hbm = pl.BlockSpec(memory_space=pl.ANY)
    dma = pltpu.SemaphoreType.DMA
    chunk = (K, rows // Kr, H // Kc)
    scratch = [
        pltpu.VMEM((E, H), bf16),
        pltpu.VMEM((L * C, E), bf16),
        pltpu.VMEM((L * C, H), f32),
        pltpu.VMEM((L * C, H), f32),
        pltpu.VMEM((L * C, H), bf16),
        pltpu.VMEM((width, L * C), bf16),
        pltpu.VMEM((Kc, width, H // Kc), f32),
        pltpu.VMEM((D, 8, C), f32),
        pltpu.VMEM((D, 8, C), f32),
        pltpu.VMEM((D, 8, C), f32),
        pltpu.VMEM((D, 8, C), f32),
        pltpu.VMEM((L, 8, C), f32),
        pltpu.VMEM((D, H // LANES, LANES), f32),
        pltpu.VMEM(chunk, bf16),
        pltpu.VMEM(chunk, bf16),
        pltpu.VMEM(chunk, bf16),
        pltpu.VMEM(chunk, bf16),
        dma((2,)),
        dma((L,)), dma((L,)),
        dma((D,)), dma((D,)),
        dma((D,)), dma((D,)),
        dma((L,)), dma((L,)),
        dma((D,)), dma((D,)),
        dma((K,)), dma((K,)), dma((K,)), dma((K,)),
    ]
    return pl.pallas_call(
        functools.partial(kernel, (D, M, S, C, E, H, rows, Kc, Kr)),
        out_shape=(
            pltpu.VMEM((C, E), bf16),
            pltpu.VMEM((rows, H), f32),
            pltpu.VMEM((1, H), f32),
        ),
        in_specs=[hbm, hbm, vmem, vmem, vmem, vmem],
        out_specs=(vmem, vmem, vmem),
        scratch_shapes=scratch,
        compiler_params=pltpu.CompilerParams(
            collective_id=0, has_side_effects=True, vmem_limit_bytes=56 * 1024 * 1024
        ),
    )(*operands)


def on_device(embeddings, owner_shard, query_local, labels, w_first, w_second):
    D, M, S = lax.axis_size("docs"), lax.axis_size("mp"), lax.axis_size("sub")
    C, E = embeddings.shape
    H = w_first.shape[1]
    L = M * S
    rows = E // L
    vmem = pl.BlockSpec(memory_space=pltpu.VMEM)
    hbm = pl.BlockSpec(memory_space=pl.ANY)
    dma = pltpu.SemaphoreType.DMA
    operands = (
        embeddings, w_first, owner_shard.reshape(1, C), query_local.reshape(1, C),
        labels.reshape(1, C), w_second.reshape(1, H),
    )
    P = 2 * S
    held = D * L * C * (E + 2 * H) * 2
    gathers = (
        M == 2 and S == 2 and D > 3 and C == LANES and rows % LANES == 0 and held <= 32 * 2**20
    )
    if gathers:
        emb_grad, w1g, w2g = ring_call((D, M, S, C, E, H, rows, P), operands)
        return emb_grad, w1g, w2g.reshape(H)
    emb_grad, w1g, w2g = reduce_call((D, M, S, C, E, H, rows), operands)
    emb_grad, w1g, w2g = pl.pallas_call(
        write_out,
        out_shape=tuple(jax.ShapeDtypeStruct(v.shape, v.dtype) for v in (emb_grad, w1g, w2g)),
        in_specs=[vmem] * 3,
        out_specs=(hbm,) * 3,
        scratch_shapes=[dma((3,))],
        compiler_params=pltpu.CompilerParams(vmem_limit_bytes=4 * 1024 * 1024),
    )(emb_grad, w1g, w2g)
    return emb_grad, w1g, w2g.reshape(H)


def solution(mesh):
    return jax.shard_map(
        on_device,
        mesh=mesh,
        in_specs=(
            P(("groups", "docs", "mp", "sub"), None),
            P(("groups", "docs", "mp", "sub"), None),
            P(("groups", "docs", "mp", "sub")),
            P(("groups", "docs", "mp", "sub")),
            P(),
            P(),
        ),
        out_specs=(
            P(("groups", "docs", "mp", "sub"), None),
            P(("groups", "mp", "sub"), None),
            P("groups"),
        ),
        check_vma=False,
    )
```
